256 devices in a mesh: heads: 4 (over x), ctx: 64 (over y, z, core).
Axes of the slice: x: 4, y: 4, z: 8, core: 2. Of those that a mesh axis runs over, the one named last changes fastest.
Arguments:
- hidden: bfloat16 [8192, 4096], P('ctx', 'heads'), may hold values from -6 to 6
- w_query: bfloat16 [4096, 4096], P('ctx', 'heads'), may hold values from -0.09375 to 0.09375
- key_input: bfloat16 [8192, 4096], P('ctx', 'heads'), may hold values from -6 to 6
- values: bfloat16 [8192, 2048], P('ctx', 'heads'), may hold values from -6 to 6
- cotangent: bfloat16 [8192, 2048], P('ctx', 'heads'), may hold values from -6 to 6
Outputs:
- attended: bfloat16 [8192, 2048], P('ctx', 'heads')
- query_grad: float32 [4096, 4096], P('ctx', 'heads')
- key_grad: bfloat16 [8192, 4096], P('ctx', 'heads')
- value_grad: bfloat16 [8192, 2048], P('ctx', 'heads')
The draws below stay inside these ranges and needn't reach their ends.
All inputs are finite; a program needn't handle non-finite values.
Results may differ from the reference program's by a relative error of at most 0.015.
Values may be sent and summed in bfloat16 or wider, within the bound.
A program may use at most 128 MiB of HBM per device.

```python
import jax
import jax.numpy as jnp
from jax import lax

D = 4096
HEAD_DIM = 128
FEAT = 256
HEADS_GROUP = 4
TOK_DEV = 128
HEADS = 16
LENGTH = 8192
N_HEADS = 4


def levels(own_key, extent, cuts, low, largest):
    level, own = 1.0, jax.random.fold_in(own_key, 6)
    for axis_at, blocks in cuts:
        heights = jnp.exp(jax.random.uniform(jax.random.fold_in(own, axis_at), (blocks,), jnp.float32, low / len(cuts), largest / len(cuts)))
        level = level * jnp.repeat(heights, extent[axis_at] // blocks).reshape([-1 if axis == axis_at else 1 for axis in range(len(extent))])
    return level


def normal_values(rng, dims, width, reach, pieces=(), held_as=jnp.bfloat16):
    array = width * jax.random.normal(rng, dims, jnp.float32)
    if pieces:
        array = array * levels(rng, dims, pieces, -0.22, 0.18)
    return jnp.clip(array, -reach, reach).astype(held_as)


def setup_inputs(seed: int = 0) -> dict:
    seeds = jax.random.split(jax.random.key(seed), 6)
    return {
        "hidden": normal_values(seeds[0], (LENGTH, D), 1.0, 6.0, ((0, 64), (1, 4))),
        "w_query": normal_values(seeds[1], (D, HEADS * FEAT), D ** -0.5, 0.09375, ((0, 64), (1, 4))),
        "key_input": normal_values(seeds[2], (LENGTH, HEADS * FEAT), 1.0, 6.0, ((0, 64), (1, 4))),
        "values": normal_values(seeds[3], (LENGTH, HEADS * HEAD_DIM), 1.0, 6.0, ((0, 64), (1, 4))),
        "cotangent": normal_values(seeds[4], (LENGTH, HEADS * HEAD_DIM), 1.0, 6.0, ((0, 64), (1, 4))),
    }


EPSILON = 1e-06
HIGHEST = lax.Precision.HIGHEST

def reference(hidden, w_query, key_input, values, cotangent):
    head_count = HEADS_GROUP * N_HEADS
    length = hidden.shape[0]
    blocks = length // TOK_DEV
    query_proj = jnp.dot(hidden, w_query, preferred_element_type=jnp.float32)
    query_feats = jnp.maximum(query_proj, 0.0).astype(jnp.bfloat16)
    key_feats = jnp.maximum(key_input, jnp.zeros_like(key_input))
    causal = jnp.arange(TOK_DEV)[:, None] >= jnp.arange(TOK_DEV)[None, :]
    block_queries = query_feats.reshape(blocks, TOK_DEV, head_count, FEAT)
    block_keys = key_feats.reshape(blocks, TOK_DEV, head_count, FEAT)
    block_values = values.reshape(blocks, TOK_DEV, head_count, HEAD_DIM)

    def make_scores(queries, keys_here):
        raw = jnp.einsum('thf,shf->hts', queries.astype(jnp.float32), keys_here.astype(jnp.float32))
        return jnp.where(causal[None], raw, 0.0).astype(jnp.bfloat16)

    def forward(carried, block_data):
        queries, keys_here, value_rows = block_data
        scores = make_scores(queries, keys_here)
        inner = jnp.einsum('hts,she->the', scores.astype(jnp.float32), value_rows.astype(jnp.float32))
        outer = jnp.einsum('thf,hfe->the', queries.astype(jnp.float32), carried, precision=HIGHEST)
        update = jnp.einsum('shf,she->hfe', keys_here.astype(jnp.float32), value_rows.astype(jnp.float32))
        return (carried + update, (inner + outer, carried))
    empty = jnp.zeros((head_count, FEAT, HEAD_DIM), jnp.float32)
    unused, (numerators, priors) = lax.scan(forward, empty, (block_queries, block_keys, block_values))
    numerator = numerators.reshape(length, head_count, HEAD_DIM)
    inv_rms = lax.rsqrt(lax.optimization_barrier(jnp.mean(numerator * numerator, axis=-1, keepdims=True)) + EPSILON)
    normed = numerator * inv_rms
    attended = normed.astype(jnp.bfloat16).reshape(length, head_count * HEAD_DIM)
    grad_out = cotangent.astype(jnp.float32).reshape(length, head_count, HEAD_DIM)
    d_numer = (inv_rms * (grad_out - normed * lax.optimization_barrier(jnp.mean(grad_out * normed, axis=-1, keepdims=True)))).astype(jnp.bfloat16)
    block_dnum = d_numer.reshape(blocks, TOK_DEV, head_count, HEAD_DIM)

    def backward(carried, block_data):
        queries, keys_here, value_rows, dnum_rows, prior_state = block_data
        scores = make_scores(queries, keys_here).astype(jnp.float32)
        queries32 = queries.astype(jnp.float32)
        keys32 = keys_here.astype(jnp.float32)
        values32 = value_rows.astype(jnp.float32)
        dnum32 = dnum_rows.astype(jnp.float32)
        mixed_raw = jnp.einsum('the,she->hts', dnum32, values32)
        mixed_scores = jnp.where(causal[None], mixed_raw, 0.0).astype(jnp.bfloat16).astype(jnp.float32)
        d_featq = jnp.einsum('hts,shf->thf', mixed_scores, keys32) + jnp.einsum('the,hfe->thf', dnum32, prior_state, precision=HIGHEST)
        d_vals = jnp.einsum('hts,the->she', scores, dnum32) + jnp.einsum('shf,hfe->she', keys32, carried, precision=HIGHEST)
        d_featk = jnp.einsum('hts,thf->shf', mixed_scores, queries32) + jnp.einsum('she,hfe->shf', values32, carried, precision=HIGHEST)
        update = jnp.einsum('thf,the->hfe', queries32, dnum32)
        return (carried + update, (d_featq, d_vals, d_featk))
    unused_two, (d_featq, d_vals, d_featk) = lax.scan(backward, empty, (block_queries, block_keys, block_values, block_dnum, priors), reverse=True)
    d_query = jnp.where(query_proj > 0, d_featq.reshape(length, head_count * FEAT), 0.0).astype(jnp.bfloat16)
    query_grad = lax.dot_general(hidden, d_query, (((0,), (0,)), ((), ())), preferred_element_type=jnp.float32)
    value_grad = d_vals.reshape(length, head_count * HEAD_DIM).astype(jnp.bfloat16)
    key_grad = jnp.where(key_input > 0, d_featk.reshape(length, head_count * FEAT), 0.0).astype(jnp.bfloat16)
    return (attended, query_grad, key_grad, value_grad)
```

```python
import jax
import jax.numpy as jnp
from jax import lax
from jax.experimental import pallas as pl
from jax.experimental.pallas import tpu as pltpu
from jax.sharding import PartitionSpec as P

HEAD_DIM = 128
FEAT = 256
CORES = 2
EPSILON = 1e-06
MESH = pl.DeviceIdType.MESH
F32 = jnp.float32
BF16 = jnp.bfloat16
CHANNELS = 200
LOCALS = 16


def grid_of(ctx_size):
    if ctx_size == 64:
        return 4, 8
    return 2, ctx_size // (2 * CORES)


def dot_nn(a, b):
    return lax.dot_general(a, b, (((1,), (0,)), ((), ())), preferred_element_type=F32)


def dot_nt(a, b):
    return lax.dot_general(a, b, (((1,), (1,)), ((), ())), preferred_element_type=F32)


def dot_tn(a, b):
    return lax.dot_general(a, b, (((0,), (0,)), ((), ())), preferred_element_type=F32)


class Net:
    def __init__(self, send_sems, recv_sems):
        self.send_sems, self.recv_sems = send_sems, recv_sems
        self.ids = {}
        self.copies = []

    def send(self, name, src, dst, device):
        assert name not in self.ids, name
        at = len(self.copies)
        self.ids[name] = at
        copy = pltpu.make_async_remote_copy(
            src_ref=src,
            dst_ref=dst,
            send_sem=self.send_sems.at[at],
            recv_sem=self.recv_sems.at[at],
            device_id=device,
            device_id_type=MESH,
        )
        copy.start()
        self.copies.append([copy, False, device])

    def recv(self, name, dst):
        at = self.ids[name]
        assert not self.copies[at][1], name
        self.copies[at][1] = True
        pltpu.make_async_remote_copy(
            src_ref=dst,
            dst_ref=dst,
            send_sem=self.send_sems.at[at],
            recv_sem=self.recv_sems.at[at],
            device_id=self.copies[at][2],
            device_id_type=MESH,
        ).wait_recv()

    def finish(self):
        for copy, received, _ in self.copies:
            assert received
            copy.wait_send()


def kernel(
    sizes, hidden, w_query, key_input, values, cotangent,
    out_att, out_qg, out_kg, out_vg,
    hf, wf, ki, kf, va, ct, q32, qf, att, dn, sc, mx, vg32, kg32, kg, vg,
    s_out, s_in, t_out, t_in, b_out, prior, later, pre,
    h4, h4t, dq4, g32, rs_out, rs_in, qg,
    send_sems, recv_sems, local_sems,
):
    NX, NY, NZ = sizes
    x = lax.axis_index("heads")
    ctx = lax.axis_index("ctx")
    c = ctx % CORES
    z = (ctx // CORES) % NZ
    y = ctx // (CORES * NZ)
    p = 1 - c
    T, DX = hidden.shape
    WR, NALL = w_query.shape
    NC = NALL // CORES
    VC = values.shape[1] // CORES
    CH = CORES * WR
    KY = NZ * CH
    CT = CORES * T
    HEADS = NC // FEAT
    XM, YM, ZM = NX // 2, NY // 2, NZ // 2

    def dev(dx=0, dy=0, dz=0, core=None):
        nx = (x + dx + NX) % NX
        ny = (y + dy + NY) % NY
        nz = (z + dz + NZ) % NZ
        return (nx, (ny * NZ + nz) * CORES + (c if core is None else core))

    partner = dev(core=p)
    net = Net(send_sems, recv_sems)

    own_chunk = (y * NZ + z) * CH
    my_rows = pl.ds(pl.multiple_of(c * T, T), T)
    its_rows = pl.ds(pl.multiple_of(p * T, T), T)
    my_x = pl.ds(pl.multiple_of(x * DX, DX), DX)

    def w_rows(core):
        return pl.ds(pl.multiple_of(own_chunk + core * WR, WR), WR)

    def cols(core, width):
        return pl.ds(pl.multiple_of(core * width, width), width)

    moves = [
        ("w", w_query.at[:, cols(c, NC)], wf.at[w_rows(c), :]),
        ("h", hidden, hf.at[my_rows, my_x]),
        ("k", key_input.at[:, cols(c, NC)], ki.at[my_rows, :]),
        ("v", values.at[:, cols(c, VC)], va.at[my_rows, :]),
        ("g", cotangent.at[:, cols(c, VC)], ct.at[my_rows, :]),
    ]
    local = {}
    for at, (name, src, dst) in enumerate(moves):
        local[name] = pltpu.make_async_copy(src, dst, local_sems.at[at])
        local[name].start()

    barrier = pltpu.get_barrier_semaphore()
    friends = [partner]
    friends += [dev(dx=d) for d in sorted({1, NX - 1})]
    friends += [dev(dy=d) for d in range(1, NY)]
    friends += [dev(dz=d) for d in range(1, NZ)]
    for friend in friends:
        pl.semaphore_signal(barrier, inc=1, device_id=friend, device_id_type=MESH)
    pl.semaphore_wait(barrier, len(friends))

    net.send("w", w_query.at[:, cols(p, NC)], wf.at[w_rows(c), :], partner)
    net.send("h", hidden, hf.at[my_rows, my_x], partner)
    net.send("k", key_input.at[:, cols(p, NC)], ki.at[my_rows, :], partner)
    net.send("v", values.at[:, cols(p, VC)], va.at[my_rows, :], partner)
    net.send("g", cotangent.at[:, cols(p, VC)], ct.at[my_rows, :], partner)

    def split(total, top, part):
        return {"full": (0, total), "top": (0, top), "bot": (top, total - top)}[part]

    def part_of(direction, d, most):
        if d < most:
            return "full"
        return "top" if direction > 0 else "bot"

    A_ROWS = CH * 5 // 8
    A_TOP = A_ROWS * 3 // 5
    B_ROWS = CH - A_ROWS
    B_TOP = B_ROWS * 2 // 3

    def w_piece(stream, rel_y, rel_z, part):
        if stream == "A":
            start, size = split(A_ROWS, A_TOP, part)
        else:
            start, size = split(B_ROWS, B_TOP, part)
            start = start + A_ROWS
        at = (((y + rel_y + NY) % NY) * NZ + (z + rel_z + NZ) % NZ) * CH + start
        return wf.at[pl.ds(pl.multiple_of(at, 16), size), :]

    def w_send(stream, axis, rel, direction, d):
        most = ZM if axis == "z" else YM
        back = -direction * (d - 1)
        rel_y, rel_z = (rel, back) if axis == "z" else (back, rel)
        piece = w_piece(stream, rel_y, rel_z, part_of(direction, d, most))
        to = dev(dz=direction) if axis == "z" else dev(dy=direction)
        net.send((stream, axis, rel, direction, d), piece, piece, to)

    def w_recv(stream, axis, rel, direction, d):
        most = ZM if axis == "z" else YM
        back = -direction * d
        rel_y, rel_z = (rel, back) if axis == "z" else (back, rel)
        piece = w_piece(stream, rel_y, rel_z, part_of(direction, d, most))
        net.recv((stream, axis, rel, direction, d), piece)

    def fresh(r, most):
        return [-r, r] if r < most else [most]

    BOTH = (1, -1)
    a_wait = []
    b_wait = []

    def w_round(r):
        if r == 0:
            for s in BOTH:
                w_send("A", "z", 0, s, 1)
            for s in BOTH:
                w_send("B", "y", 0, s, 1)
            for s in BOTH:
                w_send("A", "y", 0, s, 1)
            for s in BOTH:
                w_send("B", "z", 0, s, 1)
            return
        if r <= ZM:
            for s in BOTH:
                w_recv("A", "z", 0, s, r)
                if r < ZM:
                    w_send("A", "z", 0, s, r + 1)
            for rel in fresh(r, ZM):
                for s in BOTH:
                    w_send("A", "y", rel, s, 1)
        starts = {0: 0}
        for k in range(1, YM + 1):
            for rel in fresh(k, YM):
                starts[rel] = k
        for rel, start in starts.items():
            d = r - start
            if 1 <= d <= ZM:
                for s in BOTH:
                    w_recv("B", "z", rel, s, d)
                    if d < ZM:
                        w_send("B", "z", rel, s, d + 1)
        if r <= YM:
            for s in BOTH:
                w_recv("B", "y", 0, s, r)
                if r < YM:
                    w_send("B", "y", 0, s, r + 1)
            for rel in fresh(r, YM):
                for s in BOTH:
                    w_send("B", "z", rel, s, 1)
        if r <= ZM + 1:
            for rel in fresh(r - 1, ZM) if r > 1 else [0]:
                for s in BOTH:
                    w_recv("A", "y", rel, s, 1)
                    if YM > 1:
                        w_send("A", "y", rel, s, 2)

    def h_piece(core_rows, rel_x, part, rows0):
        start, size = split(T, T // 2, part)
        at = rows0 + start
        xs = (x + rel_x + NX) % NX
        return hf.at[pl.ds(pl.multiple_of(at, T // 2), size), pl.ds(pl.multiple_of(xs * DX, DX), DX)]

    def h_send(direction, d):
        piece = h_piece(None, -direction * (d - 1), part_of(direction, d, XM), c * T)
        net.send(("h", direction, d), piece, piece, dev(dx=direction))

    def h_recv(direction, d):
        piece = h_piece(None, -direction * d, part_of(direction, d, XM), c * T)
        net.recv(("h", direction, d), piece)

    def h_relay(rel, part):
        piece = h_piece(None, rel, part, c * T)
        net.send(("hp", rel, part), piece, piece, partner)

    def h_relay_recv(rel, part):
        net.recv(("hp", rel, part), h_piece(None, rel, part, p * T))

    SL = s_out.shape[1] // NZ

    def scan_start(kind):
        for o in range(1, NZ):
            to = (z + o) % NZ
            src = s_out.at[kind, pl.ds(pl.multiple_of(to * SL, SL), SL), :]
            net.send((kind, "s", o), src, s_in.at[kind, o], dev(dz=o))

    def slice_from(kind, o):
        return s_in[kind, o].astype(F32)

    def scan_totals(kind):
        own = s_out[kind, pl.ds(pl.multiple_of(z * SL, SL), SL), :].astype(F32)
        total = own
        for o in range(1, NZ):
            net.recv((kind, "s", o), s_in.at[kind, o])
            total = total + slice_from(kind, o)
        t_out[kind] = total.astype(BF16)
        for o in range(1, NY):
            net.send((kind, "t", o), t_out.at[kind], t_in.at[kind, o], dev(dy=o))
        pre[pl.ds(pl.multiple_of(z * SL, SL), SL), :] = own
        for o in range(1, NZ):
            at = (z - o + NZ) % NZ
            pre[pl.ds(pl.multiple_of(at * SL, SL), SL), :] = slice_from(kind, o)

    def scan_back(kind, result):
        offset = jnp.zeros((SL, HEAD_DIM), F32)
        for o in range(1, NY):
            net.recv((kind, "t", o), t_in.at[kind, o])
            source = (y - o + NY) % NY
            counts = source < y if kind == 0 else source > y
            offset = offset + jnp.where(counts, t_in[kind, o].astype(F32), 0.0)
        order = range(NZ) if kind == 0 else reversed(range(NZ))
        running = offset
        for k in order:
            rows = pl.ds(k * SL, SL)
            b_out[kind, rows, :] = running.astype(BF16)
            running = running + pre[rows, :]
        for o in range(1, NZ):
            to = (z + o) % NZ
            src = b_out.at[kind, pl.ds(pl.multiple_of(to * SL, SL), SL), :]
            dst = result.at[pl.ds(pl.multiple_of(z * SL, SL), SL), :]
            net.send((kind, "b", o), src, dst, dev(dz=o))
        mine = pl.ds(pl.multiple_of(z * SL, SL), SL)
        result[mine, :] = b_out[kind, mine, :]

    def scan_end(kind, result):
        for o in range(1, NZ):
            at = (z - o + NZ) % NZ
            net.recv((kind, "b", o), result.at[pl.ds(pl.multiple_of(at * SL, SL), SL), :])

    PT = T // NX

    def quarter(rel_x):
        xs = (x + rel_x + NX) % NX
        return pl.ds(pl.multiple_of(xs * PT, PT), PT)

    def h4_start():
        for o in range(1, NY):
            to = (y + o) % NY
            src = hf.at[
                pl.ds(pl.multiple_of(c * T + x * PT, PT), PT),
                pl.ds(pl.multiple_of(to * KY, KY), KY),
            ]
            net.send(("h4", o), src, h4.at[y, c, quarter(0), :], dev(dy=o))
        h4[y, c, quarter(0), :] = hf[
            pl.ds(pl.multiple_of(c * T + x * PT, PT), PT),
            pl.ds(pl.multiple_of(y * KY, KY), KY),
        ]

    def h4_piece(core, rel_x, part):
        start, size = split(NY, NY // 2, part)
        return h4.at[pl.ds(start, size), core, quarter(rel_x), :]

    def h4_send(direction, d):
        piece = h4_piece(c, -direction * (d - 1), part_of(direction, d, XM))
        net.send(("h4x", direction, d), piece, piece, dev(dx=direction))

    def h4_recv(direction, d):
        net.recv(("h4x", direction, d), h4_piece(c, -direction * d, part_of(direction, d, XM)))

    def h4_relay(rel, part):
        piece = h4_piece(c, rel, part)
        net.send(("h4p", rel, part), piece, piece, partner)

    def h4_relay_recv(rel, part):
        net.recv(("h4p", rel, part), h4_piece(p, rel, part))

    def x_first():
        return [(s, -s) for s in BOTH] if XM > 1 else []

    local["w"].wait()
    net.recv("w", wf.at[w_rows(p), :])
    w_round(0)
    local["h"].wait()
    for s in BOTH:
        h_send(s, 1)
    for name in ("k", "v", "g"):
        local[name].wait()
    net.recv("k", ki.at[its_rows, :])
    net.recv("v", va.at[its_rows, :])
    kf[...] = jnp.maximum(ki[...], jnp.zeros_like(ki[...]))
    for h in range(HEADS):
        fs, vs = slice(h * FEAT, (h + 1) * FEAT), slice(h * HEAD_DIM, (h + 1) * HEAD_DIM)
        s_out[0, fs, :] = dot_tn(kf[:, fs], va[:, vs]).astype(BF16)
    scan_start(0)
    w_round(1)
    net.recv("h", hf.at[its_rows, my_x])
    net.recv("g", ct.at[its_rows, :])
    if XM > 1:
        for s in BOTH:
            h_recv(s, 1)
            h_send(s, 2)
            h_relay(-s, "full")
    scan_totals(0)
    w_round(2)
    for s in BOTH:
        h_recv(s, XM)
    h_relay(XM, "full")
    scan_back(0, prior)
    w_round(3)
    h4_start()
    w_round(4)
    for s, rel in x_first():
        h_relay_recv(rel, "full")
    h_relay_recv(XM, "full")
    for o in range(1, NY):
        at = (y - o + NY) % NY
        net.recv(("h4", o), h4.at[at, c, quarter(0), :])
    for s in BOTH:
        h4_send(s, 1)
    h4_relay(0, "full")
    w_round(5)
    if XM > 1:
        for s in BOTH:
            h4_recv(s, 1)
            h4_send(s, 2)
            h4_relay(-s, "full")
    w_round(6)

    def region(rel):
        ys = (y + rel + NY) % NY
        rows = pl.ds(pl.multiple_of(ys * KY, KY), KY)
        return dot_nn(hf[:, rows], wf[rows, :])

    q32[...] = region(0)
    for s in BOTH:
        h4_recv(s, XM)
    h4_relay(XM, "full")
    scan_end(0, prior)
    h4_relay_recv(0, "full")
    for s, rel in x_first():
        h4_relay_recv(rel, "full")
    h4_relay_recv(XM, "full")
    width = min(KY, 256)
    for k in range(KY // width):
        cut = slice(k * width, (k + 1) * width)
        h4t[cut, :] = h4[:, :, :, cut].reshape(NY * CT, width).T
    if YM > 1:
        q32[...] += region(-1)
        q32[...] += region(1)
        for r in range(ZM + 1):
            for rel in fresh(r, ZM) if r > 0 else [0]:
                for s in BOTH:
                    w_recv("A", "y", rel, s, 2)
    q32[...] += region(YM)

    causal = lax.broadcasted_iota(jnp.int32, (CT, CT), 0) >= lax.broadcasted_iota(
        jnp.int32, (CT, CT), 1
    )

    def dq_piece(h, rel, part):
        start, size = split(CT, CT // 2, part)
        ys = (y + rel + NY) % NY
        return dq4.at[h, pl.ds(pl.multiple_of(ys * CT + start, CT // 2), size), :]

    def dq_send(h, direction, d):
        piece = dq_piece(h, -direction * (d - 1), part_of(direction, d, YM))
        net.send(("dq", h, direction, d), piece, piece, dev(dy=direction))

    def dq_recv(h, direction, d):
        net.recv(("dq", h, direction, d), dq_piece(h, -direction * d, part_of(direction, d, YM)))

    for h in range(HEADS):
        fs, vs = slice(h * FEAT, (h + 1) * FEAT), slice(h * HEAD_DIM, (h + 1) * HEAD_DIM)
        proj = q32[:, fs]
        feats = jnp.maximum(proj, 0.0).astype(BF16)
        qf[:, fs] = feats
        keys, vals, state = kf[:, fs], va[:, vs], prior[fs, :]
        scores = jnp.where(causal, dot_nt(feats, keys), 0.0).astype(BF16)
        sc[h] = scores
        numer = dot_nn(scores, vals) + dot_nn(feats, state)
        inv = lax.rsqrt(jnp.mean(numer * numer, axis=-1, keepdims=True) + EPSILON)
        normed = numer * inv
        att[:, vs] = normed.astype(BF16)
        grad = ct[:, vs].astype(F32)
        d_num = (inv * (grad - normed * jnp.mean(grad * normed, axis=-1, keepdims=True))).astype(BF16)
        dn[:, vs] = d_num
        mixed = jnp.where(causal, dot_nt(d_num, vals), 0.0).astype(BF16)
        mx[h] = mixed
        d_feat = dot_nn(mixed, keys) + dot_nt(d_num, state)
        d_q = jnp.where(proj > 0, d_feat, 0.0).astype(BF16)
        dq4[h, pl.ds(pl.multiple_of(y * CT, CT), CT), :] = d_q
        for s in BOTH:
            dq_send(h, s, 1)
        s_out[1, fs, :] = dot_tn(feats, d_num).astype(BF16)
    scan_start(1)

    def out_send(name, buf, rows, out, width, at):
        mine = out.at[:, cols(c, width)]
        keep = buf.at[pl.ds(pl.multiple_of(c * rows, rows), rows), :]
        give = buf.at[pl.ds(pl.multiple_of(p * rows, rows), rows), :]
        net.send(name, give, mine, partner)
        local[name] = pltpu.make_async_copy(keep, mine, local_sems.at[at])
        local[name].start()

    def out_recv(name, out, width):
        net.recv(name, out.at[:, cols(p, width)])
        local[name].wait()

    out_send("att", att, T, out_att, VC, 5)
    for h in range(HEADS):
        if YM > 1:
            for s in BOTH:
                dq_recv(h, s, 1)
                dq_send(h, s, 2)
    for h in range(HEADS):
        fs, vs = slice(h * FEAT, (h + 1) * FEAT), slice(h * HEAD_DIM, (h + 1) * HEAD_DIM)
        vg32[:, vs] = dot_tn(sc[h], dn[:, vs])
        kg32[:, fs] = dot_tn(mx[h], qf[:, fs])
    scan_totals(1)

    def rs_rows(part):
        start, size = split(CH, CH // 2, part)
        return slice(start, start + size)

    def rs_send(h, direction, d):
        part = part_of(direction, d, ZM)
        rows = rs_rows(part)
        to = (z + direction * d + NZ) % NZ
        base = to * CH + rows.start
        size = rows.stop - rows.start
        total = g32[h, pl.ds(pl.multiple_of(base, CH // 2), size), :]
        way = 0 if direction > 0 else 1
        if d < ZM:
            before = part_of(direction, d + 1, ZM)
            came = rs_rows(before)
            net.recv(("rs", h, direction, d + 1), rs_in.at[h, way, d, came, :])
            got = rs_in[h, way, d, came, :].astype(F32)
            if before == "full":
                total = total + got
                rs_out[h, way, d - 1, rows, :] = total.astype(BF16)
            else:
                rs_out[h, way, d - 1, rows, :] = total.astype(BF16)
                rs_out[h, way, d - 1, came, :] = (total[came, :] + got).astype(BF16)
        else:
            rs_out[h, way, d - 1, rows, :] = total.astype(BF16)
        net.send(
            ("rs", h, direction, d),
            rs_out.at[h, way, d - 1, rows, :],
            rs_in.at[h, way, d - 1, rows, :],
            dev(dz=direction),
        )

    for h in range(HEADS):
        for s in BOTH:
            dq_recv(h, s, YM)
        g32[h] = dot_nn(h4t[...], dq4[h])
        for s in BOTH:
            rs_send(h, s, ZM)
        if h == 0:
            scan_back(1, later)

    for d in reversed(range(1, ZM)):
        for h in range(HEADS):
            for s in BOTH:
                rs_send(h, s, d)
        if d == max(1, ZM - 2):
            scan_end(1, later)
            for h in range(HEADS):
                fs, vs = slice(h * FEAT, (h + 1) * FEAT), slice(h * HEAD_DIM, (h + 1) * HEAD_DIM)
                state = later[fs, :]
                vg[:, vs] = (vg32[:, vs] + dot_nn(kf[:, fs], state)).astype(BF16)
                d_key = kg32[:, fs] + dot_nt(va[:, vs], state)
                kg[:, fs] = jnp.where(ki[:, fs] > 0, d_key, 0.0).astype(BF16)
            out_send("kg", kg, T, out_kg, NC, 6)
            out_send("vg", vg, T, out_vg, VC, 7)
    if ZM == 1:
        scan_end(1, later)
        for h in range(HEADS):
            fs, vs = slice(h * FEAT, (h + 1) * FEAT), slice(h * HEAD_DIM, (h + 1) * HEAD_DIM)
            state = later[fs, :]
            vg[:, vs] = (vg32[:, vs] + dot_nn(kf[:, fs], state)).astype(BF16)
            d_key = kg32[:, fs] + dot_nt(va[:, vs], state)
            kg[:, fs] = jnp.where(ki[:, fs] > 0, d_key, 0.0).astype(BF16)
        out_send("kg", kg, T, out_kg, NC, 6)
        out_send("vg", vg, T, out_vg, VC, 7)

    for h in range(HEADS):
        fs = slice(h * FEAT, (h + 1) * FEAT)
        total = g32[h, pl.ds(pl.multiple_of(z * CH, CH), CH), :]
        if ZM > 1:
            for s in BOTH:
                way = 0 if s > 0 else 1
                net.recv(("rs", h, s, 1), rs_in.at[h, way, 0])
                total = total + rs_in[h, way, 0].astype(F32)
            qg[:, fs] = total
        else:
            for s in BOTH:
                way = 0 if s > 0 else 1
                came = rs_rows(part_of(s, 1, ZM))
                net.recv(("rs", h, s, 1), rs_in.at[h, way, 0, came, :])
                qg[came, fs] = total[came, :] + rs_in[h, way, 0, came, :].astype(F32)
    out_send("qg", qg, WR, out_qg, NC, 8)
    out_recv("att", out_att, VC)
    out_recv("kg", out_kg, NC)
    out_recv("vg", out_vg, VC)
    out_recv("qg", out_qg, NC)
    net.finish()


def solution(mesh):
    NX, ctx_size = mesh.shape["heads"], mesh.shape["ctx"]
    NY, NZ = grid_of(ctx_size)
    sizes = (NX, NY, NZ)

    def body(hidden, w_query, key_input, values, cotangent):
        T, DX = hidden.shape
        WR, NALL = w_query.shape
        NC = NALL // CORES
        VC = values.shape[1] // CORES
        D = NX * DX
        CH = CORES * WR
        KY = NZ * CH
        CT = CORES * T
        HEADS = NC // FEAT
        ZM = NZ // 2
        SL = NC // NZ
        any_space = pl.BlockSpec(memory_space=pl.ANY)

        def vmem(*shape, dtype=BF16):
            return pltpu.VMEM(shape, dtype)

        def run(*refs):
            kernel(sizes, *refs)

        return pl.pallas_call(
            run,
            out_shape=(
                jax.ShapeDtypeStruct((T, 2 * VC), BF16),
                jax.ShapeDtypeStruct((WR, NALL), F32),
                jax.ShapeDtypeStruct((T, NALL), BF16),
                jax.ShapeDtypeStruct((T, 2 * VC), BF16),
            ),
            in_specs=[any_space] * 5,
            out_specs=(any_space,) * 4,
            scratch_shapes=[
                vmem(CT, D),
                vmem(D, NC),
                vmem(CT, NC),
                vmem(CT, NC),
                vmem(CT, VC),
                vmem(CT, VC),
                vmem(CT, NC, dtype=F32),
                vmem(CT, NC),
                vmem(CT, VC),
                vmem(CT, VC),
                vmem(HEADS, CT, CT),
                vmem(HEADS, CT, CT),
                vmem(CT, VC, dtype=F32),
                vmem(CT, NC, dtype=F32),
                vmem(CT, NC),
                vmem(CT, VC),
                vmem(2, NC, HEAD_DIM),
                vmem(2, NZ, SL, HEAD_DIM),
                vmem(2, SL, HEAD_DIM),
                vmem(2, NY, SL, HEAD_DIM),
                vmem(2, NC, HEAD_DIM),
                vmem(NC, HEAD_DIM),
                vmem(NC, HEAD_DIM),
                vmem(NC, HEAD_DIM, dtype=F32),
                vmem(NY, CORES, T, KY),
                vmem(KY, NY * CT),
                vmem(HEADS, NY * CT, FEAT),
                vmem(HEADS, KY, FEAT, dtype=F32),
                vmem(HEADS, 2, ZM, CH, FEAT),
                vmem(HEADS, 2, ZM, CH, FEAT),
                vmem(CH, NC, dtype=F32),
                pltpu.SemaphoreType.DMA((CHANNELS,)),
                pltpu.SemaphoreType.DMA((CHANNELS,)),
                pltpu.SemaphoreType.DMA((LOCALS,)),
            ],
            compiler_params=pltpu.CompilerParams(
                collective_id=0, has_side_effects=True, vmem_limit_bytes=60000 * 1024
            ),
        )(hidden, w_query, key_input, values, cotangent)

    spec = P("ctx", "heads")
    return jax.shard_map(
        body, mesh=mesh, in_specs=(spec,) * 5, out_specs=(spec,) * 4, check_vma=False
    )
```

```python
import jax
import jax.numpy as jnp
from jax import lax
from jax.experimental import pallas as pl
from jax.experimental.pallas import tpu as pltpu
from jax.sharding import PartitionSpec as P

HEAD_DIM = 128
FEAT = 256
CORES = 2
EPSILON = 1e-06
MESH = pl.DeviceIdType.MESH
F32 = jnp.float32
BF16 = jnp.bfloat16
GROUPS = 84
LANES = 12
LOCALS = 10


def grid_of(ctx_size):
    if ctx_size == 64:
        return 4, 8
    return 2, ctx_size // (2 * CORES)


def dot_nn(a, b):
    return lax.dot_general(a, b, (((1,), (0,)), ((), ())), preferred_element_type=F32)


def dot_nt(a, b):
    return lax.dot_general(a, b, (((1,), (1,)), ((), ())), preferred_element_type=F32)


def dot_tn(a, b):
    return lax.dot_general(a, b, (((0,), (0,)), ((), ())), preferred_element_type=F32)


class Net:
    def __init__(self, ruler, send_sems, recv_sems):
        self.ruler, self.send_sems, self.recv_sems = ruler, send_sems, recv_sems
        self.groups = {}
        self.lanes = {}
        self.row_bytes = ruler.shape[1] * 2

    def send(self, group, src, dst, device, lane):
        size = 4 if src.dtype == F32 else 2
        for extent in src.shape:
            size *= extent
        group_at = self.groups.setdefault(group, [len(self.groups), 0, False])
        lane_at = self.lanes.setdefault(lane, [len(self.lanes), 0])
        group_at[1] += size
        lane_at[1] += size
        self.device = device
        pltpu.make_async_remote_copy(
            src_ref=src,
            dst_ref=dst,
            send_sem=self.send_sems.at[lane_at[0]],
            recv_sem=self.recv_sems.at[group_at[0]],
            device_id=device,
            device_id_type=MESH,
        ).start()

    def measure(self, size, send_at, recv_at):
        ref = self.ruler.at[pl.ds(0, size // self.row_bytes), :]
        return pltpu.make_async_remote_copy(
            src_ref=ref,
            dst_ref=ref,
            send_sem=self.send_sems.at[send_at],
            recv_sem=self.recv_sems.at[recv_at],
            device_id=self.device,
            device_id_type=MESH,
        )

    def recv(self, group):
        at = self.groups[group]
        assert not at[2]
        at[2] = True
        self.measure(at[1], 0, at[0]).wait_recv()

    def finish(self):
        assert len(self.groups) <= GROUPS and len(self.lanes) <= LANES
        assert all(at[2] for at in self.groups.values())
        for at, size in self.lanes.values():
            self.measure(size, at, 0).wait_send()


def kernel(
    sizes, hidden, w_query, key_input, values, cotangent,
    out_att, out_qg, out_kg, out_vg,
    hf, wf, ki, kf, va, ct, q32, qf, att, dn, sc, mx, vg32, kg32, kg, vg,
    s_out, s_in, t_out, t_in, b_out, prior, later, pre,
    h4, h4t, dq4, g32, rs_out, rs_in, qg,
    send_sems, recv_sems, local_sems,
):
    NX, NY, NZ = sizes
    x = lax.axis_index("heads")
    ctx = lax.axis_index("ctx")
    c = ctx % CORES
    z = (ctx // CORES) % NZ
    y = ctx // (CORES * NZ)
    p = 1 - c
    T, DX = hidden.shape
    WR, NALL = w_query.shape
    NC = NALL // CORES
    VC = values.shape[1] // CORES
    CH = CORES * WR
    KY = NZ * CH
    CT = CORES * T
    HEADS = NC // FEAT
    XM, YM, ZM = NX // 2, NY // 2, NZ // 2

    def dev(dx=0, dy=0, dz=0, core=None):
        nx = (x + dx + NX) % NX
        ny = (y + dy + NY) % NY
        nz = (z + dz + NZ) % NZ
        return (nx, (ny * NZ + nz) * CORES + (c if core is None else core))

    partner = dev(core=p)
    net = Net(wf, send_sems, recv_sems)
    D = NX * DX

    def head(h):
        return slice(h * FEAT, (h + 1) * FEAT), slice(h * HEAD_DIM, (h + 1) * HEAD_DIM)

    own_chunk = (y * NZ + z) * CH
    my_rows = pl.ds(pl.multiple_of(c * T, T), T)
    its_rows = pl.ds(pl.multiple_of(p * T, T), T)
    my_x = pl.ds(pl.multiple_of(x * DX, DX), DX)

    def w_rows(h):
        return pl.ds(pl.multiple_of(h * D + own_chunk + c * WR, WR), WR)

    def cols(core, width):
        return pl.ds(pl.multiple_of(core * width, width), width)

    def w_cols(core, h):
        return pl.ds(pl.multiple_of(core * NC + h * FEAT, FEAT), FEAT)

    moves = [(("w", h), w_query.at[:, w_cols(c, h)], wf.at[w_rows(h), :]) for h in range(HEADS)]
    moves += [
        ("h", hidden, hf.at[my_rows, my_x]),
        ("k", key_input.at[:, cols(c, NC)], ki.at[my_rows, :]),
        ("v", values.at[:, cols(c, VC)], va.at[my_rows, :]),
        ("g", cotangent.at[:, cols(c, VC)], ct.at[my_rows, :]),
    ]

    local = {}
    for at, (name, src, dst) in enumerate(moves):
        local[name] = pltpu.make_async_copy(src, dst, local_sems.at[at])
        local[name].start()

    barrier = pltpu.get_barrier_semaphore()
    friends = [partner]
    friends += [dev(dx=d) for d in sorted({1, NX - 1})]
    friends += [dev(dy=d) for d in range(1, NY)]
    friends += [dev(dz=d) for d in range(1, NZ)]
    for friend in friends:
        pl.semaphore_signal(barrier, inc=1, device_id=friend, device_id_type=MESH)
    pl.semaphore_wait(barrier, len(friends))


    for h in range(HEADS):
        net.send(("w", h), w_query.at[:, w_cols(p, h)], wf.at[w_rows(h), :], partner, "in")
    net.send("h", hidden, hf.at[my_rows, my_x], partner, "in")
    net.send("k", key_input.at[:, cols(p, NC)], ki.at[my_rows, :], partner, "in")
    net.send("v", values.at[:, cols(p, VC)], va.at[my_rows, :], partner, "in")
    net.send("g", cotangent.at[:, cols(p, VC)], ct.at[my_rows, :], partner, "in")

    def split(total, part):
        return {"full": (0, total), "top": (0, total // 2), "bot": (total // 2, total // 2)}[part]

    def part_of(direction, d, most):
        if d < most:
            return "full"
        return "top" if direction > 0 else "bot"

    A_ROWS = CH * 3 // 4
    B_ROWS = CH - A_ROWS

    def w_piece(stream, h, rel_y, rel_z, part):
        start, size = split(A_ROWS if stream == "A" else B_ROWS, part)
        if stream == "B":
            start = start + A_ROWS
        at = h * D + (((y + rel_y + NY) % NY) * NZ + (z + rel_z + NZ) % NZ) * CH + start
        return wf.at[pl.ds(pl.multiple_of(at, 16), size), :]

    BOTH = (1, -1)

    def w_send(group, stream, axis, h, rel, d):
        most = ZM if axis == "z" else YM
        for s in BOTH:
            back = -s * (d - 1)
            rel_y, rel_z = (rel, back) if axis == "z" else (back, rel)
            piece = w_piece(stream, h, rel_y, rel_z, part_of(s, d, most))
            to = dev(dz=s) if axis == "z" else dev(dy=s)
            net.send(group, piece, piece, to, ("w", h))

    def fresh(r, most):
        if r == 0:
            return [0]
        return [-r, r] if r < most else [most]

    def w_round(h, r):
        if r == 0:
            w_send(("Az", h, 1), "A", "z", h, 0, 1)
            w_send(("By", h, 1), "B", "y", h, 0, 1)
            w_send(("Ay", h, 0), "A", "y", h, 0, 1)
            w_send(("Bz", h, 0, 1), "B", "z", h, 0, 1)
            return
        if r <= ZM:
            net.recv(("Az", h, r))
            if r < ZM:
                w_send(("Az", h, r + 1), "A", "z", h, 0, r + 1)
            for rel in fresh(r, ZM):
                w_send(("Ay", h, r), "A", "y", h, rel, 1)
        for start in range(YM + 1):
            d = r - start
            if 1 <= d <= ZM:
                net.recv(("Bz", h, start, d))
                if d < ZM:
                    for rel in fresh(start, YM):
                        w_send(("Bz", h, start, d + 1), "B", "z", h, rel, d + 1)
        if r <= YM:
            net.recv(("By", h, r))
            if r < YM:
                w_send(("By", h, r + 1), "B", "y", h, 0, r + 1)
            for rel in fresh(r, YM):
                w_send(("Bz", h, r, 1), "B", "z", h, rel, 1)
        if r <= ZM + 1:
            net.recv(("Ay", h, r - 1))
            if YM > 1:
                for rel in fresh(r - 1, ZM):
                    w_send(("Ay2", h), "A", "y", h, rel, 2)

    LAST = ZM + YM

    def w_last(h):
        if YM > 1:
            net.recv(("Ay2", h))

    def h_piece(rel_x, part):
        start, size = split(T, part)
        xs = (x + rel_x + NX) % NX
        return hf.at[
            pl.ds(pl.multiple_of(c * T + start, T // 2), size),
            pl.ds(pl.multiple_of(xs * DX, DX), DX),
        ]

    def h_send(d):
        for s in BOTH:
            piece = h_piece(-s * (d - 1), part_of(s, d, XM))
            net.send(("hx", d), piece, piece, dev(dx=s), "h")

    def h_relay(d):
        for rel in fresh(d, XM):
            piece = h_piece(rel, "full")
            net.send(("hp", d), piece, piece, partner, "h")

    SL = s_out.shape[1] // NZ

    def slice_at(k):
        return pl.ds(pl.multiple_of(k * SL, SL), SL)

    def scan_start(kind):
        for o in range(1, NZ):
            src = s_out.at[kind, slice_at((z + o) % NZ), :]
            net.send((kind, "s"), src, s_in.at[kind, o], dev(dz=o), ("scan", kind))

    def scan_totals(kind):
        own = s_out[kind, slice_at(z), :].astype(F32)
        total = own
        net.recv((kind, "s"))
        pre[slice_at(z), :] = own
        for o in range(1, NZ):
            came = s_in[kind, o].astype(F32)
            total = total + came
            pre[slice_at((z - o + NZ) % NZ), :] = came
        t_out[kind] = total.astype(BF16)
        for o in range(1, NY):
            net.send((kind, "t"), t_out.at[kind], t_in.at[kind, o], dev(dy=o), ("scan", kind))

    def scan_back(kind, result):
        offset = jnp.zeros((SL, HEAD_DIM), F32)
        net.recv((kind, "t"))
        for o in range(1, NY):
            source = (y - o + NY) % NY
            counts = source < y if kind == 0 else source > y
            offset = offset + jnp.where(counts, t_in[kind, o].astype(F32), 0.0)
        running = offset
        for k in range(NZ) if kind == 0 else reversed(range(NZ)):
            rows = pl.ds(k * SL, SL)
            b_out[kind, rows, :] = running.astype(BF16)
            running = running + pre[rows, :]
        for o in range(1, NZ):
            src = b_out.at[kind, slice_at((z + o) % NZ), :]
            net.send((kind, "b"), src, result.at[slice_at(z), :], dev(dz=o), ("scan", kind))
        result[slice_at(z), :] = b_out[kind, slice_at(z), :]

    PT = T // NX

    def quarter(rel_x):
        xs = (x + rel_x + NX) % NX
        return pl.ds(pl.multiple_of(xs * PT, PT), PT)

    def h4_source(to):
        return (
            pl.ds(pl.multiple_of(c * T + x * PT, PT), PT),
            pl.ds(pl.multiple_of(to * KY, KY), KY),
        )

    def h4_start():
        for o in range(1, NY):
            src = hf.at[h4_source((y + o) % NY)]
            net.send("h4", src, h4.at[y, c, quarter(0), :], dev(dy=o), "h4")
        h4[y, c, quarter(0), :] = hf[h4_source(y)]

    def h4_piece(rel_x, part):
        start, size = split(NY, part)
        return h4.at[pl.ds(start, size), c, quarter(rel_x), :]

    def h4_send(d):
        for s in BOTH:
            piece = h4_piece(-s * (d - 1), part_of(s, d, XM))
            net.send(("h4x", d), piece, piece, dev(dx=s), "h4")

    def h4_relay(d):
        for rel in fresh(d, XM):
            piece = h4_piece(rel, "full")
            net.send("h4p", piece, piece, partner, "h4")

    def h4_turn():
        net.recv("h4p")
        width = min(KY, 256)
        for k in range(KY // width):
            cut = slice(k * width, (k + 1) * width)
            h4t[cut, :] = h4[:, :, :, cut].reshape(NY * CT, width).T

    def project(h, rel, first=False):
        fs, _ = head(h)
        ys = (y + rel + NY) % NY
        rows = pl.ds(pl.multiple_of(ys * KY, KY), KY)
        w_at = pl.ds(pl.multiple_of(h * D + ys * KY, KY), KY)
        product = dot_nn(hf[:, rows], wf[w_at, :])
        q32[:, fs] = product if first else q32[:, fs] + product

    def project_all(h):
        for k, rel in enumerate(range(NY)):
            project(h, rel, k == 0)

    causal = lax.broadcasted_iota(jnp.int32, (CT, CT), 0) >= lax.broadcasted_iota(
        jnp.int32, (CT, CT), 1
    )

    def attend(h):
        fs, vs = head(h)
        proj = q32[:, fs]
        feats = jnp.maximum(proj, 0.0).astype(BF16)
        qf[:, fs] = feats
        keys, vals, state = kf[:, fs], va[:, vs], prior[fs, :]
        scores = jnp.where(causal, dot_nt(feats, keys), 0.0).astype(BF16)
        sc[h] = scores
        numer = dot_nn(scores, vals) + dot_nn(feats, state)
        inv = lax.rsqrt(jnp.mean(numer * numer, axis=-1, keepdims=True) + EPSILON)
        normed = numer * inv
        att[:, vs] = normed.astype(BF16)
        grad = ct[:, vs].astype(F32)
        d_num = (inv * (grad - normed * jnp.mean(grad * normed, axis=-1, keepdims=True))).astype(BF16)
        dn[:, vs] = d_num
        mixed = jnp.where(causal, dot_nt(d_num, vals), 0.0).astype(BF16)
        mx[h] = mixed
        d_feat = dot_nn(mixed, keys) + dot_nt(d_num, state)
        d_q = jnp.where(proj > 0, d_feat, 0.0).astype(BF16)
        dq4[h, pl.ds(pl.multiple_of(y * CT, CT), CT), :] = d_q
        dq_send(h, 1)

    def attend_rest(h):
        fs, vs = head(h)
        s_out[1, fs, :] = dot_tn(qf[:, fs], dn[:, vs]).astype(BF16)

    def block_parts(h):
        fs, vs = head(h)
        vg32[:, vs] = dot_tn(sc[h], dn[:, vs])
        kg32[:, fs] = dot_tn(mx[h], qf[:, fs])

    def state_parts(h):
        fs, vs = head(h)
        state = later[fs, :]
        vg[:, vs] = (vg32[:, vs] + dot_nn(kf[:, fs], state)).astype(BF16)
        d_key = kg32[:, fs] + dot_nt(va[:, vs], state)
        kg[:, fs] = jnp.where(ki[:, fs] > 0, d_key, 0.0).astype(BF16)

    def dq_send(h, d):
        for s in BOTH:
            start, size = split(CT, part_of(s, d, YM))
            ys = (y - s * (d - 1) + NY) % NY
            piece = dq4.at[h, pl.ds(pl.multiple_of(ys * CT + start, CT // 2), size), :]
            net.send(("dq", h, d), piece, piece, dev(dy=s), ("dq", h))

    def dq_pass(h):
        if YM > 1:
            net.recv(("dq", h, 1))
            dq_send(h, 2)

    def contract(h):
        net.recv(("dq", h, YM))
        g32[h] = dot_nn(h4t[...], dq4[h])

    def rs_rows(part):
        start, size = split(CH, part)
        return slice(start, start + size)

    def rs_send(h, d):
        if d < ZM:
            net.recv(("rs", h, d + 1))
        for s in BOTH:
            part = part_of(s, d, ZM)
            rows = rs_rows(part)
            to = (z + s * d + NZ) % NZ
            size = rows.stop - rows.start
            total = g32[h, pl.ds(pl.multiple_of(to * CH + rows.start, CH // 2), size), :]
            way = 0 if s > 0 else 1
            rs_out[h, way, d - 1, rows, :] = total.astype(BF16)
            if d < ZM:
                came = rs_rows(part_of(s, d + 1, ZM))
                got = rs_in[h, way, d, came, :].astype(F32)
                rs_out[h, way, d - 1, came, :] = (total[came, :] + got).astype(BF16)
            net.send(
                ("rs", h, d),
                rs_out.at[h, way, d - 1, rows, :],
                rs_in.at[h, way, d - 1, rows, :],
                dev(dz=s),
                ("rs", h),
            )

    def rs_last(h):
        fs, _ = head(h)
        net.recv(("rs", h, 1))
        total = g32[h, pl.ds(pl.multiple_of(z * CH, CH), CH), :]
        if ZM > 1:
            qg[:, fs] = total + rs_in[h, 0, 0].astype(F32) + rs_in[h, 1, 0].astype(F32)
        else:
            for way, part in enumerate(("top", "bot")):
                came = rs_rows(part)
                qg[came, fs] = total[came, :] + rs_in[h, way, 0, came, :].astype(F32)

    def out_send(name, buf, rows, out, width, at):
        mine = out.at[:, cols(c, width)]
        keep = buf.at[pl.ds(pl.multiple_of(c * rows, rows), rows), :]
        give = buf.at[pl.ds(pl.multiple_of(p * rows, rows), rows), :]
        net.send(name, give, mine, partner, "out")
        local[name] = pltpu.make_async_copy(keep, mine, local_sems.at[at])
        local[name].start()

    def out_recv(name):
        net.recv(name)
        local[name].wait()

    def states():
        for name in ("k", "v", "g"):
            local[name].wait()
        net.recv("k")
        net.recv("v")
        kf[...] = jnp.maximum(ki[...], jnp.zeros_like(ki[...]))
        for h in range(HEADS):
            fs, vs = head(h)
            s_out[0, fs, :] = dot_tn(kf[:, fs], va[:, vs]).astype(BF16)

    def w_rounds(h, *rounds):
        for r in rounds:
            if r <= LAST:
                w_round(h, r)


    local["w", 0].wait()
    net.recv(("w", 0))
    w_round(0, 0)

    local["h"].wait()
    h_send(1)
    states()
    scan_start(0)
    local["w", 1].wait()
    net.recv(("w", 1))

    w_rounds(0, 1)
    w_rounds(1, 0)

    w_rounds(0, 2)

    net.recv("h")
    net.recv("g")
    if XM > 1:
        net.recv(("hx", 1))
        h_send(2)
        h_relay(1)

    scan_totals(0)

    w_rounds(0, 3)
    w_rounds(1, 1)

    scan_back(0, prior)

    net.recv(("hx", XM))
    h_relay(XM)

    w_rounds(0, 4)
    h4_start()
    w_rounds(1, 2)

    w_rounds(0, 5)
    w_rounds(1, 3)

    net.recv("h4")
    h4_send(1)
    h4_relay(0)

    w_rounds(0, 6)
    for d in range(1, XM + 1):
        net.recv(("hp", d))

    w_last(0)

    project_all(0)

    net.recv((0, "b"))

    attend(0)
    attend_rest(0)

    w_rounds(1, 4)

    if XM > 1:
        net.recv(("h4x", 1))
        h4_send(2)
        h4_relay(1)

    dq_pass(0)

    w_rounds(1, 5)

    net.recv(("h4x", XM))
    h4_relay(XM)

    w_rounds(1, 6)

    h4_turn()

    contract(0)
    rs_send(0, ZM)

    w_last(1)

    project_all(1)

    attend(1)
    attend_rest(1)
    scan_start(1)

    out_send("att", att, T, out_att, VC, 6)
    if ZM > 1:
        rs_send(0, ZM - 1)

    dq_pass(1)

    block_parts(0)
    block_parts(1)

    if ZM > 2:
        rs_send(0, ZM - 2)

    scan_totals(1)

    contract(1)
    rs_send(1, ZM)

    if ZM > 3:
        rs_send(0, ZM - 3)

    scan_back(1, later)

    if ZM > 1:
        rs_send(1, ZM - 1)

    rs_last(0)

    if ZM > 2:
        rs_send(1, ZM - 2)

    net.recv((1, "b"))
    state_parts(0)
    state_parts(1)
    out_send("kg", kg, T, out_kg, NC, 7)
    out_send("vg", vg, T, out_vg, VC, 8)

    if ZM > 3:
        rs_send(1, ZM - 3)

    rs_last(1)

    out_send("qg", qg, WR, out_qg, NC, 9)
    for name in ("att", "kg", "vg", "qg"):
        out_recv(name)
    net.finish()


def solution(mesh):
    NX, ctx_size = mesh.shape["heads"], mesh.shape["ctx"]
    NY, NZ = grid_of(ctx_size)
    sizes = (NX, NY, NZ)

    def body(hidden, w_query, key_input, values, cotangent):
        T, DX = hidden.shape
        WR, NALL = w_query.shape
        NC = NALL // CORES
        VC = values.shape[1] // CORES
        D = NX * DX
        CH = CORES * WR
        KY = NZ * CH
        CT = CORES * T
        HEADS = NC // FEAT
        ZM = NZ // 2
        SL = NC // NZ
        any_space = pl.BlockSpec(memory_space=pl.ANY)

        def vmem(*shape, dtype=BF16):
            return pltpu.VMEM(shape, dtype)

        def run(*refs):
            kernel(sizes, *refs)

        return pl.pallas_call(
            run,
            out_shape=(
                jax.ShapeDtypeStruct((T, 2 * VC), BF16),
                jax.ShapeDtypeStruct((WR, NALL), F32),
                jax.ShapeDtypeStruct((T, NALL), BF16),
                jax.ShapeDtypeStruct((T, 2 * VC), BF16),
            ),
            in_specs=[any_space] * 5,
            out_specs=(any_space,) * 4,
            scratch_shapes=[
                vmem(CT, D),
                vmem(HEADS * D, FEAT),
                vmem(CT, NC),
                vmem(CT, NC),
                vmem(CT, VC),
                vmem(CT, VC),
                vmem(CT, NC, dtype=F32),
                vmem(CT, NC),
                vmem(CT, VC),
                vmem(CT, VC),
                vmem(HEADS, CT, CT),
                vmem(HEADS, CT, CT),
                vmem(CT, VC, dtype=F32),
                vmem(CT, NC, dtype=F32),
                vmem(CT, NC),
                vmem(CT, VC),
                vmem(2, NC, HEAD_DIM),
                vmem(2, NZ, SL, HEAD_DIM),
                vmem(2, SL, HEAD_DIM),
                vmem(2, NY, SL, HEAD_DIM),
                vmem(2, NC, HEAD_DIM),
                vmem(NC, HEAD_DIM),
                vmem(NC, HEAD_DIM),
                vmem(NC, HEAD_DIM, dtype=F32),
                vmem(NY, CORES, T, KY),
                vmem(KY, NY * CT),
                vmem(HEADS, NY * CT, FEAT),
                vmem(HEADS, KY, FEAT, dtype=F32),
                vmem(HEADS, 2, ZM, CH, FEAT),
                vmem(HEADS, 2, ZM, CH, FEAT),
                vmem(CH, NC, dtype=F32),
                pltpu.SemaphoreType.DMA((LANES,)),
                pltpu.SemaphoreType.DMA((GROUPS,)),
                pltpu.SemaphoreType.DMA((LOCALS,)),
            ],
            compiler_params=pltpu.CompilerParams(
                collective_id=0, has_side_effects=True, vmem_limit_bytes=60000 * 1024
            ),
        )(hidden, w_query, key_input, values, cotangent)

    spec = P("ctx", "heads")
    return jax.shard_map(
        body, mesh=mesh, in_specs=(spec,) * 5, out_specs=(spec,) * 4, check_vma=False
    )
```

```python
import jax
import jax.numpy as jnp
from jax import lax
from jax.experimental import pallas as pl
from jax.experimental.pallas import tpu as pltpu
from jax.sharding import PartitionSpec as P

HEAD_DIM = 128
FEAT = 256
CORES = 2
EPSILON = 1e-06
MESH = pl.DeviceIdType.MESH
F32 = jnp.float32
BF16 = jnp.bfloat16
GROUPS = 70
LANES = 13
LOCALS = 11
A_EIGHTHS = 5


def dot_nn(a, b):
    return lax.dot_general(a, b, (((1,), (0,)), ((), ())), preferred_element_type=F32)


def dot_nt(a, b):
    return lax.dot_general(a, b, (((1,), (1,)), ((), ())), preferred_element_type=F32)


def dot_tn(a, b):
    return lax.dot_general(a, b, (((0,), (0,)), ((), ())), preferred_element_type=F32)


class Net:
    def __init__(self, ruler, send_sems, recv_sems):
        self.ruler, self.send_sems, self.recv_sems = ruler, send_sems, recv_sems
        self.groups = {}
        self.lanes = {}
        self.row_bytes = ruler.shape[1] * 2

    def send(self, group, src, dst, device, lane):
        size = 4 if src.dtype == F32 else 2
        for extent in src.shape:
            size *= extent
        group_at = self.groups.setdefault(group, [len(self.groups), 0, False])
        lane_at = self.lanes.setdefault(lane, [len(self.lanes), 0])
        group_at[1] += size
        lane_at[1] += size
        self.device = device
        pltpu.make_async_remote_copy(
            src_ref=src,
            dst_ref=dst,
            send_sem=self.send_sems.at[lane_at[0]],
            recv_sem=self.recv_sems.at[group_at[0]],
            device_id=device,
            device_id_type=MESH,
        ).start()

    def measure(self, size, send_at, recv_at):
        ref = self.ruler.at[pl.ds(0, size // self.row_bytes), :]
        return pltpu.make_async_remote_copy(
            src_ref=ref,
            dst_ref=ref,
            send_sem=self.send_sems.at[send_at],
            recv_sem=self.recv_sems.at[recv_at],
            device_id=self.device,
            device_id_type=MESH,
        )

    def recv(self, group):
        at = self.groups[group]
        assert not at[2]
        at[2] = True
        self.measure(at[1], 0, at[0]).wait_recv()

    def finish(self):
        assert len(self.groups) <= GROUPS and len(self.lanes) <= LANES
        assert all(at[2] for at in self.groups.values())
        for at, size in self.lanes.values():
            self.measure(size, at, 0).wait_send()


def kernel(
    sizes, hidden, w_query, key_input, values, cotangent,
    out_att, out_qg, out_kg, out_vg,
    hf, wf, kb, kf, vb, gb, q32, qf, att, dn, sc, mx, vg32, kg32, kg, vg,
    s_out, s_in, t_out, t_in, b_out, prior, later, pre,
    h4, h4t, dq4, g32, rs_out, rs_in, qg,
    send_sems, recv_sems, local_sems,
):
    NX, NY, NZ = sizes
    x = lax.axis_index("heads")
    ctx = lax.axis_index("ctx")
    c = ctx % CORES
    z = (ctx // CORES) % NZ
    y = ctx // (CORES * NZ)
    p = 1 - c
    u = y % 2
    pair = y // 2
    py = y + 1 - 2 * u
    qy = NY - 1 - y
    ry = NY - 1 - py
    own_y = (y, py, qy, ry)
    e = ((y + 1) // 2) % 2
    T, DX = hidden.shape
    WR, NALL = w_query.shape
    D = NX * DX
    CH = CORES * WR
    KY = NZ * CH
    KH = 2 * KY
    CT = CORES * T
    XM, ZM = NX // 2, NZ // 2
    BOTH = (1, -1)
    BLOCKS = (0, 1)

    def at(y_, z_, core):
        return (x, (y_ * NZ + z_) * CORES + core)

    def dev_x(step):
        return ((x + step + NX) % NX, ctx)

    def dev_z(step):
        return at(y, (z + step + NZ) % NZ, c)

    partner = at(y, z, p)
    pair_same = at(py, z, c)
    pair_other = at(py, z, p)
    across = at(qy, z, c)
    net = Net(wf, send_sems, recv_sems)

    def rows_of(start, size, unit=16):
        return pl.ds(pl.multiple_of(start, unit), size)

    def head_cols(core, parity, width):
        return pl.ds(pl.multiple_of((2 * core + parity) * width, width), width)

    def split(total, part):
        top = (total // 2 + 15) // 16 * 16
        return {"full": (0, total), "top": (0, top), "bot": (top, total - top)}[part]

    def part_of(direction, d, most):
        if d < most:
            return "full"
        return "top" if direction > 0 else "bot"

    def fresh(r, most):
        if r == 0:
            return [0]
        return [-r, r] if r < most else [most]

    w_mine = rows_of((y * NZ + z) * CH + c * WR, WR)
    t_mine = rows_of(c * T, T)
    x_mine = pl.ds(pl.multiple_of(x * DX, DX), DX)
    moves = [
        ("w", w_query.at[:, head_cols(c, e, FEAT)], wf.at[w_mine, :]),
        ("h", hidden, hf.at[t_mine, x_mine]),
        ("k0", key_input.at[:, head_cols(c, e, FEAT)], kb.at[0, t_mine, :]),
        ("k2", key_input.at[:, head_cols(c, 1 - e, FEAT)], kb.at[2, t_mine, :]),
        ("v0", values.at[:, head_cols(c, e, HEAD_DIM)], vb.at[0, t_mine, :]),
        ("v2", values.at[:, head_cols(c, 1 - e, HEAD_DIM)], vb.at[2, t_mine, :]),
        ("g", cotangent.at[:, head_cols(c, e, HEAD_DIM)], gb.at[0, t_mine, :]),
    ]

    local = {}
    for n, (name, src, dst) in enumerate(moves):
        local[name] = pltpu.make_async_copy(src, dst, local_sems.at[n])
        local[name].start()

    barrier = pltpu.get_barrier_semaphore()
    friends = [partner, pair_same, pair_other, across, at(ry, z, c)]
    friends += [dev_x(d) for d in sorted({1, NX - 1})]
    friends += [dev_z(d) for d in range(1, NZ)]
    for friend in friends:
        pl.semaphore_signal(barrier, inc=1, device_id=friend, device_id_type=MESH)
    pl.semaphore_wait(barrier, len(friends))

    pair_cores = ((c, pair_same), (p, pair_other))
    for core, to in pair_cores:
        net.send("w1", w_query.at[:, head_cols(core, 1 - e, FEAT)], wf.at[w_mine, :], to, "in")
    net.send("w0", w_query.at[:, head_cols(p, e, FEAT)], wf.at[w_mine, :], partner, "in")
    net.send("h1", hidden, hf.at[rows_of(CT + c * T, T), x_mine], pair_same, "in")
    for slot, parity in ((0, e), (2, 1 - e)):
        net.send(
            "kv0", key_input.at[:, head_cols(p, parity, FEAT)], kb.at[slot, t_mine, :], partner, "in"
        )
        net.send(
            "kv0", values.at[:, head_cols(p, parity, HEAD_DIM)], vb.at[slot, t_mine, :], partner, "in"
        )
    net.send("h0", hidden, hf.at[t_mine, x_mine], partner, "in")
    for core, to in pair_cores:
        cut, narrow = head_cols(core, 1 - e, FEAT), head_cols(core, 1 - e, HEAD_DIM)
        net.send("kv1", key_input.at[:, cut], kb.at[1, t_mine, :], to, "in")
        net.send("kv1", values.at[:, narrow], vb.at[1, t_mine, :], to, "in")
        net.send("kv1", cotangent.at[:, narrow], gb.at[1, t_mine, :], to, "in")
    net.send("g0", cotangent.at[:, head_cols(p, e, HEAD_DIM)], gb.at[0, t_mine, :], partner, "in")


    A_ROWS = CH * A_EIGHTHS // 8
    B_ROWS = CH - A_ROWS

    def w_piece(stream, which, rel_z, part):
        start, size = split(A_ROWS if stream == "A" else B_ROWS, part)
        if stream == "B":
            start = start + A_ROWS
        return wf.at[rows_of((own_y[which] * NZ + (z + rel_z + NZ) % NZ) * CH + start, size), :]

    def w_ring(stream, which, d):
        for s in BOTH:
            piece = w_piece(stream, which, -s * (d - 1), part_of(s, d, ZM))
            net.send((stream, which, d), piece, piece, dev_z(s), ("w", which % 2))

    def w_across(stream, b, rel):
        piece = w_piece(stream, b, rel, "full")
        net.send((stream, "across", b), piece, piece, across, ("w", b))

    def w_next(stream, which, d):
        if 1 <= d <= ZM:
            net.recv((stream, which, d))
            if d < ZM:
                w_ring(stream, which, d + 1)

    def w_round(b, r):
        if r == 0:
            w_ring("A", b, 1)
            w_across("B", b, 0)
            w_across("A", b, 0)
            w_ring("B", b, 1)
            return
        w_next("A", b, r)
        if r <= ZM:
            for rel in fresh(r, ZM):
                w_across("A", b, rel)
        if r == 1:
            net.recv(("B", "across", b))
            w_ring("B", 2 + b, 1)
        w_next("B", b, r)
        w_next("B", 2 + b, r - 1)

    def w_rounds(*pairs):
        for b, r in pairs:
            if r <= ZM + 1:
                w_round(b, r)

    def h_piece(b, rel_x, part):
        start, size = split(T, part)
        xs = (x + rel_x + NX) % NX
        return hf.at[
            rows_of(b * CT + c * T + start, size), pl.ds(pl.multiple_of(xs * DX, DX), DX)
        ]

    def h_send(b, d):
        for s in BOTH:
            piece = h_piece(b, -s * (d - 1), part_of(s, d, XM))
            net.send(("hx", b, d), piece, piece, dev_x(s), ("h", b))

    def h_relay(b, d):
        for rel in fresh(d, XM):
            piece = h_piece(b, rel, "full")
            net.send(("hp", b), piece, piece, partner, ("h", b))

    def h_step(b, d):
        if d <= XM:
            net.recv(("hx", b, d))
            if d < XM:
                h_send(b, d + 1)
            h_relay(b, d)

    SR = FEAT // NZ

    def slice_at(k):
        return pl.ds(pl.multiple_of(k * SR, SR), SR)

    def scan_start(kind):
        for o in range(1, NZ):
            src = s_out.at[kind, :, slice_at((z + o) % NZ), :]
            net.send((kind, "s"), src, s_in.at[kind, o], dev_z(o), ("scan", kind))

    def scan_totals(kind):
        own = s_out[kind, :, slice_at(z), :].astype(F32)
        total = own
        net.recv((kind, "s"))
        pre[z] = own
        for o in range(1, NZ):
            came = s_in[kind, o].astype(F32)
            total = total + came
            pre[(z - o + NZ) % NZ] = came
        t_out[kind] = total.astype(BF16)
        if kind == 0:
            for n, to in ((1, pair_same), (2, across), (3, at(ry, z, c))):
                net.send((kind, "t"), t_out.at[kind], t_in.at[kind, n], to, ("scan", kind))
        else:
            net.send((kind, "t"), t_out.at[kind], t_in.at[kind, 2], across, ("scan", kind))

    def scan_back(kind, result):
        net.recv((kind, "t"))
        zero = jnp.zeros((SR, HEAD_DIM), F32)
        if kind == 0:
            offset = [zero, zero]
            for n in (1, 2, 3):
                for half in (0, 1):
                    term = t_in[0, n, half].astype(F32)
                    offset[half] = offset[half] + jnp.where(own_y[n] < y, term, 0.0)
        else:
            sums = (
                t_out[1, 0].astype(F32),
                t_out[1, 1].astype(F32),
                t_in[1, 2, 0].astype(F32),
                t_in[1, 2, 1].astype(F32),
            )
            offset = []
            for b in BLOCKS:
                total = zero
                for n in range(4):
                    if n != b:
                        total = total + jnp.where(own_y[n] > own_y[b], sums[n], 0.0)
                offset.append(total)
        for half in (0, 1):
            running = offset[half]
            for k in range(NZ) if kind == 0 else reversed(range(NZ)):
                b_out[kind, k, half] = running.astype(BF16)
                running = running + pre[k, half]
        for o in range(1, NZ):
            src = b_out.at[kind, (z + o) % NZ]
            dst = result.at[pl.ds(0, 2), slice_at(z), :]
            net.send((kind, "b"), src, dst, dev_z(o), ("scan", kind))
        result[pl.ds(0, 2), slice_at(z), :] = b_out[kind, z]

    PT = T // NX

    def quarter(rel_x):
        xs = (x + rel_x + NX) % NX
        return pl.ds(pl.multiple_of(xs * PT, PT), PT)

    def h4_start():
        src = hf.at[
            rows_of(c * T + x * PT, PT), pl.ds(pl.multiple_of((1 - pair) * KH, KH), KH)
        ]
        net.send(("h4", 0), src, h4.at[0, c, quarter(0), :], across, "h4")

    def h4_ring(j, d):
        for s in BOTH:
            start, size = {"full": (0, KH), "top": (0, KH // 2), "bot": (KH // 2, KH // 2)}[
                part_of(s, d, XM)
            ]
            piece = h4.at[j, c, quarter(-s * (d - 1)), pl.ds(start, size)]
            net.send(("h4x", j, d), piece, piece, dev_x(s), "h4")

    def h4_relay(j, d):
        for rel in fresh(d, XM):
            piece = h4.at[j, c, quarter(rel), :]
            net.send(("h4p", j), piece, piece, partner, "h4")

    def h4_first(j):
        net.recv(("h4", j))
        h4_ring(j, 1)
        if j == 0:
            net.send(
                ("h4", 1), h4.at[0, c, quarter(0), :], h4.at[1, c, quarter(0), :], pair_same, "h4"
            )
        h4_relay(j, 0)

    def h4_step(j, d):
        if d <= XM:
            net.recv(("h4x", j, d))
            if d < XM:
                h4_ring(j, d + 1)
            h4_relay(j, d)

    WIDE = 256

    def h4_turn_own():
        for k in range(KH // WIDE):
            cols = pl.ds(pl.multiple_of(pair * KH + k * WIDE, WIDE), WIDE)
            h4t[k * WIDE : (k + 1) * WIDE, 0 : 2 * CT] = hf[:, cols].T

    def h4_turn(j):
        net.recv(("h4p", j))
        for k in range(KH // WIDE):
            cut = slice(k * WIDE, (k + 1) * WIDE)
            h4t[cut, (2 + j) * CT : (3 + j) * CT] = h4[j, :, :, cut].reshape(CT, WIDE).T

    def project():
        q32[...] = dot_nn(hf[...], wf[...])

    causal = lax.broadcasted_iota(jnp.int32, (CT, CT), 0) >= lax.broadcasted_iota(
        jnp.int32, (CT, CT), 1
    )

    def attend(b):
        proj = q32[b * CT : (b + 1) * CT, :]
        feats = jnp.maximum(proj, 0.0).astype(BF16)
        qf[b] = feats
        keys, vals = kf[b], vb[b]
        state = prior[e] if b == 0 else prior[2]
        scores = jnp.where(causal, dot_nt(feats, keys), 0.0).astype(BF16)
        sc[b] = scores
        numer = dot_nn(scores, vals) + dot_nn(feats, state)
        inv = lax.rsqrt(jnp.mean(numer * numer, axis=-1, keepdims=True) + EPSILON)
        normed = numer * inv
        att[b] = normed.astype(BF16)
        grad = gb[b].astype(F32)
        d_num = (inv * (grad - normed * jnp.mean(grad * normed, axis=-1, keepdims=True))).astype(BF16)
        dn[b] = d_num
        mixed = jnp.where(causal, dot_nt(d_num, vals), 0.0).astype(BF16)
        mx[b] = mixed
        d_feat = dot_nn(mixed, keys) + dot_nt(d_num, state)
        d_q = jnp.where(proj > 0, d_feat, 0.0).astype(BF16)
        mine = slice(b * CT, (b + 1) * CT)
        dq4[mine, :] = d_q
        net.send(("dq", b), dq4.at[mine, :], dq4.at[(2 + b) * CT : (3 + b) * CT, :], across, "dq")

    def attend_rest(b):
        s_out[1, b] = dot_tn(qf[b], dn[b]).astype(BF16)

    def block_parts(b):
        vg32[b] = dot_tn(sc[b], dn[b])
        kg32[b] = dot_tn(mx[b], qf[b])

    def state_parts(b):
        state = later[b]
        vg[b] = (vg32[b] + dot_nn(kf[b], state)).astype(BF16)
        d_key = kg32[b] + dot_nt(vb[b], state)
        kg[b] = jnp.where(kb[b] > 0, d_key, 0.0).astype(BF16)

    def contract_own(k):
        g32[k] = dot_nn(h4t[k * KY : (k + 1) * KY, 0 : 2 * CT], dq4[0 : 2 * CT, :])

    def contract_rest(k):
        rest = slice(2 * CT, 4 * CT)
        g32[k] = g32[k] + dot_nn(h4t[k * KY : (k + 1) * KY, rest], dq4[rest, :])

    def rs_rows(part):
        start, size = split(CH, part)
        return slice(start, start + size)

    def rs_send(k, d):
        if not 1 <= d <= ZM:
            return
        if d < ZM:
            net.recv(("rs", k, d + 1))
        for s in BOTH:
            rows = rs_rows(part_of(s, d, ZM))
            size = rows.stop - rows.start
            to = (z + s * d + NZ) % NZ
            total = g32[k, rows_of(to * CH + rows.start, size), :]
            way = 0 if s > 0 else 1
            rs_out[k, way, d - 1, rows, :] = total.astype(BF16)
            if d < ZM:
                came = rs_rows(part_of(s, d + 1, ZM))
                got = rs_in[k, way, d, came, :].astype(F32)
                rs_out[k, way, d - 1, came, :] = (total[came, :] + got).astype(BF16)
            net.send(
                ("rs", k, d),
                rs_out.at[k, way, d - 1, rows, :],
                rs_in.at[k, way, d - 1, rows, :],
                dev_z(s),
                ("rs", k),
            )

    def rs_last(k):
        net.recv(("rs", k, 1))
        total = g32[k, rows_of(z * CH, CH), :]
        if ZM > 1:
            qg[k] = total + rs_in[k, 0, 0].astype(F32) + rs_in[k, 1, 0].astype(F32)
        else:
            for way, part in enumerate(("top", "bot")):
                came = rs_rows(part)
                qg[k, came, :] = total[came, :] + rs_in[k, way, 0, came, :].astype(F32)

    def out_send(name, buf, out, rows, width, n, first):
        mine = out.at[:, head_cols(c, e, width)]

        def piece(block, core):
            return buf.at[block, rows_of(core * rows, rows), :]

        net.send(name, piece(first, p), mine, partner, "out")
        net.send(name, piece(1 - first, c), mine, pair_same, "out")
        net.send(name, piece(1 - first, p), mine, pair_other, "out")
        local[name] = pltpu.make_async_copy(piece(first, c), mine, local_sems.at[n])
        local[name].start()

    def out_recv(name):
        net.recv(name)
        local[name].wait()


    local["w"].wait()
    net.recv("w0")
    w_rounds((0, 0))

    local["h"].wait()
    h_send(0, 1)

    for name in ("k0", "k2", "v0", "v2"):
        local[name].wait()
    net.recv("kv0")
    kf[0] = jnp.maximum(kb[0], jnp.zeros_like(kb[0]))
    s_out[0, e] = dot_tn(kf[0], vb[0]).astype(BF16)
    s_out[0, 1 - e] = dot_tn(jnp.maximum(kb[2], jnp.zeros_like(kb[2])), vb[2]).astype(BF16)
    scan_start(0)

    net.recv("w1")
    w_rounds((1, 0))

    w_rounds((0, 1))

    h_step(0, 1)

    w_rounds((1, 1))

    scan_totals(0)

    net.recv("h1")
    h_send(1, 1)
    h_relay(1, 0)

    w_rounds((0, 2), (1, 2))

    scan_back(0, prior)

    h_step(0, 2)

    h4_start()

    w_rounds((0, 3), (1, 3))

    h_step(1, 1)

    net.recv((0, "b"))
    net.send("prior", prior.at[1 - e], prior.at[2], pair_same, "prior")

    w_rounds((0, 4), (1, 4))

    h4_first(0)

    w_rounds((0, 5), (1, 5))

    h_step(1, 2)

    h4_first(1)

    net.recv("kv1")
    kf[1] = jnp.maximum(kb[1], jnp.zeros_like(kb[1]))
    local["g"].wait()
    net.recv("g0")
    net.recv("h0")

    net.recv(("hp", 0))

    net.recv(("A", "across", 0))
    net.recv(("A", "across", 1))

    net.recv(("hp", 1))

    project()

    net.recv("prior")

    attend(0)

    attend(1)

    attend_rest(0)
    attend_rest(1)
    scan_start(1)

    h4_step(0, 1)

    h4_turn_own()

    contract_own(0)
    contract_own(1)

    h4_step(1, 1)
    h4_step(0, 2)

    out_send("att", att, out_att, T, HEAD_DIM, 7, 0)
    block_parts(0)
    block_parts(1)

    scan_totals(1)

    h4_step(1, 2)

    h4_turn(0)

    h4_turn(1)

    net.recv(("dq", 0))
    net.recv(("dq", 1))

    for k in BLOCKS:
        contract_rest(k)
        rs_send(k, ZM)

    scan_back(1, later)

    for k in BLOCKS:
        rs_send(k, ZM - 1)

    net.recv((1, "b"))
    state_parts(0)
    state_parts(1)
    out_send("kg", kg, out_kg, T, FEAT, 8, 0)
    out_send("vg", vg, out_vg, T, HEAD_DIM, 9, 0)

    for k in BLOCKS:
        rs_send(k, ZM - 2)

    for k in BLOCKS:
        rs_send(k, ZM - 3)

    for k in BLOCKS:
        rs_last(k)

    out_send("qg", qg, out_qg, WR, FEAT, 10, u)
    for name in ("att", "kg", "vg", "qg"):
        out_recv(name)
    net.finish()


def solution(mesh):
    NX, ctx_size = mesh.shape["heads"], mesh.shape["ctx"]
    NY = 4
    NZ = ctx_size // (NY * CORES)
    sizes = (NX, NY, NZ)

    def body(hidden, w_query, key_input, values, cotangent):
        T, DX = hidden.shape
        WR, NALL = w_query.shape
        VALL = values.shape[1]
        D = NX * DX
        CH = CORES * WR
        KY = NZ * CH
        CT = CORES * T
        ZM = NZ // 2
        SR = FEAT // NZ
        any_space = pl.BlockSpec(memory_space=pl.ANY)

        def vmem(*shape, dtype=BF16):
            return pltpu.VMEM(shape, dtype)

        def run(*refs):
            kernel(sizes, *refs)

        return pl.pallas_call(
            run,
            out_shape=(
                jax.ShapeDtypeStruct((T, VALL), BF16),
                jax.ShapeDtypeStruct((WR, NALL), F32),
                jax.ShapeDtypeStruct((T, NALL), BF16),
                jax.ShapeDtypeStruct((T, VALL), BF16),
            ),
            in_specs=[any_space] * 5,
            out_specs=(any_space,) * 4,
            scratch_shapes=[
                vmem(2 * CT, D),
                vmem(D, FEAT),
                vmem(3, CT, FEAT),
                vmem(2, CT, FEAT),
                vmem(3, CT, HEAD_DIM),
                vmem(2, CT, HEAD_DIM),
                vmem(2 * CT, FEAT, dtype=F32),
                vmem(2, CT, FEAT),
                vmem(2, CT, HEAD_DIM),
                vmem(2, CT, HEAD_DIM),
                vmem(2, CT, CT),
                vmem(2, CT, CT),
                vmem(2, CT, HEAD_DIM, dtype=F32),
                vmem(2, CT, FEAT, dtype=F32),
                vmem(2, CT, FEAT),
                vmem(2, CT, HEAD_DIM),
                vmem(2, 2, FEAT, HEAD_DIM),
                vmem(2, NZ, 2, SR, HEAD_DIM),
                vmem(2, 2, SR, HEAD_DIM),
                vmem(2, NY, 2, SR, HEAD_DIM),
                vmem(2, NZ, 2, SR, HEAD_DIM),
                vmem(3, FEAT, HEAD_DIM),
                vmem(2, FEAT, HEAD_DIM),
                vmem(NZ, 2, SR, HEAD_DIM, dtype=F32),
                vmem(2, CORES, T, 2 * KY),
                vmem(2 * KY, 4 * CT),
                vmem(4 * CT, FEAT),
                vmem(2, KY, FEAT, dtype=F32),
                vmem(2, 2, ZM, CH, FEAT),
                vmem(2, 2, ZM, CH, FEAT),
                vmem(2, CH, FEAT, dtype=F32),
                pltpu.SemaphoreType.DMA((LANES,)),
                pltpu.SemaphoreType.DMA((GROUPS,)),
                pltpu.SemaphoreType.DMA((LOCALS,)),
            ],
            compiler_params=pltpu.CompilerParams(
                collective_id=0, has_side_effects=True, vmem_limit_bytes=60000 * 1024
            ),
        )(hidden, w_query, key_input, values, cotangent)

    spec = P("ctx", "heads")
    return jax.shard_map(
        body, mesh=mesh, in_specs=(spec,) * 5, out_specs=(spec,) * 4, check_vma=False
    )
```

```python
import jax
import jax.numpy as jnp
from jax import lax
from jax.experimental import pallas as pl
from jax.experimental.pallas import tpu as pltpu
from jax.sharding import PartitionSpec as P

HEAD_DIM = 128
FEAT = 256
CORES = 2
EPSILON = 1e-06
MESH = pl.DeviceIdType.MESH
F32 = jnp.float32
BF16 = jnp.bfloat16
GROUPS = 82
LANES = 13
LOCALS = 12
A_EIGHTHS = 5

ORDER = (
    ('h', 0),
    ('w', 0),
    ('state',),
    ('g0',),
    ('w', 1),
    ('across', 0),
    ('A', 0, 1),
    ('B', 0, 1),
    ('hx', 0, 1),
    ('across', 1),
    ('hx', 0, 2),
    ('A', 1, 1),
    ('h', 1),
    ('B', 1, 1),
    ('B', 2, 1),
    ('tot', 0),
    ('A', 0, 2),
    ('hx', 0, 3),
    ('B', 0, 2),
    ('h4s',),
    ('B', 3, 1),
    ('A', 1, 2),
    ('hp', 0),
    ('B', 1, 2),
    ('B', 2, 2),
    ('hx', 1, 1),
    ('kv1',),
    ('A', 0, 3),
    ('back', 0),
    ('B', 0, 3),
    ('B', 3, 2),
    ('A', 1, 3),
    ('hx', 1, 2),
    ('B', 1, 3),
    ('B', 2, 3),
    ('h4', 0),
    ('A', 0, 4),
    ('hx', 1, 3),
    ('h4x', 0, 1),
    ('hp', 1),
    ('turnown',),
    ('B', 0, 4),
    ('h4', 1),
    ('B', 3, 3),
    ('h4x', 0, 2),
    ('A', 1, 4),
    ('B', 1, 4),
    ('mm', 0, 0),
    ('B', 2, 4),
    ('prior',),
    ('last', 0),
    ('mm', 1, 0),
    ('B', 3, 4),
    ('h4x', 0, 3),
    ('last', 1),
    ('h4x', 1, 1),
    ('mm', 0, 1),
    ('att', 0),
    ('s1', 0),
    ('h4x', 1, 2),
    ('mm', 1, 1),
    ('att', 1),
    ('s1', 1),
    ('h4x', 1, 3),
    ('own', 0),
    ('own', 1),
    ('turn', 0),
    ('turn', 1),
    ('outatt',),
    ('blk', 0),
    ('blk', 1),
    ('rest', 0),
    ('tot', 1),
    ('rest', 1),
    ('rs', 0, 0, 3),
    ('back', 1),
    ('rs', 0, 1, 3),
    ('rs', 1, 0, 3),
    ('rs', 1, 1, 3),
    ('rs', 0, 0, 2),
    ('rs', 0, 1, 2),
    ('rs', 1, 0, 2),
    ('rs', 1, 1, 2),
    ('later',),
    ('rs', 0, 0, 1),
    ('rs', 0, 1, 1),
    ('rs', 1, 0, 1),
    ('rs', 1, 1, 1),
    ('rsl', 0, 0),
    ('rsl', 0, 1),
    ('rsl', 1, 0),
    ('rsl', 1, 1),
)


def dot_nn(a, b):
    return lax.dot_general(a, b, (((1,), (0,)), ((), ())), preferred_element_type=F32)


def dot_nt(a, b):
    return lax.dot_general(a, b, (((1,), (1,)), ((), ())), preferred_element_type=F32)


def dot_tn(a, b):
    return lax.dot_general(a, b, (((0,), (0,)), ((), ())), preferred_element_type=F32)


class Net:
    def __init__(self, ruler, send_sems, recv_sems):
        self.ruler, self.send_sems, self.recv_sems = ruler, send_sems, recv_sems
        self.groups = {}
        self.lanes = {}
        self.row_bytes = ruler.shape[1] * 2

    def send(self, group, src, dst, device, lane):
        size = 4 if src.dtype == F32 else 2
        for extent in src.shape:
            size *= extent
        group_at = self.groups.setdefault(group, [len(self.groups), 0, False])
        lane_at = self.lanes.setdefault(lane, [len(self.lanes), 0])
        group_at[1] += size
        lane_at[1] += size
        self.device = device
        pltpu.make_async_remote_copy(
            src_ref=src,
            dst_ref=dst,
            send_sem=self.send_sems.at[lane_at[0]],
            recv_sem=self.recv_sems.at[group_at[0]],
            device_id=device,
            device_id_type=MESH,
        ).start()

    def measure(self, size, send_at, recv_at):
        ref = self.ruler.at[pl.ds(0, size // self.row_bytes), :]
        return pltpu.make_async_remote_copy(
            src_ref=ref,
            dst_ref=ref,
            send_sem=self.send_sems.at[send_at],
            recv_sem=self.recv_sems.at[recv_at],
            device_id=self.device,
            device_id_type=MESH,
        )

    def recv(self, group):
        at = self.groups[group]
        assert not at[2]
        at[2] = True
        self.measure(at[1], 0, at[0]).wait_recv()

    def finish(self):
        assert len(self.groups) <= GROUPS and len(self.lanes) <= LANES
        assert all(at[2] for at in self.groups.values())
        for at, size in self.lanes.values():
            self.measure(size, at, 0).wait_send()


def kernel(
    sizes, hidden, w_query, key_input, values, cotangent,
    out_att, out_qg, out_kg, out_vg,
    hf, wf, kb, kf, vb, gb, q32, qf, att, dn, sc, mx, vg32, kg32, kg, vg,
    s_out, s_in, t_out, t_in, b_out, prior, later, pre,
    h4, h4t, dq4, g32, rs_out, rs_in, qg,
    send_sems, recv_sems, local_sems,
):
    NX, NY, NZ = sizes
    x = lax.axis_index("heads")
    ctx = lax.axis_index("ctx")
    c = ctx % CORES
    z = (ctx // CORES) % NZ
    y = ctx // (CORES * NZ)
    p = 1 - c
    u = y % 2
    pair = y // 2
    py = y + 1 - 2 * u
    qy = NY - 1 - y
    ry = NY - 1 - py
    own_y = (y, py, qy, ry)
    e = ((y + 1) // 2) % 2
    T, DX = hidden.shape
    WR, NALL = w_query.shape
    D = NX * DX
    CH = CORES * WR
    KY = NZ * CH
    KH = 2 * KY
    CT = CORES * T
    XM, ZM = NX // 2, NZ // 2
    BOTH = (1, -1)
    BLOCKS = (0, 1)

    def at(y_, z_, core):
        return (x, (y_ * NZ + z_) * CORES + core)

    def dev_x(step):
        return ((x + step + NX) % NX, ctx)

    def dev_z(step):
        return at(y, (z + step + NZ) % NZ, c)

    partner = at(y, z, p)
    pair_same = at(py, z, c)
    pair_other = at(py, z, p)
    across = at(qy, z, c)
    net = Net(wf, send_sems, recv_sems)

    def rows_of(start, size, unit=16):
        return pl.ds(pl.multiple_of(start, unit), size)

    def head_cols(core, parity, width):
        return pl.ds(pl.multiple_of((2 * core + parity) * width, width), width)

    def split(total, part):
        top = (total // 2 + 15) // 16 * 16
        return {"full": (0, total), "top": (0, top), "bot": (top, total - top)}[part]

    def part_of(direction, d, most):
        if d < most:
            return "full"
        return "top" if direction > 0 else "bot"

    def fresh(r, most):
        if r == 0:
            return [0]
        return [-r, r] if r < most else [most]

    w_mine = rows_of((y * NZ + z) * CH + c * WR, WR)
    t_mine = rows_of(c * T, T)
    x_mine = pl.ds(pl.multiple_of(x * DX, DX), DX)
    moves = [
        ("w", w_query.at[:, head_cols(c, e, FEAT)], wf.at[w_mine, :]),
        ("h", hidden, hf.at[t_mine, x_mine]),
        ("k0", key_input.at[:, head_cols(c, e, FEAT)], kb.at[0, t_mine, :]),
        ("k2", key_input.at[:, head_cols(c, 1 - e, FEAT)], kb.at[2, t_mine, :]),
        ("v0", values.at[:, head_cols(c, e, HEAD_DIM)], vb.at[0, t_mine, :]),
        ("v2", values.at[:, head_cols(c, 1 - e, HEAD_DIM)], vb.at[2, t_mine, :]),
        ("g", cotangent.at[:, head_cols(c, e, HEAD_DIM)], gb.at[0, t_mine, :]),
    ]
    local = {}
    for n, (name, src, dst) in enumerate(moves):
        local[name] = pltpu.make_async_copy(src, dst, local_sems.at[n])
        local[name].start()
    barrier = pltpu.get_barrier_semaphore()
    friends = [partner, pair_same, pair_other, across, at(ry, z, c)]
    friends += [dev_x(d) for d in sorted({1, NX - 1})]
    friends += [dev_z(d) for d in range(1, NZ)]
    for friend in friends:
        pl.semaphore_signal(barrier, inc=1, device_id=friend, device_id_type=MESH)
    pl.semaphore_wait(barrier, len(friends))
    pair_cores = ((c, pair_same), (p, pair_other))
    for core, to in pair_cores:
        net.send(("w", 1), w_query.at[:, head_cols(core, 1 - e, FEAT)], wf.at[w_mine, :], to, "in")
    net.send(("w", 0), w_query.at[:, head_cols(p, e, FEAT)], wf.at[w_mine, :], partner, "in")
    net.send("h1", hidden, hf.at[rows_of(CT + c * T, T), x_mine], pair_same, "in")
    for slot, parity in ((0, e), (2, 1 - e)):
        net.send(
            "kv0", key_input.at[:, head_cols(p, parity, FEAT)], kb.at[slot, t_mine, :], partner, "in"
        )
        net.send(
            "kv0", values.at[:, head_cols(p, parity, HEAD_DIM)], vb.at[slot, t_mine, :], partner, "in"
        )
    net.send("h0", hidden, hf.at[t_mine, x_mine], partner, "in")
    for core, to in pair_cores:
        cut, narrow = head_cols(core, 1 - e, FEAT), head_cols(core, 1 - e, HEAD_DIM)
        net.send("kv1", key_input.at[:, cut], kb.at[1, t_mine, :], to, "in")
        net.send("kv1", values.at[:, narrow], vb.at[1, t_mine, :], to, "in")
        net.send("kv1", cotangent.at[:, narrow], gb.at[1, t_mine, :], to, "in")
    net.send("g0", cotangent.at[:, head_cols(p, e, HEAD_DIM)], gb.at[0, t_mine, :], partner, "in")

    A_ROWS = CH * A_EIGHTHS // 8
    B_ROWS = CH - A_ROWS

    def w_piece(stream, which, rel_z, part):
        start, size = split(A_ROWS if stream == "A" else B_ROWS, part)
        if stream == "B":
            start = start + A_ROWS
        return wf.at[rows_of((own_y[which] * NZ + (z + rel_z + NZ) % NZ) * CH + start, size), :]

    def w_ring(stream, which, d):
        for s in BOTH:
            piece = w_piece(stream, which, -s * (d - 1), part_of(s, d, ZM))
            net.send((stream, which, d), piece, piece, dev_z(s), ("w", which % 2))

    def w_across(stream, b, rel):
        piece = w_piece(stream, b, rel, "full")
        net.send((stream, "across", b), piece, piece, across, ("w", b))

    def w_next(stream, which, d):
        net.recv((stream, which, d))
        if d < ZM:
            w_ring(stream, which, d + 1)

    def w_begin(b):
        if b == 0:
            local["w"].wait()
        net.recv(("w", b))
        w_ring("A", b, 1)
        w_across("B", b, 0)
        w_across("A", b, 0)
        w_ring("B", b, 1)

    def w_a(b, r):
        w_next("A", b, r)
        for rel in fresh(r, ZM):
            w_across("A", b, rel)

    def w_turn(b):
        net.recv(("B", "across", b))
        w_ring("B", 2 + b, 1)

    def w_last(b):
        net.recv(("A", "across", b))

    def x_ring(name, piece, stage, lane):
        for s in BOTH:
            first, second = ("top", "bot") if s > 0 else ("bot", "top")
            back = 0 if stage < 3 else -s
            ref = piece(back, second if stage == 2 else first)
            net.send((*name, stage), ref, ref, dev_x(s), lane)

    def x_relay(name, piece, stage, lane):
        for s in BOTH:
            first, second = ("top", "bot") if s > 0 else ("bot", "top")
            ref = piece(-s if stage < 3 else -2 * s, second if stage == 2 else first)
            net.send(name, ref, ref, partner, lane)

    def x_begin(name, piece, lane):
        x_ring(name, piece, 1, lane)
        if XM > 1:
            x_ring(name, piece, 2, lane)

    def x_step(name, relay, piece, stage, lane):
        net.recv((*name, stage))
        if stage == 1 and XM > 1:
            x_ring(name, piece, 3, lane)
        x_relay(relay, piece, stage, lane)

    def h_piece(b):
        def piece(rel_x, part):
            start, size = split(T, part)
            xs = (x + rel_x + NX) % NX
            return hf.at[
                rows_of(b * CT + c * T + start, size), pl.ds(pl.multiple_of(xs * DX, DX), DX)
            ]

        return piece

    def h_begin(b):
        if b == 0:
            local["h"].wait()
        else:
            net.recv("h1")
        x_begin(("hx", b), h_piece(b), ("h", b))
        if b == 1:
            piece = h_piece(b)(0, "full")
            net.send(("hp", b), piece, piece, partner, ("h", b))

    def h_step(b, stage):
        x_step(("hx", b), ("hp", b), h_piece(b), stage, ("h", b))

    def h_all(b):
        if b == 0:
            net.recv("h0")
        net.recv(("hp", b))

    SR = FEAT // NZ

    def slice_at(k):
        return pl.ds(pl.multiple_of(k * SR, SR), SR)

    def scan_start(kind):
        for o in range(1, NZ):
            src = s_out.at[kind, :, slice_at((z + o) % NZ), :]
            net.send((kind, "s"), src, s_in.at[kind, o], dev_z(o), ("scan", kind))

    def scan_totals(kind):
        own = s_out[kind, :, slice_at(z), :].astype(F32)
        total = own
        net.recv((kind, "s"))
        pre[z] = own
        for o in range(1, NZ):
            came = s_in[kind, o].astype(F32)
            total = total + came
            pre[(z - o + NZ) % NZ] = came
        t_out[kind] = total.astype(BF16)
        if kind == 0:
            for n, to in ((1, pair_same), (2, across), (3, at(ry, z, c))):
                net.send((kind, "t"), t_out.at[kind], t_in.at[kind, n], to, ("scan", kind))
        else:
            net.send((kind, "t"), t_out.at[kind], t_in.at[kind, 2], across, ("scan", kind))

    def scan_back(kind, result):
        net.recv((kind, "t"))
        zero = jnp.zeros((SR, HEAD_DIM), F32)
        if kind == 0:
            offset = [zero, zero]
            for n in (1, 2, 3):
                for half in (0, 1):
                    term = t_in[0, n, half].astype(F32)
                    offset[half] = offset[half] + jnp.where(own_y[n] < y, term, 0.0)
        else:
            sums = (
                t_out[1, 0].astype(F32),
                t_out[1, 1].astype(F32),
                t_in[1, 2, 0].astype(F32),
                t_in[1, 2, 1].astype(F32),
            )
            offset = []
            for b in BLOCKS:
                total = zero
                for n in range(4):
                    if n != b:
                        total = total + jnp.where(own_y[n] > own_y[b], sums[n], 0.0)
                offset.append(total)
        for half in (0, 1):
            running = offset[half]
            for k in range(NZ) if kind == 0 else reversed(range(NZ)):
                b_out[kind, k, half] = running.astype(BF16)
                running = running + pre[k, half]
        for o in range(1, NZ):
            src = b_out.at[kind, (z + o) % NZ]
            dst = result.at[pl.ds(0, 2), slice_at(z), :]
            net.send((kind, "b"), src, dst, dev_z(o), ("scan", kind))
        result[pl.ds(0, 2), slice_at(z), :] = b_out[kind, z]

    PT = T // NX

    def quarter(rel_x):
        xs = (x + rel_x + NX) % NX
        return pl.ds(pl.multiple_of(xs * PT, PT), PT)

    def h4_start():
        src = hf.at[
            rows_of(c * T + x * PT, PT), pl.ds(pl.multiple_of((1 - pair) * KH, KH), KH)
        ]
        net.send(("h4", 0), src, h4.at[0, c, quarter(0), :], across, "h4")

    def h4_piece(j):
        def piece(rel_x, part):
            start, size = {"full": (0, KH), "top": (0, KH // 2), "bot": (KH // 2, KH // 2)}[part]
            return h4.at[j, c, quarter(rel_x), pl.ds(start, size)]

        return piece

    def h4_begin(j):
        net.recv(("h4", j))
        x_begin(("h4x", j), h4_piece(j), "h4")
        mine = h4_piece(j)(0, "full")
        if j == 0:
            net.send(("h4", 1), mine, h4_piece(1)(0, "full"), pair_same, "h4")
        net.send(("h4p", j), mine, mine, partner, "h4")

    def h4_step(j, stage):
        x_step(("h4x", j), ("h4p", j), h4_piece(j), stage, "h4")

    WIDE = 256

    def h4_turn_own():
        for k in range(KH // WIDE):
            cols = pl.ds(pl.multiple_of(pair * KH + k * WIDE, WIDE), WIDE)
            h4t[k * WIDE : (k + 1) * WIDE, 0 : 2 * CT] = hf[:, cols].T

    def h4_turn(j):
        net.recv(("h4p", j))
        for k in range(KH // WIDE):
            cut = slice(k * WIDE, (k + 1) * WIDE)
            h4t[cut, (2 + j) * CT : (3 + j) * CT] = h4[j, :, :, cut].reshape(CT, WIDE).T

    def project(b, half):
        which = pair if half == 0 else 1 - pair
        rows = pl.ds(pl.multiple_of(which * KH, KH), KH)
        block = slice(b * CT, (b + 1) * CT)
        product = dot_nn(hf[block, rows], wf[rows, :])
        q32[block, :] = product if half == 0 else q32[block, :] + product

    causal = lax.broadcasted_iota(jnp.int32, (CT, CT), 0) >= lax.broadcasted_iota(
        jnp.int32, (CT, CT), 1
    )

    def attend(b):
        if b == 1:
            net.recv("prior")
        proj = q32[b * CT : (b + 1) * CT, :]
        feats = jnp.maximum(proj, 0.0).astype(BF16)
        qf[b] = feats
        keys, vals = kf[b], vb[b]
        state = prior[e] if b == 0 else prior[2]
        scores = jnp.where(causal, dot_nt(feats, keys), 0.0).astype(BF16)
        sc[b] = scores
        numer = dot_nn(scores, vals) + dot_nn(feats, state)
        inv = lax.rsqrt(jnp.mean(numer * numer, axis=-1, keepdims=True) + EPSILON)
        normed = numer * inv
        att[b] = normed.astype(BF16)
        grad = gb[b].astype(F32)
        d_num = (inv * (grad - normed * jnp.mean(grad * normed, axis=-1, keepdims=True))).astype(BF16)
        dn[b] = d_num
        mixed = jnp.where(causal, dot_nt(d_num, vals), 0.0).astype(BF16)
        mx[b] = mixed
        d_feat = dot_nn(mixed, keys) + dot_nt(d_num, state)
        d_q = jnp.where(proj > 0, d_feat, 0.0).astype(BF16)
        mine = slice(b * CT, (b + 1) * CT)
        dq4[mine, :] = d_q
        net.send(("dq", b), dq4.at[mine, :], dq4.at[(2 + b) * CT : (3 + b) * CT, :], across, "dq")

    def state_send(b):
        s_out[1, b] = dot_tn(qf[b], dn[b]).astype(BF16)
        for o in range(1, NZ):
            src = s_out.at[1, b, slice_at((z + o) % NZ), :]
            net.send((1, "s"), src, s_in.at[1, o, b], dev_z(o), ("scan", 1))

    def states():
        for name in ("k0", "k2", "v0", "v2"):
            local[name].wait()
        net.recv("kv0")
        kf[0] = jnp.maximum(kb[0], jnp.zeros_like(kb[0]))
        s_out[0, e] = dot_tn(kf[0], vb[0]).astype(BF16)
        s_out[0, 1 - e] = dot_tn(jnp.maximum(kb[2], jnp.zeros_like(kb[2])), vb[2]).astype(BF16)
        scan_start(0)

    def prior_send():
        net.recv((0, "b"))
        net.send("prior", prior.at[1 - e], prior.at[2], pair_same, "prior")

    def keys_in():
        net.recv("kv1")
        kf[1] = jnp.maximum(kb[1], jnp.zeros_like(kb[1]))

    def grads_in():
        local["g"].wait()
        net.recv("g0")

    def block_parts(b):
        vg32[b] = dot_tn(sc[b], dn[b])
        kg32[b] = dot_tn(mx[b], qf[b])

    def state_parts(b):
        state = later[b]
        vg[b] = (vg32[b] + dot_nn(kf[b], state)).astype(BF16)
        d_key = kg32[b] + dot_nt(vb[b], state)
        kg[b] = jnp.where(kb[b] > 0, d_key, 0.0).astype(BF16)

    def part_rows(k):
        return pl.ds(pl.multiple_of(((1 - u) if k == 0 else u) * KY, KY), KY)

    def contract_own(k):
        g32[k] = dot_nn(h4t[part_rows(k), 0 : 2 * CT], dq4[0 : 2 * CT, :])

    def contract_rest(k):
        if k == 0:
            net.recv(("dq", 0))
            net.recv(("dq", 1))
        rest = slice(2 * CT, 4 * CT)
        g32[k] = g32[k] + dot_nn(h4t[part_rows(k), rest], dq4[rest, :])
        for h in (0, 1):
            rs_send(k, h, ZM)

    def rs_rows(part):
        start, size = split(CH, part)
        return slice(start, start + size)

    def half_cols(h):
        return slice(h * FEAT // 2, (h + 1) * FEAT // 2)

    def rs_send(k, h, d):
        cols = half_cols(h)
        if d < ZM:
            net.recv(("rs", k, h, d + 1))
        for s in BOTH:
            rows = rs_rows(part_of(s, d, ZM))
            size = rows.stop - rows.start
            to = (z + s * d + NZ) % NZ
            total = g32[k, rows_of(to * CH + rows.start, size), cols]
            way = 0 if s > 0 else 1
            rs_out[k, way, d - 1, rows, cols] = total.astype(BF16)
            if d < ZM:
                came = rs_rows(part_of(s, d + 1, ZM))
                got = rs_in[k, way, d, came, cols].astype(F32)
                rs_out[k, way, d - 1, came, cols] = (total[came, :] + got).astype(BF16)
            net.send(
                ("rs", k, h, d),
                rs_out.at[k, way, d - 1, rows, cols],
                rs_in.at[k, way, d - 1, rows, cols],
                dev_z(s),
                ("rs", k),
            )

    def rs_last(k, h):
        cols = half_cols(h)
        net.recv(("rs", k, h, 1))
        total = g32[k, rows_of(z * CH, CH), cols]
        if ZM > 1:
            qg[k, :, cols] = (
                total + rs_in[k, 0, 0, :, cols].astype(F32) + rs_in[k, 1, 0, :, cols].astype(F32)
            )
        else:
            for way, part in enumerate(("top", "bot")):
                came = rs_rows(part)
                qg[k, came, cols] = total[came, :] + rs_in[k, way, 0, came, cols].astype(F32)
        at_cols = (2 * c + e) * FEAT + h * (FEAT // 2)
        mine = out_qg.at[:, pl.ds(pl.multiple_of(at_cols, FEAT // 2), FEAT // 2)]

        def piece(core):
            return qg.at[k, rows_of(core * WR, WR), cols]

        if k == 0:
            net.send("qg", piece(c), mine, pair_same, "out")
            net.send("qg", piece(p), mine, pair_other, "out")
        else:
            net.send("qg", piece(p), mine, partner, "out")
            local["qg", h] = pltpu.make_async_copy(piece(c), mine, local_sems.at[10 + h])
            local["qg", h].start()

    def out_send(name, buf, out, rows, width, n):
        mine = out.at[:, head_cols(c, e, width)]

        def piece(block, core):
            return buf.at[block, rows_of(core * rows, rows), :]

        net.send(name, piece(1, c), mine, pair_same, "out")
        net.send(name, piece(1, p), mine, pair_other, "out")
        net.send(name, piece(0, p), mine, partner, "out")
        local[name] = pltpu.make_async_copy(piece(0, c), mine, local_sems.at[n])
        local[name].start()

    def att_out():
        out_send("att", att, out_att, T, HEAD_DIM, 7)

    def later_parts():
        net.recv((1, "b"))
        for b in BLOCKS:
            state_parts(b)
        out_send("kg", kg, out_kg, T, FEAT, 8)
        out_send("vg", vg, out_vg, T, HEAD_DIM, 9)

    tasks = {
        "w": w_begin,
        "A": w_a,
        "B": lambda which, d: w_next("B", which, d),
        "across": w_turn,
        "last": w_last,
        "h": h_begin,
        "hx": h_step,
        "hp": h_all,
        "state": states,
        "tot": scan_totals,
        "back": lambda kind: scan_back(kind, later if kind else prior),
        "prior": prior_send,
        "kv1": keys_in,
        "g0": grads_in,
        "h4s": h4_start,
        "h4": h4_begin,
        "h4x": h4_step,
        "turnown": h4_turn_own,
        "turn": h4_turn,
        "mm": project,
        "att": attend,
        "s1": state_send,
        "outatt": att_out,
        "blk": block_parts,
        "own": contract_own,
        "rest": contract_rest,
        "rs": rs_send,
        "rsl": rs_last,
        "later": later_parts,
    }
    for name, *where in ORDER:
        tasks[name](*where)
    for name in ("att", "kg", "vg"):
        net.recv(name)
        local[name].wait()
    net.recv("qg")
    for h in (0, 1):
        local["qg", h].wait()
    net.finish()


def solution(mesh):
    NX, ctx_size = mesh.shape["heads"], mesh.shape["ctx"]
    NY = 4
    NZ = ctx_size // (NY * CORES)
    sizes = (NX, NY, NZ)

    def body(hidden, w_query, key_input, values, cotangent):
        T, DX = hidden.shape
        WR, NALL = w_query.shape
        VALL = values.shape[1]
        D = NX * DX
        CH = CORES * WR
        KY = NZ * CH
        CT = CORES * T
        ZM = NZ // 2
        SR = FEAT // NZ
        any_space = pl.BlockSpec(memory_space=pl.ANY)

        def vmem(*shape, dtype=BF16):
            return pltpu.VMEM(shape, dtype)

        def run(*refs):
            kernel(sizes, *refs)

        return pl.pallas_call(
            run,
            out_shape=(
                jax.ShapeDtypeStruct((T, VALL), BF16),
                jax.ShapeDtypeStruct((WR, NALL), F32),
                jax.ShapeDtypeStruct((T, NALL), BF16),
                jax.ShapeDtypeStruct((T, VALL), BF16),
            ),
            in_specs=[any_space] * 5,
            out_specs=(any_space,) * 4,
            scratch_shapes=[
                vmem(2 * CT, D),
                vmem(D, FEAT),
                vmem(3, CT, FEAT),
                vmem(2, CT, FEAT),
                vmem(3, CT, HEAD_DIM),
                vmem(2, CT, HEAD_DIM),
                vmem(2 * CT, FEAT, dtype=F32),
                vmem(2, CT, FEAT),
                vmem(2, CT, HEAD_DIM),
                vmem(2, CT, HEAD_DIM),
                vmem(2, CT, CT),
                vmem(2, CT, CT),
                vmem(2, CT, HEAD_DIM, dtype=F32),
                vmem(2, CT, FEAT, dtype=F32),
                vmem(2, CT, FEAT),
                vmem(2, CT, HEAD_DIM),
                vmem(2, 2, FEAT, HEAD_DIM),
                vmem(2, NZ, 2, SR, HEAD_DIM),
                vmem(2, 2, SR, HEAD_DIM),
                vmem(2, NY, 2, SR, HEAD_DIM),
                vmem(2, NZ, 2, SR, HEAD_DIM),
                vmem(3, FEAT, HEAD_DIM),
                vmem(2, FEAT, HEAD_DIM),
                vmem(NZ, 2, SR, HEAD_DIM, dtype=F32),
                vmem(2, CORES, T, 2 * KY),
                vmem(2 * KY, 4 * CT),
                vmem(4 * CT, FEAT),
                vmem(2, KY, FEAT, dtype=F32),
                vmem(2, 2, ZM, CH, FEAT),
                vmem(2, 2, ZM, CH, FEAT),
                vmem(2, CH, FEAT, dtype=F32),
                pltpu.SemaphoreType.DMA((LANES,)),
                pltpu.SemaphoreType.DMA((GROUPS,)),
                pltpu.SemaphoreType.DMA((LOCALS,)),
            ],
            compiler_params=pltpu.CompilerParams(
                collective_id=0, has_side_effects=True, vmem_limit_bytes=60000 * 1024
            ),
        )(hidden, w_query, key_input, values, cotangent)

    spec = P("ctx", "heads")
    return jax.shard_map(
        body, mesh=mesh, in_specs=(spec,) * 5, out_specs=(spec,) * 4, check_vma=False
    )
```

```python
import jax
import jax.numpy as jnp
from jax import lax
from jax.experimental import pallas as pl
from jax.experimental.pallas import tpu as pltpu
from jax.sharding import PartitionSpec as P

HEAD_DIM = 128
FEAT = 256
CORES = 2
EPSILON = 1e-06
MESH = pl.DeviceIdType.MESH
F32 = jnp.float32
BF16 = jnp.bfloat16
GROUPS = 82
LANES = 13
LOCALS = 7
A_EIGHTHS = 5
A_FIFTHS = 1
RS_EIGHTHS = 2

ORDER = (
    ('h', 0),
    ('w', 0),
    ('state',),
    ('g0',),
    ('w', 1),
    ('across', 0),
    ('A', 0, 1),
    ('B', 0, 1),
    ('hx', 0, 1),
    ('across', 1),
    ('hx', 0, 2),
    ('A', 1, 1),
    ('h', 1),
    ('B', 1, 1),
    ('B', 2, 1),
    ('tot', 0),
    ('A', 0, 2),
    ('hx', 0, 3),
    ('B', 0, 2),
    ('h4s',),
    ('B', 3, 1),
    ('A', 1, 2),
    ('hp', 0),
    ('B', 1, 2),
    ('B', 2, 2),
    ('hx', 1, 1),
    ('kv1',),
    ('A', 0, 3),
    ('back', 0),
    ('B', 0, 3),
    ('B', 3, 2),
    ('A', 1, 3),
    ('hx', 1, 2),
    ('B', 1, 3),
    ('B', 2, 3),
    ('h4', 0),
    ('A', 0, 4),
    ('hx', 1, 3),
    ('h4x', 0, 1),
    ('B', 0, 4),
    ('hp', 1),
    ('turnown',),
    ('A', 1, 4),
    ('B', 3, 3),
    ('B', 1, 4),
    ('mm', 0, 0),
    ('B', 2, 4),
    ('h4', 1),
    ('h4x', 0, 2),
    ('mm', 1, 0),
    ('prior',),
    ('last', 0),
    ('h4x', 0, 3),
    ('B', 3, 4),
    ('last', 1),
    ('mm', 0, 1),
    ('att', 0),
    ('s1', 0),
    ('h4x', 1, 1),
    ('mm', 1, 1),
    ('att', 1),
    ('s1', 1),
    ('h4x', 1, 2),
    ('own', 0),
    ('own', 1),
    ('h4x', 1, 3),
    ('turn', 0),
    ('outatt',),
    ('blk', 0),
    ('blk', 1),
    ('turn', 1),
    ('far', 0),
    ('far', 1),
    ('rest', 0),
    ('tot', 1),
    ('rest', 1),
    ('rs', 0, 0, 3),
    ('rs', 0, 1, 3),
    ('back', 1),
    ('rs', 1, 0, 3),
    ('rs', 1, 1, 3),
    ('rs', 0, 0, 2),
    ('rs', 0, 1, 2),
    ('rs', 1, 0, 2),
    ('rs', 1, 1, 2),
    ('rs', 0, 0, 1),
    ('later',),
    ('rs', 0, 1, 1),
    ('rs', 1, 0, 1),
    ('rs', 1, 1, 1),
    ('rsl', 0, 0),
    ('rsl', 0, 1),
    ('rsl', 1, 0),
    ('rsl', 1, 1),
)


def dot_nn(a, b):
    return lax.dot_general(a, b, (((1,), (0,)), ((), ())), preferred_element_type=F32)


def dot_nt(a, b):
    return lax.dot_general(a, b, (((1,), (1,)), ((), ())), preferred_element_type=F32)


def dot_tn(a, b):
    return lax.dot_general(a, b, (((0,), (0,)), ((), ())), preferred_element_type=F32)


class Net:
    def __init__(self, ruler, send_sems, recv_sems):
        self.ruler, self.send_sems, self.recv_sems = ruler, send_sems, recv_sems
        self.groups = {}
        self.lanes = {}
        self.row_bytes = ruler.shape[1] * 2

    def send(self, group, src, dst, device, lane):
        size = 4 if src.dtype == F32 else 2
        for extent in src.shape:
            size *= extent
        group_at = self.groups.setdefault(group, [len(self.groups), 0, False])
        lane_at = self.lanes.setdefault(lane, [len(self.lanes), 0])
        group_at[1] += size
        lane_at[1] += size
        self.device = device
        pltpu.make_async_remote_copy(
            src_ref=src,
            dst_ref=dst,
            send_sem=self.send_sems.at[lane_at[0]],
            recv_sem=self.recv_sems.at[group_at[0]],
            device_id=device,
            device_id_type=MESH,
        ).start()

    def measure(self, size, send_at, recv_at):
        ref = self.ruler.at[pl.ds(0, size // self.row_bytes), :]
        return pltpu.make_async_remote_copy(
            src_ref=ref,
            dst_ref=ref,
            send_sem=self.send_sems.at[send_at],
            recv_sem=self.recv_sems.at[recv_at],
            device_id=self.device,
            device_id_type=MESH,
        )

    def recv(self, group):
        at = self.groups[group]
        assert not at[2]
        at[2] = True
        self.measure(at[1], 0, at[0]).wait_recv()

    def finish(self):
        assert len(self.groups) <= GROUPS and len(self.lanes) <= LANES
        assert all(at[2] for at in self.groups.values())
        for at, size in self.lanes.values():
            self.measure(size, at, 0).wait_send()


def kernel(
    sizes, hidden, w_query, key_input, values, cotangent,
    out_att, out_qg, out_kg, out_vg,
    hf, wf, kb, kf, vb, gb, q32, qf, att, dn, sc, mx, vg32, kg32, kg, vg,
    s_out, s_in, t_out, t_in, b_out, prior, later, pre,
    h4, h4t, dq4, g32, rs_out, rs_in, qg,
    send_sems, recv_sems, local_sems,
):
    NX, NY, NZ = sizes
    x = lax.axis_index("heads")
    ctx = lax.axis_index("ctx")
    c = ctx % CORES
    z = (ctx // CORES) % NZ
    y = ctx // (CORES * NZ)
    p = 1 - c
    u = y % 2
    pair = y // 2
    py = y + 1 - 2 * u
    qy = NY - 1 - y
    ry = NY - 1 - py
    own_y = (y, py, qy, ry)
    e = ((y + 1) // 2) % 2
    T, DX = hidden.shape
    WR, NALL = w_query.shape
    D = NX * DX
    CH = CORES * WR
    KY = NZ * CH
    KH = 2 * KY
    CT = CORES * T
    XM, ZM = NX // 2, NZ // 2
    BOTH = (1, -1)
    BLOCKS = (0, 1)

    def at(y_, z_, core):
        return (x, (y_ * NZ + z_) * CORES + core)

    def dev_x(step):
        return ((x + step + NX) % NX, ctx)

    def dev_z(step):
        return at(y, (z + step + NZ) % NZ, c)

    partner = at(y, z, p)
    pair_same = at(py, z, c)
    pair_other = at(py, z, p)
    across = at(qy, z, c)
    net = Net(wf, send_sems, recv_sems)

    def rows_of(start, size, unit=16):
        return pl.ds(pl.multiple_of(start, unit), size)

    def head_cols(core, parity, width):
        return pl.ds(pl.multiple_of((2 * core + parity) * width, width), width)

    def split(total, part, top=None):
        top = total // 2 if top is None else top
        return {"full": (0, total), "top": (0, top), "bot": (top, total - top)}[part]

    def part_of(direction, d, most):
        if d < most:
            return "full"
        return "top" if direction > 0 else "bot"

    def fresh(r, most):
        if r == 0:
            return [0]
        return [-r, r] if r < most else [most]

    w_mine = rows_of((y * NZ + z) * CH + c * WR, WR)
    t_mine = rows_of(c * T, T)
    x_mine = pl.ds(pl.multiple_of(x * DX, DX), DX)
    moves = [
        ("w", w_query.at[:, head_cols(c, e, FEAT)], wf.at[w_mine, :]),
        ("h", hidden, hf.at[t_mine, x_mine]),
        ("k0", key_input.at[:, head_cols(c, e, FEAT)], kb.at[0, t_mine, :]),
        ("k2", key_input.at[:, head_cols(c, 1 - e, FEAT)], kb.at[2, t_mine, :]),
        ("v0", values.at[:, head_cols(c, e, HEAD_DIM)], vb.at[0, t_mine, :]),
        ("v2", values.at[:, head_cols(c, 1 - e, HEAD_DIM)], vb.at[2, t_mine, :]),
        ("g", cotangent.at[:, head_cols(c, e, HEAD_DIM)], gb.at[0, t_mine, :]),
    ]
    local = {}
    for n, (name, src, dst) in enumerate(moves):
        local[name] = pltpu.make_async_copy(src, dst, local_sems.at[n])
        local[name].start()
    barrier = pltpu.get_barrier_semaphore()
    friends = [partner, pair_same, pair_other, across, at(ry, z, c)]
    friends += [dev_x(d) for d in sorted({1, NX - 1})]
    friends += [dev_z(d) for d in range(1, NZ)]
    for friend in friends:
        pl.semaphore_signal(barrier, inc=1, device_id=friend, device_id_type=MESH)
    pl.semaphore_wait(barrier, len(friends))
    pair_cores = ((c, pair_same), (p, pair_other))
    for core, to in pair_cores:
        net.send(("w", 1), w_query.at[:, head_cols(core, 1 - e, FEAT)], wf.at[w_mine, :], to, "in")
    net.send(("w", 0), w_query.at[:, head_cols(p, e, FEAT)], wf.at[w_mine, :], partner, "in")
    net.send("h1", hidden, hf.at[rows_of(CT + c * T, T), x_mine], pair_same, "in")
    for slot, parity in ((0, e), (2, 1 - e)):
        net.send(
            "kv0", key_input.at[:, head_cols(p, parity, FEAT)], kb.at[slot, t_mine, :], partner, "in"
        )
        net.send(
            "kv0", values.at[:, head_cols(p, parity, HEAD_DIM)], vb.at[slot, t_mine, :], partner, "in"
        )
    net.send("h0", hidden, hf.at[t_mine, x_mine], partner, "in")
    for core, to in pair_cores:
        cut, narrow = head_cols(core, 1 - e, FEAT), head_cols(core, 1 - e, HEAD_DIM)
        net.send("kv1", key_input.at[:, cut], kb.at[1, t_mine, :], to, "in")
        net.send("kv1", values.at[:, narrow], vb.at[1, t_mine, :], to, "in")
        net.send("kv1", cotangent.at[:, narrow], gb.at[1, t_mine, :], to, "in")
    net.send("g0", cotangent.at[:, head_cols(p, e, HEAD_DIM)], gb.at[0, t_mine, :], partner, "in")

    A_ROWS = CH * A_EIGHTHS // 8
    B_ROWS = CH - A_ROWS
    A_TOP, B_TOP = A_ROWS * A_FIFTHS // 5, B_ROWS // 3

    def w_piece(stream, which, rel_z, part):
        total, first = (A_ROWS, A_TOP) if stream == "A" else (B_ROWS, B_TOP)
        start, size = split(total, part, first)
        if stream == "B":
            start = start + A_ROWS
        return wf.at[rows_of((own_y[which] * NZ + (z + rel_z + NZ) % NZ) * CH + start, size), :]

    def w_ring(stream, which, d):
        for s in BOTH:
            piece = w_piece(stream, which, -s * (d - 1), part_of(s, d, ZM))
            net.send((stream, which, d), piece, piece, dev_z(s), ("w", which % 2))

    def w_across(stream, b, rel):
        piece = w_piece(stream, b, rel, "full")
        net.send((stream, "across", b), piece, piece, across, ("w", b))

    def w_next(stream, which, d):
        net.recv((stream, which, d))
        if d < ZM:
            w_ring(stream, which, d + 1)

    def w_begin(b):
        if b == 0:
            local["w"].wait()
        net.recv(("w", b))
        w_ring("A", b, 1)
        w_across("B", b, 0)
        w_across("A", b, 0)
        w_ring("B", b, 1)

    def w_a(b, r):
        w_next("A", b, r)
        for rel in fresh(r, ZM):
            w_across("A", b, rel)

    def w_turn(b):
        net.recv(("B", "across", b))
        w_ring("B", 2 + b, 1)

    def w_last(b):
        net.recv(("A", "across", b))

    def x_ring(name, piece, stage, lane):
        for s in BOTH:
            first, second = ("top", "bot") if s > 0 else ("bot", "top")
            back = 0 if stage < 3 else -s
            ref = piece(back, second if stage == 2 else first)
            net.send((*name, stage), ref, ref, dev_x(s), lane)

    def x_relay(name, piece, stage, lane):
        for s in BOTH:
            first, second = ("top", "bot") if s > 0 else ("bot", "top")
            ref = piece(-s if stage < 3 else -2 * s, second if stage == 2 else first)
            net.send(name, ref, ref, partner, lane)

    def x_begin(name, piece, lane):
        x_ring(name, piece, 1, lane)
        if XM > 1:
            x_ring(name, piece, 2, lane)

    def x_step(name, relay, piece, stage, lane):
        net.recv((*name, stage))
        if stage == 1 and XM > 1:
            x_ring(name, piece, 3, lane)
        x_relay(relay, piece, stage, lane)

    def h_piece(b):
        def piece(rel_x, part):
            start, size = split(T, part)
            xs = (x + rel_x + NX) % NX
            return hf.at[
                rows_of(b * CT + c * T + start, size), pl.ds(pl.multiple_of(xs * DX, DX), DX)
            ]

        return piece

    def h_begin(b):
        if b == 0:
            local["h"].wait()
        else:
            net.recv("h1")
        x_begin(("hx", b), h_piece(b), ("h", b))
        if b == 1:
            piece = h_piece(b)(0, "full")
            net.send(("hp", b), piece, piece, partner, ("h", b))

    def h_step(b, stage):
        x_step(("hx", b), ("hp", b), h_piece(b), stage, ("h", b))

    def h_all(b):
        if b == 0:
            net.recv("h0")
        net.recv(("hp", b))

    SR = FEAT // NZ

    def slice_at(k):
        return pl.ds(pl.multiple_of(k * SR, SR), SR)

    def scan_start(kind):
        for o in range(1, NZ):
            src = s_out.at[kind, :, slice_at((z + o) % NZ), :]
            net.send((kind, "s"), src, s_in.at[kind, o], dev_z(o), ("scan", kind))

    def scan_totals(kind):
        own = s_out[kind, :, slice_at(z), :].astype(F32)
        total = own
        net.recv((kind, "s"))
        pre[z] = own
        for o in range(1, NZ):
            came = s_in[kind, o].astype(F32)
            total = total + came
            pre[(z - o + NZ) % NZ] = came
        t_out[kind] = total.astype(BF16)
        if kind == 0:
            for n, to in ((1, pair_same), (2, across), (3, at(ry, z, c))):
                net.send((kind, "t"), t_out.at[kind], t_in.at[kind, n], to, ("scan", kind))
        else:
            net.send((kind, "t"), t_out.at[kind], t_in.at[kind, 2], across, ("scan", kind))

    def scan_back(kind, result):
        net.recv((kind, "t"))
        zero = jnp.zeros((SR, HEAD_DIM), F32)
        if kind == 0:
            offset = [zero, zero]
            for n in (1, 2, 3):
                for half in (0, 1):
                    term = t_in[0, n, half].astype(F32)
                    offset[half] = offset[half] + jnp.where(own_y[n] < y, term, 0.0)
        else:
            sums = (
                t_out[1, 0].astype(F32),
                t_out[1, 1].astype(F32),
                t_in[1, 2, 0].astype(F32),
                t_in[1, 2, 1].astype(F32),
            )
            offset = []
            for b in BLOCKS:
                total = zero
                for n in range(4):
                    if n != b:
                        total = total + jnp.where(own_y[n] > own_y[b], sums[n], 0.0)
                offset.append(total)
        for half in (0, 1):
            running = offset[half]
            for k in range(NZ) if kind == 0 else reversed(range(NZ)):
                b_out[kind, k, half] = running.astype(BF16)
                running = running + pre[k, half]
        for o in range(1, NZ):
            src = b_out.at[kind, (z + o) % NZ]
            dst = result.at[pl.ds(0, 2), slice_at(z), :]
            net.send((kind, "b"), src, dst, dev_z(o), ("scan", kind))
        result[pl.ds(0, 2), slice_at(z), :] = b_out[kind, z]

    PT = T // NX

    def quarter(rel_x):
        xs = (x + rel_x + NX) % NX
        return pl.ds(pl.multiple_of(xs * PT, PT), PT)

    def h4_start():
        src = hf.at[
            rows_of(c * T + x * PT, PT), pl.ds(pl.multiple_of((1 - pair) * KH, KH), KH)
        ]
        net.send(("h4", 0), src, h4.at[0, c, quarter(0), :], across, "h4")

    def h4_piece(j):
        def piece(rel_x, part):
            start, size = {"full": (0, KH), "top": (0, KH // 2), "bot": (KH // 2, KH // 2)}[part]
            return h4.at[j, c, quarter(rel_x), pl.ds(start, size)]

        return piece

    def h4_begin(j):
        net.recv(("h4", j))
        x_begin(("h4x", j), h4_piece(j), "h4")
        mine = h4_piece(j)(0, "full")
        if j == 0:
            net.send(("h4", 1), mine, h4_piece(1)(0, "full"), pair_same, "h4")
        net.send(("h4p", j), mine, mine, partner, "h4")

    def h4_step(j, stage):
        x_step(("h4x", j), ("h4p", j), h4_piece(j), stage, "h4")

    WIDE = 256

    def h4_turn_own():
        for k in range(KH // WIDE):
            cols = pl.ds(pl.multiple_of(pair * KH + k * WIDE, WIDE), WIDE)
            h4t[k * WIDE : (k + 1) * WIDE, 0 : 2 * CT] = hf[:, cols].T

    def h4_turn(j):
        net.recv(("h4p", j))
        for k in range(KH // WIDE):
            cut = slice(k * WIDE, (k + 1) * WIDE)
            h4t[cut, (2 + j) * CT : (3 + j) * CT] = h4[j, :, :, cut].reshape(CT, WIDE).T

    def project(b, half):
        which = pair if half == 0 else 1 - pair
        rows = pl.ds(pl.multiple_of(which * KH, KH), KH)
        block = slice(b * CT, (b + 1) * CT)
        product = dot_nn(hf[block, rows], wf[rows, :])
        q32[block, :] = product if half == 0 else q32[block, :] + product

    causal = lax.broadcasted_iota(jnp.int32, (CT, CT), 0) >= lax.broadcasted_iota(
        jnp.int32, (CT, CT), 1
    )

    def attend(b):
        if b == 1:
            net.recv("prior")
        proj = q32[b * CT : (b + 1) * CT, :]
        feats = jnp.maximum(proj, 0.0).astype(BF16)
        qf[b] = feats
        keys, vals = kf[b], vb[b]
        state = prior[e] if b == 0 else prior[2]
        scores = jnp.where(causal, dot_nt(feats, keys), 0.0).astype(BF16)
        sc[b] = scores
        numer = dot_nn(scores, vals) + dot_nn(feats, state)
        inv = lax.rsqrt(jnp.mean(numer * numer, axis=-1, keepdims=True) + EPSILON)
        normed = numer * inv
        att[b] = normed.astype(BF16)
        grad = gb[b].astype(F32)
        d_num = (inv * (grad - normed * jnp.mean(grad * normed, axis=-1, keepdims=True))).astype(BF16)
        dn[b] = d_num
        mixed = jnp.where(causal, dot_nt(d_num, vals), 0.0).astype(BF16)
        mx[b] = mixed
        d_feat = dot_nn(mixed, keys) + dot_nt(d_num, state)
        d_q = jnp.where(proj > 0, d_feat, 0.0).astype(BF16)
        mine = slice(b * CT, (b + 1) * CT)
        dq4[mine, :] = d_q
        net.send(("dq", b), dq4.at[mine, :], dq4.at[(2 + b) * CT : (3 + b) * CT, :], across, "dq")

    def state_send(b):
        s_out[1, b] = dot_tn(qf[b], dn[b]).astype(BF16)
        for o in range(1, NZ):
            src = s_out.at[1, b, slice_at((z + o) % NZ), :]
            net.send((1, "s"), src, s_in.at[1, o, b], dev_z(o), ("scan", 1))

    def states():
        for name in ("k0", "k2", "v0", "v2"):
            local[name].wait()
        net.recv("kv0")
        kf[0] = jnp.maximum(kb[0], jnp.zeros_like(kb[0]))
        s_out[0, e] = dot_tn(kf[0], vb[0]).astype(BF16)
        s_out[0, 1 - e] = dot_tn(jnp.maximum(kb[2], jnp.zeros_like(kb[2])), vb[2]).astype(BF16)
        scan_start(0)

    def prior_send():
        net.recv((0, "b"))
        net.send("prior", prior.at[1 - e], prior.at[2], pair_same, "prior")

    def keys_in():
        net.recv("kv1")
        kf[1] = jnp.maximum(kb[1], jnp.zeros_like(kb[1]))

    def grads_in():
        local["g"].wait()
        net.recv("g0")

    def block_parts(b):
        vg32[b] = dot_tn(sc[b], dn[b])
        kg32[b] = dot_tn(mx[b], qf[b])

    def state_parts(b):
        state = later[b]
        vg[b] = (vg32[b] + dot_nn(kf[b], state)).astype(BF16)
        d_key = kg32[b] + dot_nt(vb[b], state)
        kg[b] = jnp.where(kb[b] > 0, d_key, 0.0).astype(BF16)

    def part_rows(k):
        return pl.ds(pl.multiple_of(((1 - u) if k == 0 else u) * KY, KY), KY)

    def contract_own(k):
        g32[k] = dot_nn(h4t[part_rows(k), 0 : 2 * CT], dq4[0 : 2 * CT, :])

    def contract_rest(k):
        rest = slice(2 * CT, 4 * CT)
        g32[k] = g32[k] + dot_nn(h4t[part_rows(k), rest], dq4[rest, :])

    def contract_far(k):
        if k == 0:
            net.recv(("dq", 0))
            net.recv(("dq", 1))
        to = ((z + ZM) % NZ) * CH
        rows = rows_of(((1 - u) if k == 0 else u) * KY + to, CH)
        rest = slice(2 * CT, 4 * CT)
        far = g32[k, rows_of(to, CH), :] + dot_nn(h4t[rows, rest], dq4[rest, :])
        for s in BOTH:
            rows = rs_rows(part_of(s, ZM, ZM))
            rs_out[k, 0 if s > 0 else 1, ZM - 1, rows, :] = far[rows, :].astype(BF16)
        for h in (0, 1):
            for s in BOTH:
                rs_put(k, h, s, ZM)

    def rs_rows(part):
        start, size = split(CH, part, CH * RS_EIGHTHS // 8)
        return slice(start, start + size)

    def rs_put(k, h, s, d):
        way, rows, cols = 0 if s > 0 else 1, rs_rows(part_of(s, d, ZM)), half_cols(h)
        net.send(
            ("rs", k, h, d),
            rs_out.at[k, way, d - 1, rows, cols],
            rs_in.at[k, way, d - 1, rows, cols],
            dev_z(s),
            ("rs", k),
        )

    def half_cols(h):
        return slice(h * FEAT // 2, (h + 1) * FEAT // 2)

    def rs_send(k, h, d):
        cols = half_cols(h)
        net.recv(("rs", k, h, d + 1))
        for s in BOTH:
            rows = rs_rows(part_of(s, d, ZM))
            size = rows.stop - rows.start
            to = (z + s * d + NZ) % NZ
            total = g32[k, rows_of(to * CH + rows.start, size), cols]
            way = 0 if s > 0 else 1
            rs_out[k, way, d - 1, rows, cols] = total.astype(BF16)
            came = rs_rows(part_of(s, d + 1, ZM))
            got = rs_in[k, way, d, came, cols].astype(F32)
            rs_out[k, way, d - 1, came, cols] = (total[came, :] + got).astype(BF16)
            rs_put(k, h, s, d)

    def rs_last(k, h):
        cols = half_cols(h)
        net.recv(("rs", k, h, 1))
        total = g32[k, rows_of(z * CH, CH), cols]
        if ZM > 1:
            qg[k, :, cols] = (
                total + rs_in[k, 0, 0, :, cols].astype(F32) + rs_in[k, 1, 0, :, cols].astype(F32)
            )
        else:
            for way, part in enumerate(("top", "bot")):
                came = rs_rows(part)
                qg[k, came, cols] = total[came, :] + rs_in[k, way, 0, came, cols].astype(F32)
        at_cols = (2 * c + e) * FEAT + h * (FEAT // 2)
        mine = out_qg.at[:, pl.ds(pl.multiple_of(at_cols, FEAT // 2), FEAT // 2)]

        def piece(core):
            return qg.at[k, rows_of(core * WR, WR), cols]

        if k == 0:
            net.send("qg", piece(c), mine, pair_same, "out")
            net.send("qg", piece(p), mine, pair_other, "out")
        else:
            net.send("qg", piece(p), mine, partner, "out")
            out_qg[:, pl.ds(pl.multiple_of(at_cols, FEAT // 2), FEAT // 2)] = qg[
                k, rows_of(c * WR, WR), cols
            ]

    def out_send(name, buf, out, rows, width):
        mine = out.at[:, head_cols(c, e, width)]

        def piece(block, core):
            return buf.at[block, rows_of(core * rows, rows), :]

        net.send(name, piece(1, c), mine, pair_same, "out")
        net.send(name, piece(1, p), mine, pair_other, "out")
        net.send(name, piece(0, p), mine, partner, "out")
        out[:, head_cols(c, e, width)] = buf[0, rows_of(c * rows, rows), :]

    def att_out():
        out_send("att", att, out_att, T, HEAD_DIM)

    def later_parts():
        net.recv((1, "b"))
        for b in BLOCKS:
            state_parts(b)
        out_send("kg", kg, out_kg, T, FEAT)
        out_send("vg", vg, out_vg, T, HEAD_DIM)

    tasks = {
        "w": w_begin,
        "A": w_a,
        "B": lambda which, d: w_next("B", which, d),
        "across": w_turn,
        "last": w_last,
        "h": h_begin,
        "hx": h_step,
        "hp": h_all,
        "state": states,
        "tot": scan_totals,
        "back": lambda kind: scan_back(kind, later if kind else prior),
        "prior": prior_send,
        "kv1": keys_in,
        "g0": grads_in,
        "h4s": h4_start,
        "h4": h4_begin,
        "h4x": h4_step,
        "turnown": h4_turn_own,
        "turn": h4_turn,
        "mm": project,
        "att": attend,
        "s1": state_send,
        "outatt": att_out,
        "blk": block_parts,
        "own": contract_own,
        "far": contract_far,
        "rest": contract_rest,
        "rs": rs_send,
        "rsl": rs_last,
        "later": later_parts,
    }
    for name, *where in ORDER:
        tasks[name](*where)
    for name in ("att", "kg", "vg"):
        net.recv(name)
    net.recv("qg")
    net.finish()


def write_out(*refs):
    ins, outs, sems = refs[:4], refs[4:8], refs[8]
    copies = [
        pltpu.make_async_copy(src, dst, sems.at[n]) for n, (src, dst) in enumerate(zip(ins, outs))
    ]
    for copy in copies:
        copy.start()
    for copy in copies:
        copy.wait()


def solution(mesh):
    NX, ctx_size = mesh.shape["heads"], mesh.shape["ctx"]
    NY = 4
    NZ = ctx_size // (NY * CORES)
    sizes = (NX, NY, NZ)

    def body(hidden, w_query, key_input, values, cotangent):
        T, DX = hidden.shape
        WR, NALL = w_query.shape
        VALL = values.shape[1]
        D = NX * DX
        CH = CORES * WR
        KY = NZ * CH
        CT = CORES * T
        ZM = NZ // 2
        SR = FEAT // NZ
        any_space = pl.BlockSpec(memory_space=pl.ANY)
        vmem_space = pl.BlockSpec(memory_space=pltpu.VMEM)
        outs = (((T, VALL), BF16), ((WR, NALL), F32), ((T, NALL), BF16), ((T, VALL), BF16))

        def vmem(*shape, dtype=BF16):
            return pltpu.VMEM(shape, dtype)

        def run(*refs):
            kernel(sizes, *refs)

        parts = pl.pallas_call(
            run,
            out_shape=tuple(pltpu.VMEM(*of) for of in outs),
            in_specs=[any_space] * 5,
            out_specs=(vmem_space,) * 4,
            scratch_shapes=[
                vmem(2 * CT, D),
                vmem(D, FEAT),
                vmem(3, CT, FEAT),
                vmem(2, CT, FEAT),
                vmem(3, CT, HEAD_DIM),
                vmem(2, CT, HEAD_DIM),
                vmem(2 * CT, FEAT, dtype=F32),
                vmem(2, CT, FEAT),
                vmem(2, CT, HEAD_DIM),
                vmem(2, CT, HEAD_DIM),
                vmem(2, CT, CT),
                vmem(2, CT, CT),
                vmem(2, CT, HEAD_DIM, dtype=F32),
                vmem(2, CT, FEAT, dtype=F32),
                vmem(2, CT, FEAT),
                vmem(2, CT, HEAD_DIM),
                vmem(2, 2, FEAT, HEAD_DIM),
                vmem(2, NZ, 2, SR, HEAD_DIM),
                vmem(2, 2, SR, HEAD_DIM),
                vmem(2, NY, 2, SR, HEAD_DIM),
                vmem(2, NZ, 2, SR, HEAD_DIM),
                vmem(3, FEAT, HEAD_DIM),
                vmem(2, FEAT, HEAD_DIM),
                vmem(NZ, 2, SR, HEAD_DIM, dtype=F32),
                vmem(2, CORES, T, 2 * KY),
                vmem(2 * KY, 4 * CT),
                vmem(4 * CT, FEAT),
                vmem(2, KY, FEAT, dtype=F32),
                vmem(2, 2, ZM, CH, FEAT),
                vmem(2, 2, ZM, CH, FEAT),
                vmem(2, CH, FEAT, dtype=F32),
                pltpu.SemaphoreType.DMA((LANES,)),
                pltpu.SemaphoreType.DMA((GROUPS,)),
                pltpu.SemaphoreType.DMA((LOCALS,)),
            ],
            compiler_params=pltpu.CompilerParams(
                collective_id=0, has_side_effects=True, vmem_limit_bytes=60000 * 1024
            ),
        )(hidden, w_query, key_input, values, cotangent)
        return pl.pallas_call(
            write_out,
            out_shape=tuple(jax.ShapeDtypeStruct(*of) for of in outs),
            in_specs=[vmem_space] * 4,
            out_specs=(any_space,) * 4,
            scratch_shapes=[pltpu.SemaphoreType.DMA((4,))],
        )(*[pltpu.with_memory_space_constraint(part, pltpu.VMEM) for part in parts])

    spec = P("ctx", "heads")
    return jax.shard_map(
        body, mesh=mesh, in_specs=(spec,) * 5, out_specs=(spec,) * 4, check_vma=False
    )
```

```python
import jax
import jax.numpy as jnp
from jax import lax
from jax.experimental import pallas as pl
from jax.experimental.pallas import tpu as pltpu
from jax.sharding import PartitionSpec as P

HEAD_DIM = 128
FEAT = 256
CORES = 2
EPSILON = 1e-06
MESH = pl.DeviceIdType.MESH
F32 = jnp.float32
BF16 = jnp.bfloat16
GROUPS = 84
LANES = 13
LOCALS = 7
A_EIGHTHS = 5
A_FIFTHS = 1
RS_EIGHTHS = 2

ORDER = (
    ('h', 0),
    ('w', 0),
    ('state',),
    ('g0',),
    ('w', 1),
    ('across', 0),
    ('A', 0, 1),
    ('B', 0, 1),
    ('hx', 0, 1),
    ('across', 1),
    ('hx', 0, 2),
    ('A', 1, 1),
    ('h', 1),
    ('B', 1, 1),
    ('B', 2, 1),
    ('tot', 0),
    ('A', 0, 2),
    ('hx', 0, 3),
    ('B', 0, 2),
    ('h4s',),
    ('B', 3, 1),
    ('A', 1, 2),
    ('hp', 0),
    ('B', 1, 2),
    ('B', 2, 2),
    ('hx', 1, 1),
    ('kv1',),
    ('A', 0, 3),
    ('back', 0),
    ('B', 0, 3),
    ('B', 3, 2),
    ('A', 1, 3),
    ('hx', 1, 2),
    ('B', 1, 3),
    ('B', 2, 3),
    ('h4', 0),
    ('A', 0, 4),
    ('hx', 1, 3),
    ('h4x', 0, 1),
    ('B', 0, 4),
    ('hp', 1),
    ('turnown',),
    ('A', 1, 4),
    ('B', 3, 3),
    ('B', 1, 4),
    ('mm', 0, 0),
    ('B', 2, 4),
    ('h4', 1),
    ('h4x', 0, 2),
    ('prior',),
    ('mm', 1, 0),
    ('last', 0),
    ('mm', 0, 1),
    ('h4x', 0, 3),
    ('B', 3, 4),
    ('mm', 1, 1),
    ('last', 1),
    ('mm', 0, 2),
    ('att', 0),
    ('s1', 0),
    ('h4x', 1, 1),
    ('mm', 1, 2),
    ('att', 1),
    ('s1', 1),
    ('h4x', 1, 2),
    ('own', 0),
    ('own', 1),
    ('turn', 0),
    ('h4x', 1, 3),
    ('outatt',),
    ('blk', 0),
    ('blk', 1),
    ('turn', 1),
    ('tot', 1),
    ('far', 0, 0),
    ('far', 1, 0),
    ('far', 0, 1),
    ('far', 1, 1),
    ('rest', 0, 0),
    ('rest', 1, 0),
    ('back', 1),
    ('rest', 0, 1),
    ('rest', 1, 1),
    ('rs', 0, 0, 3),
    ('rs', 1, 0, 3),
    ('rs', 0, 1, 3),
    ('rs', 1, 1, 3),
    ('rs', 0, 0, 2),
    ('rs', 1, 0, 2),
    ('rs', 0, 1, 2),
    ('rs', 1, 1, 2),
    ('rs', 0, 0, 1),
    ('later',),
    ('rs', 1, 0, 1),
    ('rs', 0, 1, 1),
    ('rs', 1, 1, 1),
    ('rsl', 0, 0),
    ('rsl', 1, 0),
    ('rsl', 0, 1),
    ('rsl', 1, 1),
)


def dot_nn(a, b):
    return lax.dot_general(a, b, (((1,), (0,)), ((), ())), preferred_element_type=F32)


def dot_nt(a, b):
    return lax.dot_general(a, b, (((1,), (1,)), ((), ())), preferred_element_type=F32)


def dot_tn(a, b):
    return lax.dot_general(a, b, (((0,), (0,)), ((), ())), preferred_element_type=F32)


class Net:
    def __init__(self, ruler, send_sems, recv_sems):
        self.ruler, self.send_sems, self.recv_sems = ruler, send_sems, recv_sems
        self.groups = {}
        self.lanes = {}
        self.row_bytes = ruler.shape[1] * 2

    def send(self, group, src, dst, device, lane):
        size = 4 if src.dtype == F32 else 2
        for extent in src.shape:
            size *= extent
        group_at = self.groups.setdefault(group, [len(self.groups), 0, False])
        lane_at = self.lanes.setdefault(lane, [len(self.lanes), 0])
        group_at[1] += size
        lane_at[1] += size
        self.device = device
        pltpu.make_async_remote_copy(
            src_ref=src,
            dst_ref=dst,
            send_sem=self.send_sems.at[lane_at[0]],
            recv_sem=self.recv_sems.at[group_at[0]],
            device_id=device,
            device_id_type=MESH,
        ).start()

    def measure(self, size, send_at, recv_at):
        ref = self.ruler.at[pl.ds(0, size // self.row_bytes), :]
        return pltpu.make_async_remote_copy(
            src_ref=ref,
            dst_ref=ref,
            send_sem=self.send_sems.at[send_at],
            recv_sem=self.recv_sems.at[recv_at],
            device_id=self.device,
            device_id_type=MESH,
        )

    def recv(self, group):
        at = self.groups[group]
        assert not at[2]
        at[2] = True
        self.measure(at[1], 0, at[0]).wait_recv()

    def finish(self):
        assert len(self.groups) <= GROUPS and len(self.lanes) <= LANES
        assert all(at[2] for at in self.groups.values())
        for at, size in self.lanes.values():
            self.measure(size, at, 0).wait_send()


def kernel(
    sizes, hidden, w_query, key_input, values, cotangent,
    out_att, out_qg, out_kg, out_vg,
    hf, wf, kb, kf, vb, gb, q32, qf, att, dn, sc, mx, vg32, kg32, kg, vg,
    s_out, s_in, t_out, t_in, b_out, prior, later, pre,
    h4, h4t, dq4, g32, rs_out, rs_in, qg, qsend, qin,
    send_sems, recv_sems, local_sems,
):
    NX, NY, NZ = sizes
    x = lax.axis_index("heads")
    ctx = lax.axis_index("ctx")
    c = ctx % CORES
    z = (ctx // CORES) % NZ
    y = ctx // (CORES * NZ)
    p = 1 - c
    u = y % 2
    pair = y // 2
    py = y + 1 - 2 * u
    qy = NY - 1 - y
    ry = NY - 1 - py
    own_y = (y, py, qy, ry)
    e = ((y + 1) // 2) % 2
    T, DX = hidden.shape
    WR, NALL = w_query.shape
    D = NX * DX
    CH = CORES * WR
    KY = NZ * CH
    KH = 2 * KY
    CT = CORES * T
    XM, ZM = NX // 2, NZ // 2
    BOTH = (1, -1)
    BLOCKS = (0, 1)

    def at(y_, z_, core):
        return (x, (y_ * NZ + z_) * CORES + core)

    def dev_x(step):
        return ((x + step + NX) % NX, ctx)

    def dev_z(step):
        return at(y, (z + step + NZ) % NZ, c)

    partner = at(y, z, p)
    pair_same = at(py, z, c)
    pair_other = at(py, z, p)
    across = at(qy, z, c)
    net = Net(wf, send_sems, recv_sems)

    def rows_of(start, size, unit=16):
        return pl.ds(pl.multiple_of(start, unit), size)

    def head_cols(core, parity, width):
        return pl.ds(pl.multiple_of((2 * core + parity) * width, width), width)

    def split(total, part, top=None):
        top = total // 2 if top is None else top
        return {"full": (0, total), "top": (0, top), "bot": (top, total - top)}[part]

    def part_of(direction, d, most):
        if d < most:
            return "full"
        return "top" if direction > 0 else "bot"

    def fresh(r, most):
        if r == 0:
            return [0]
        return [-r, r] if r < most else [most]

    w_mine = rows_of((y * NZ + z) * CH + c * WR, WR)
    t_mine = rows_of(c * T, T)
    x_mine = pl.ds(pl.multiple_of(x * DX, DX), DX)
    moves = [
        ("w", w_query.at[:, head_cols(c, e, FEAT)], wf.at[w_mine, :]),
        ("h", hidden, hf.at[t_mine, x_mine]),
        ("k0", key_input.at[:, head_cols(c, e, FEAT)], kb.at[0, t_mine, :]),
        ("k2", key_input.at[:, head_cols(c, 1 - e, FEAT)], kb.at[2, t_mine, :]),
        ("v0", values.at[:, head_cols(c, e, HEAD_DIM)], vb.at[0, t_mine, :]),
        ("v2", values.at[:, head_cols(c, 1 - e, HEAD_DIM)], vb.at[2, t_mine, :]),
        ("g", cotangent.at[:, head_cols(c, e, HEAD_DIM)], gb.at[0, t_mine, :]),
    ]
    local = {}
    for n, (name, src, dst) in enumerate(moves):
        local[name] = pltpu.make_async_copy(src, dst, local_sems.at[n])
        local[name].start()
    barrier = pltpu.get_barrier_semaphore()
    friends = [partner, pair_same, pair_other, across, at(ry, z, c)]
    friends += [dev_x(d) for d in sorted({1, NX - 1})]
    friends += [dev_z(d) for d in range(1, NZ)]
    for friend in friends:
        pl.semaphore_signal(barrier, inc=1, device_id=friend, device_id_type=MESH)
    pl.semaphore_wait(barrier, len(friends))
    pair_cores = ((c, pair_same), (p, pair_other))
    for core, to in pair_cores:
        net.send(("w", 1), w_query.at[:, head_cols(core, 1 - e, FEAT)], wf.at[w_mine, :], to, "in")
    net.send(("w", 0), w_query.at[:, head_cols(p, e, FEAT)], wf.at[w_mine, :], partner, "in")
    net.send("h1", hidden, hf.at[rows_of(CT + c * T, T), x_mine], pair_same, "in")
    for slot, parity in ((0, e), (2, 1 - e)):
        net.send(
            "kv0", key_input.at[:, head_cols(p, parity, FEAT)], kb.at[slot, t_mine, :], partner, "in"
        )
        net.send(
            "kv0", values.at[:, head_cols(p, parity, HEAD_DIM)], vb.at[slot, t_mine, :], partner, "in"
        )
    net.send("h0", hidden, hf.at[t_mine, x_mine], partner, "in")
    for core, to in pair_cores:
        cut, narrow = head_cols(core, 1 - e, FEAT), head_cols(core, 1 - e, HEAD_DIM)
        net.send("kv1", key_input.at[:, cut], kb.at[1, t_mine, :], to, "in")
        net.send("kv1", values.at[:, narrow], vb.at[1, t_mine, :], to, "in")
        net.send("kv1", cotangent.at[:, narrow], gb.at[1, t_mine, :], to, "in")
    net.send("g0", cotangent.at[:, head_cols(p, e, HEAD_DIM)], gb.at[0, t_mine, :], partner, "in")

    A_ROWS = CH * A_EIGHTHS // 8
    B_ROWS = CH - A_ROWS
    A_TOP, B_TOP = A_ROWS * A_FIFTHS // 5, B_ROWS // 3

    def w_piece(stream, which, rel_z, part):
        total, first = (A_ROWS, A_TOP) if stream == "A" else (B_ROWS, B_TOP)
        start, size = split(total, part, first)
        if stream == "B":
            start = start + A_ROWS
        return wf.at[rows_of((own_y[which] * NZ + (z + rel_z + NZ) % NZ) * CH + start, size), :]

    def w_ring(stream, which, d):
        for s in BOTH:
            piece = w_piece(stream, which, -s * (d - 1), part_of(s, d, ZM))
            net.send((stream, which, d), piece, piece, dev_z(s), ("w", which % 2))

    def w_across(stream, b, rel):
        piece = w_piece(stream, b, rel, "full")
        net.send((stream, "across", b), piece, piece, across, ("w", b))

    def w_next(stream, which, d):
        net.recv((stream, which, d))
        if d < ZM:
            w_ring(stream, which, d + 1)

    def w_begin(b):
        if b == 0:
            local["w"].wait()
        net.recv(("w", b))
        w_ring("A", b, 1)
        w_across("B", b, 0)
        w_across("A", b, 0)
        w_ring("B", b, 1)

    def w_a(b, r):
        w_next("A", b, r)
        for rel in fresh(r, ZM):
            w_across("A", b, rel)

    def w_turn(b):
        net.recv(("B", "across", b))
        w_ring("B", 2 + b, 1)

    def w_last(b):
        net.recv(("A", "across", b))

    def x_ring(name, piece, stage, lane):
        for s in BOTH:
            first, second = ("top", "bot") if s > 0 else ("bot", "top")
            back = 0 if stage < 3 else -s
            ref = piece(back, second if stage == 2 else first)
            net.send((*name, stage), ref, ref, dev_x(s), lane)

    def x_relay(name, piece, stage, lane):
        for s in BOTH:
            first, second = ("top", "bot") if s > 0 else ("bot", "top")
            ref = piece(-s if stage < 3 else -2 * s, second if stage == 2 else first)
            net.send(name, ref, ref, partner, lane)

    def x_begin(name, piece, lane):
        x_ring(name, piece, 1, lane)
        if XM > 1:
            x_ring(name, piece, 2, lane)

    def x_step(name, relay, piece, stage, lane):
        net.recv((*name, stage))
        if stage == 1 and XM > 1:
            x_ring(name, piece, 3, lane)
        x_relay(relay, piece, stage, lane)

    def h_piece(b):
        def piece(rel_x, part):
            start, size = split(T, part)
            xs = (x + rel_x + NX) % NX
            return hf.at[
                rows_of(b * CT + c * T + start, size), pl.ds(pl.multiple_of(xs * DX, DX), DX)
            ]

        return piece

    def h_begin(b):
        if b == 0:
            local["h"].wait()
        else:
            net.recv("h1")
        x_begin(("hx", b), h_piece(b), ("h", b))
        if b == 1:
            piece = h_piece(b)(0, "full")
            net.send(("hp", b), piece, piece, partner, ("h", b))

    def h_step(b, stage):
        x_step(("hx", b), ("hp", b), h_piece(b), stage, ("h", b))

    def h_all(b):
        if b == 0:
            net.recv("h0")
        net.recv(("hp", b))

    SR = FEAT // NZ

    def slice_at(k):
        return pl.ds(pl.multiple_of(k * SR, SR), SR)

    FAR_FIRST = sorted(range(1, NZ), key=lambda o: -min(o, NZ - o))

    def scan_start(kind):
        for o in FAR_FIRST:
            src = s_out.at[kind, :, slice_at((z + o) % NZ), :]
            net.send((kind, "s"), src, s_in.at[kind, o], dev_z(o), ("scan", kind))

    def scan_totals(kind):
        own = s_out[kind, :, slice_at(z), :].astype(F32)
        total = own
        net.recv((kind, "s"))
        pre[z] = own
        for o in range(1, NZ):
            came = s_in[kind, o].astype(F32)
            total = total + came
            pre[(z - o + NZ) % NZ] = came
        t_out[kind] = total.astype(BF16)
        if kind == 0:
            for n, to in ((1, pair_same), (2, across), (3, at(ry, z, c))):
                net.send((kind, "t"), t_out.at[kind], t_in.at[kind, n], to, ("scan", kind))
        else:
            net.send((kind, "t"), t_out.at[kind], t_in.at[kind, 2], across, ("scan", kind))

    def scan_back(kind, result):
        net.recv((kind, "t"))
        zero = jnp.zeros((SR, HEAD_DIM), F32)
        if kind == 0:
            offset = [zero, zero]
            for n in (1, 2, 3):
                for half in (0, 1):
                    term = t_in[0, n, half].astype(F32)
                    offset[half] = offset[half] + jnp.where(own_y[n] < y, term, 0.0)
        else:
            sums = (
                t_out[1, 0].astype(F32),
                t_out[1, 1].astype(F32),
                t_in[1, 2, 0].astype(F32),
                t_in[1, 2, 1].astype(F32),
            )
            offset = []
            for b in BLOCKS:
                total = zero
                for n in range(4):
                    if n != b:
                        total = total + jnp.where(own_y[n] > own_y[b], sums[n], 0.0)
                offset.append(total)
        for half in (0, 1):
            running = offset[half]
            for k in range(NZ) if kind == 0 else reversed(range(NZ)):
                b_out[kind, k, half] = running.astype(BF16)
                running = running + pre[k, half]
        for o in FAR_FIRST:
            src = b_out.at[kind, (z + o) % NZ]
            dst = result.at[pl.ds(0, 2), slice_at(z), :]
            net.send((kind, "b"), src, dst, dev_z(o), ("scan", kind))
        result[pl.ds(0, 2), slice_at(z), :] = b_out[kind, z]

    PT = T // NX

    def quarter(rel_x):
        xs = (x + rel_x + NX) % NX
        return pl.ds(pl.multiple_of(xs * PT, PT), PT)

    def h4_start():
        src = hf.at[
            rows_of(c * T + x * PT, PT), pl.ds(pl.multiple_of((1 - pair) * KH, KH), KH)
        ]
        net.send(("h4", 0), src, h4.at[0, c, quarter(0), :], across, "h4")

    def h4_piece(j):
        def piece(rel_x, part):
            start, size = {"full": (0, KH), "top": (0, KH // 2), "bot": (KH // 2, KH // 2)}[part]
            return h4.at[j, c, quarter(rel_x), pl.ds(start, size)]

        return piece

    def h4_begin(j):
        net.recv(("h4", j))
        x_begin(("h4x", j), h4_piece(j), "h4")
        mine = h4_piece(j)(0, "full")
        if j == 0:
            net.send(("h4", 1), mine, h4_piece(1)(0, "full"), pair_same, "h4")
        net.send(("h4p", j), mine, mine, partner, "h4")

    def h4_step(j, stage):
        x_step(("h4x", j), ("h4p", j), h4_piece(j), stage, "h4")

    WIDE = 256

    def h4_turn_own():
        for k in range(KH // WIDE):
            cols = pl.ds(pl.multiple_of(pair * KH + k * WIDE, WIDE), WIDE)
            h4t[k * WIDE : (k + 1) * WIDE, 0 : 2 * CT] = hf[:, cols].T

    def h4_turn(j):
        net.recv(("h4p", j))
        for k in range(KH // WIDE):
            cut = slice(k * WIDE, (k + 1) * WIDE)
            h4t[cut, (2 + j) * CT : (3 + j) * CT] = h4[j, :, :, cut].reshape(CT, WIDE).T

    def project(b, part):
        start, size = (pair * KH, KH) if part == 0 else (own_y[1 + part] * KY, KY)
        rows = pl.ds(pl.multiple_of(start, KY), size)
        block = slice(b * CT, (b + 1) * CT)
        product = dot_nn(hf[block, rows], wf[rows, :])
        q32[block, :] = product if part == 0 else q32[block, :] + product

    causal = lax.broadcasted_iota(jnp.int32, (CT, CT), 0) >= lax.broadcasted_iota(
        jnp.int32, (CT, CT), 1
    )

    def attend(b):
        if b == 1:
            net.recv("prior")
        proj = q32[b * CT : (b + 1) * CT, :]
        feats = jnp.maximum(proj, 0.0).astype(BF16)
        qf[b] = feats
        keys, vals = kf[b], vb[b]
        state = prior[e] if b == 0 else prior[2]
        scores = jnp.where(causal, dot_nt(feats, keys), 0.0).astype(BF16)
        sc[b] = scores
        numer = dot_nn(scores, vals) + dot_nn(feats, state)
        inv = lax.rsqrt(jnp.mean(numer * numer, axis=-1, keepdims=True) + EPSILON)
        normed = numer * inv
        att[b] = normed.astype(BF16)
        grad = gb[b].astype(F32)
        d_num = (inv * (grad - normed * jnp.mean(grad * normed, axis=-1, keepdims=True))).astype(BF16)
        dn[b] = d_num
        mixed = jnp.where(causal, dot_nt(d_num, vals), 0.0).astype(BF16)
        mx[b] = mixed
        d_feat = dot_nn(mixed, keys) + dot_nt(d_num, state)
        d_q = jnp.where(proj > 0, d_feat, 0.0).astype(BF16)
        mine = slice(b * CT, (b + 1) * CT)
        dq4[mine, :] = d_q
        theirs = slice((2 + b) * CT, (3 + b) * CT)
        if b == 0:
            net.send(("dq", 0), dq4.at[mine, :], dq4.at[theirs, :], across, "dq")
        else:
            for h in (0, 1):
                cols = half_cols(h)
                net.send(("dq", 1, h), dq4.at[mine, cols], dq4.at[theirs, cols], across, "dq")

    def state_send(b):
        s_out[1, b] = dot_tn(qf[b], dn[b]).astype(BF16)
        for o in FAR_FIRST:
            src = s_out.at[1, b, slice_at((z + o) % NZ), :]
            net.send((1, "s"), src, s_in.at[1, o, b], dev_z(o), ("scan", 1))

    def states():
        for name in ("k0", "k2", "v0", "v2"):
            local[name].wait()
        net.recv("kv0")
        kf[0] = jnp.maximum(kb[0], jnp.zeros_like(kb[0]))
        s_out[0, e] = dot_tn(kf[0], vb[0]).astype(BF16)
        s_out[0, 1 - e] = dot_tn(jnp.maximum(kb[2], jnp.zeros_like(kb[2])), vb[2]).astype(BF16)
        scan_start(0)

    def prior_send():
        net.recv((0, "b"))
        net.send("prior", prior.at[1 - e], prior.at[2], pair_same, "prior")

    def keys_in():
        net.recv("kv1")
        kf[1] = jnp.maximum(kb[1], jnp.zeros_like(kb[1]))

    def grads_in():
        local["g"].wait()
        net.recv("g0")

    def block_parts(b):
        vg32[b] = dot_tn(sc[b], dn[b])
        kg32[b] = dot_tn(mx[b], qf[b])

    def state_parts(b):
        state = later[b]
        vg[b] = (vg32[b] + dot_nn(kf[b], state)).astype(BF16)
        d_key = kg32[b] + dot_nt(vb[b], state)
        kg[b] = jnp.where(kb[b] > 0, d_key, 0.0).astype(BF16)

    def part_rows(k):
        return pl.ds(pl.multiple_of(((1 - u) if k == 0 else u) * KY, KY), KY)

    def contract_own(k):
        g32[k] = dot_nn(h4t[part_rows(k), 0 : 2 * CT], dq4[0 : 2 * CT, :])

    REST = slice(2 * CT, 4 * CT)

    def half_cols(h):
        return slice(h * FEAT // 2, (h + 1) * FEAT // 2)

    def contract_far(k, h):
        cols = half_cols(h)
        if k == 0:
            if h == 0:
                net.recv(("dq", 0))
            net.recv(("dq", 1, h))
        to = ((z + ZM) % NZ) * CH
        rows = rows_of(((1 - u) if k == 0 else u) * KY + to, CH)
        far = g32[k, rows_of(to, CH), cols] + dot_nn(h4t[rows, REST], dq4[REST, cols])
        for s in BOTH:
            rows = rs_rows(part_of(s, ZM, ZM))
            rs_out[k, 0 if s > 0 else 1, ZM - 1, rows, cols] = far[rows, :].astype(BF16)
            rs_put(k, h, s, ZM)

    def contract_rest(k, h):
        cols = half_cols(h)
        g32[k, :, cols] = g32[k, :, cols] + dot_nn(h4t[part_rows(k), REST], dq4[REST, cols])

    def rs_rows(part):
        start, size = split(CH, part, CH * RS_EIGHTHS // 8)
        return slice(start, start + size)

    def rs_put(k, h, s, d):
        way, rows, cols = 0 if s > 0 else 1, rs_rows(part_of(s, d, ZM)), half_cols(h)
        net.send(
            ("rs", k, h, d),
            rs_out.at[k, way, d - 1, rows, cols],
            rs_in.at[k, way, d - 1, rows, cols],
            dev_z(s),
            ("rs", k),
        )

    def rs_send(k, h, d):
        cols = half_cols(h)
        net.recv(("rs", k, h, d + 1))
        for s in BOTH:
            rows = rs_rows(part_of(s, d, ZM))
            size = rows.stop - rows.start
            to = (z + s * d + NZ) % NZ
            total = g32[k, rows_of(to * CH + rows.start, size), cols]
            way = 0 if s > 0 else 1
            rs_out[k, way, d - 1, rows, cols] = total.astype(BF16)
            came = rs_rows(part_of(s, d + 1, ZM))
            got = rs_in[k, way, d, came, cols].astype(F32)
            rs_out[k, way, d - 1, came, cols] = (total[came, :] + got).astype(BF16)
            rs_put(k, h, s, d)

    def rs_last(k, h):
        cols = half_cols(h)
        net.recv(("rs", k, h, 1))
        total = g32[k, rows_of(z * CH, CH), cols]
        if ZM > 1:
            total = total + rs_in[k, 0, 0, :, cols].astype(F32) + rs_in[k, 1, 0, :, cols].astype(F32)
        else:
            came = [
                rs_in[k, way, 0, rs_rows(part), cols].astype(F32)
                for way, part in enumerate(("top", "bot"))
            ]
            total = total + jnp.concatenate(came, axis=0)
        at_cols = (2 * c + e) * FEAT + h * (FEAT // 2)
        mine = out_qg.at[:, pl.ds(pl.multiple_of(at_cols, FEAT // 2), FEAT // 2)]

        if k == 0:
            qsend[:, cols] = total.astype(BF16)
            for core, to in pair_cores:
                piece = qsend.at[rows_of(core * WR, WR), cols]
                net.send("qin", piece, qin.at[c, :, cols], to, "out")
        else:
            qg[:, cols] = total
            net.send("qg", qg.at[rows_of(p * WR, WR), cols], mine, partner, "out")
            out_qg[:, pl.ds(pl.multiple_of(at_cols, FEAT // 2), FEAT // 2)] = qg[
                rows_of(c * WR, WR), cols
            ]

    def out_send(name, buf, out, rows, width):
        mine = out.at[:, head_cols(c, e, width)]

        def piece(block, core):
            return buf.at[block, rows_of(core * rows, rows), :]

        net.send(name, piece(1, c), mine, pair_same, "out")
        net.send(name, piece(1, p), mine, pair_other, "out")
        net.send(name, piece(0, p), mine, partner, "out")
        out[:, head_cols(c, e, width)] = buf[0, rows_of(c * rows, rows), :]

    def att_out():
        out_send("att", att, out_att, T, HEAD_DIM)

    def later_parts():
        net.recv((1, "b"))
        for b in BLOCKS:
            state_parts(b)
        out_send("kg", kg, out_kg, T, FEAT)
        out_send("vg", vg, out_vg, T, HEAD_DIM)

    tasks = {
        "w": w_begin,
        "A": w_a,
        "B": lambda which, d: w_next("B", which, d),
        "across": w_turn,
        "last": w_last,
        "h": h_begin,
        "hx": h_step,
        "hp": h_all,
        "state": states,
        "tot": scan_totals,
        "back": lambda kind: scan_back(kind, later if kind else prior),
        "prior": prior_send,
        "kv1": keys_in,
        "g0": grads_in,
        "h4s": h4_start,
        "h4": h4_begin,
        "h4x": h4_step,
        "turnown": h4_turn_own,
        "turn": h4_turn,
        "mm": project,
        "att": attend,
        "s1": state_send,
        "outatt": att_out,
        "blk": block_parts,
        "own": contract_own,
        "far": contract_far,
        "rest": contract_rest,
        "rs": rs_send,
        "rsl": rs_last,
        "later": later_parts,
    }
    for name, *where in ORDER:
        tasks[name](*where)
    for name in ("att", "kg", "vg"):
        net.recv(name)
    net.recv("qin")
    for core in (0, 1):
        out_qg[:, head_cols(core, 1 - e, FEAT)] = qin[core].astype(F32)
    net.recv("qg")
    net.finish()


def write_out(*refs):
    ins, outs, sems = refs[:4], refs[4:8], refs[8]
    copies = [
        pltpu.make_async_copy(src, dst, sems.at[n]) for n, (src, dst) in enumerate(zip(ins, outs))
    ]
    for copy in copies:
        copy.start()
    for copy in copies:
        copy.wait()


def solution(mesh):
    NX, ctx_size = mesh.shape["heads"], mesh.shape["ctx"]
    NY = 4
    NZ = ctx_size // (NY * CORES)
    sizes = (NX, NY, NZ)

    def body(hidden, w_query, key_input, values, cotangent):
        T, DX = hidden.shape
        WR, NALL = w_query.shape
        VALL = values.shape[1]
        D = NX * DX
        CH = CORES * WR
        KY = NZ * CH
        CT = CORES * T
        ZM = NZ // 2
        SR = FEAT // NZ
        any_space = pl.BlockSpec(memory_space=pl.ANY)
        vmem_space = pl.BlockSpec(memory_space=pltpu.VMEM)
        outs = (((T, VALL), BF16), ((WR, NALL), F32), ((T, NALL), BF16), ((T, VALL), BF16))

        def vmem(*shape, dtype=BF16):
            return pltpu.VMEM(shape, dtype)

        def run(*refs):
            kernel(sizes, *refs)

        parts = pl.pallas_call(
            run,
            out_shape=tuple(pltpu.VMEM(*of) for of in outs),
            in_specs=[any_space] * 5,
            out_specs=(vmem_space,) * 4,
            scratch_shapes=[
                vmem(2 * CT, D),
                vmem(D, FEAT),
                vmem(3, CT, FEAT),
                vmem(2, CT, FEAT),
                vmem(3, CT, HEAD_DIM),
                vmem(2, CT, HEAD_DIM),
                vmem(2 * CT, FEAT, dtype=F32),
                vmem(2, CT, FEAT),
                vmem(2, CT, HEAD_DIM),
                vmem(2, CT, HEAD_DIM),
                vmem(2, CT, CT),
                vmem(2, CT, CT),
                vmem(2, CT, HEAD_DIM, dtype=F32),
                vmem(2, CT, FEAT, dtype=F32),
                vmem(2, CT, FEAT),
                vmem(2, CT, HEAD_DIM),
                vmem(2, 2, FEAT, HEAD_DIM),
                vmem(2, NZ, 2, SR, HEAD_DIM),
                vmem(2, 2, SR, HEAD_DIM),
                vmem(2, NY, 2, SR, HEAD_DIM),
                vmem(2, NZ, 2, SR, HEAD_DIM),
                vmem(3, FEAT, HEAD_DIM),
                vmem(2, FEAT, HEAD_DIM),
                vmem(NZ, 2, SR, HEAD_DIM, dtype=F32),
                vmem(2, CORES, T, 2 * KY),
                vmem(2 * KY, 4 * CT),
                vmem(4 * CT, FEAT),
                vmem(2, KY, FEAT, dtype=F32),
                vmem(2, 2, ZM, CH, FEAT),
                vmem(2, 2, ZM, CH, FEAT),
                vmem(CH, FEAT, dtype=F32),
                vmem(CH, FEAT),
                vmem(CORES, WR, FEAT),
                pltpu.SemaphoreType.DMA((LANES,)),
                pltpu.SemaphoreType.DMA((GROUPS,)),
                pltpu.SemaphoreType.DMA((LOCALS,)),
            ],
            compiler_params=pltpu.CompilerParams(
                collective_id=0, has_side_effects=True, vmem_limit_bytes=60000 * 1024
            ),
        )(hidden, w_query, key_input, values, cotangent)
        return pl.pallas_call(
            write_out,
            out_shape=tuple(jax.ShapeDtypeStruct(*of) for of in outs),
            in_specs=[vmem_space] * 4,
            out_specs=(any_space,) * 4,
            scratch_shapes=[pltpu.SemaphoreType.DMA((4,))],
        )(*[pltpu.with_memory_space_constraint(part, pltpu.VMEM) for part in parts])

    spec = P("ctx", "heads")
    return jax.shard_map(
        body, mesh=mesh, in_specs=(spec,) * 5, out_specs=(spec,) * 4, check_vma=False
    )
```

```python
import jax
import jax.numpy as jnp
from jax import lax
from jax.experimental import pallas as pl
from jax.experimental.pallas import tpu as pltpu
from jax.sharding import PartitionSpec as P

HEAD_DIM = 128
FEAT = 256
CORES = 2
EPSILON = 1e-06
MESH = pl.DeviceIdType.MESH
F32 = jnp.float32
BF16 = jnp.bfloat16
GROUPS = 100
LANES = 13
LOCALS = 7
A_EIGHTHS = 5
A_FIFTHS = 1
RS_EIGHTHS = 2

ORDER = (
    ('h', 0),
    ('w', 0),
    ('state',),
    ('g0',),
    ('w', 1),
    ('across', 0),
    ('A', 0, 1),
    ('B', 0, 1),
    ('hx', 0, 1),
    ('across', 1),
    ('hx', 0, 2),
    ('A', 1, 1),
    ('h', 1),
    ('B', 1, 1),
    ('B', 2, 1),
    ('tot', 0),
    ('A', 0, 2),
    ('hx', 0, 3),
    ('B', 0, 2),
    ('h4s',),
    ('B', 3, 1),
    ('A', 1, 2),
    ('hp', 0),
    ('B', 1, 2),
    ('B', 2, 2),
    ('hx', 1, 1),
    ('kv1',),
    ('A', 0, 3),
    ('back', 0),
    ('B', 0, 3),
    ('B', 3, 2),
    ('A', 1, 3),
    ('hx', 1, 2),
    ('B', 1, 3),
    ('B', 2, 3),
    ('h4', 0),
    ('A', 0, 4),
    ('hx', 1, 3),
    ('h4x', 0, 1),
    ('B', 0, 4),
    ('hp', 1),
    ('turnown',),
    ('A', 1, 4),
    ('B', 3, 3),
    ('B', 1, 4),
    ('mm', 0, 0),
    ('B', 2, 4),
    ('h4', 1),
    ('h4x', 0, 2),
    ('prior',),
    ('mm', 1, 0),
    ('last', 0),
    ('mm', 0, 1),
    ('h4x', 0, 3),
    ('B', 3, 4),
    ('mm', 1, 1),
    ('last', 1),
    ('mm', 0, 2),
    ('att', 0),
    ('s1', 0),
    ('h4x', 1, 1),
    ('mm', 1, 2),
    ('att', 1),
    ('s1', 1),
    ('h4x', 1, 2),
    ('own', 0),
    ('own', 1),
    ('turn', 0),
    ('h4x', 1, 3),
    ('outatt',),
    ('blk', 0),
    ('blk', 1),
    ('turn', 1),
    ('far', 0, 0),
    ('far', 1, 0),
    ('tot', 1),
    ('far', 0, 1),
    ('far', 1, 1),
    ('rest', 0, 0),
    ('rest', 0, 1),
    ('back', 1),
    ('rest', 1, 0),
    ('rest', 1, 1),
    ('rs', 0, 0, 3),
    ('rs', 0, 1, 3),
    ('rs', 1, 0, 3),
    ('rs', 1, 1, 3),
    ('rs', 0, 0, 2),
    ('rs', 0, 1, 2),
    ('rs', 1, 0, 2),
    ('rs', 1, 1, 2),
    ('later',),
    ('rs', 0, 0, 1),
    ('rs', 0, 1, 1),
    ('rs', 1, 0, 1),
    ('rs', 1, 1, 1),
    ('rsl', 0, 0),
    ('rsl', 0, 1),
    ('rsl', 1, 0),
    ('rsl', 1, 1),
)


def dot_nn(a, b):
    return lax.dot_general(a, b, (((1,), (0,)), ((), ())), preferred_element_type=F32)


def dot_nt(a, b):
    return lax.dot_general(a, b, (((1,), (1,)), ((), ())), preferred_element_type=F32)


def dot_tn(a, b):
    return lax.dot_general(a, b, (((0,), (0,)), ((), ())), preferred_element_type=F32)


class Net:
    def __init__(self, ruler, send_sems, recv_sems):
        self.ruler, self.send_sems, self.recv_sems = ruler, send_sems, recv_sems
        self.groups = {}
        self.lanes = {}
        self.row_bytes = ruler.shape[1] * 2

    def send(self, group, src, dst, device, lane):
        size = 4 if src.dtype == F32 else 2
        for extent in src.shape:
            size *= extent
        group_at = self.groups.setdefault(group, [len(self.groups), 0, False])
        lane_at = self.lanes.setdefault(lane, [len(self.lanes), 0])
        group_at[1] += size
        lane_at[1] += size
        self.device = device
        pltpu.make_async_remote_copy(
            src_ref=src,
            dst_ref=dst,
            send_sem=self.send_sems.at[lane_at[0]],
            recv_sem=self.recv_sems.at[group_at[0]],
            device_id=device,
            device_id_type=MESH,
        ).start()

    def measure(self, size, send_at, recv_at):
        ref = self.ruler.at[pl.ds(0, size // self.row_bytes), :]
        return pltpu.make_async_remote_copy(
            src_ref=ref,
            dst_ref=ref,
            send_sem=self.send_sems.at[send_at],
            recv_sem=self.recv_sems.at[recv_at],
            device_id=self.device,
            device_id_type=MESH,
        )

    def recv(self, group):
        at = self.groups[group]
        assert not at[2]
        at[2] = True
        self.measure(at[1], 0, at[0]).wait_recv()

    def finish(self):
        assert len(self.groups) <= GROUPS and len(self.lanes) <= LANES
        assert all(at[2] for at in self.groups.values())
        for at, size in self.lanes.values():
            self.measure(size, at, 0).wait_send()


def kernel(
    sizes, hidden, w_query, key_input, values, cotangent,
    out_att, out_qg, out_kg, out_vg,
    hf, wf, kb, kf, vb, gb, q32, qf, att, dn, sc, mx, vg32, kg32, kg, vg,
    s_out, s_in, t_out, t_in, b_out, prior, later, pre,
    h4, h4t, dq4, g32, rs_out, rs_in, qg, qsend, qin,
    send_sems, recv_sems, local_sems,
):
    NX, NY, NZ = sizes
    x = lax.axis_index("heads")
    ctx = lax.axis_index("ctx")
    c = ctx % CORES
    z = (ctx // CORES) % NZ
    y = ctx // (CORES * NZ)
    p = 1 - c
    u = y % 2
    pair = y // 2
    py = y + 1 - 2 * u
    qy = NY - 1 - y
    ry = NY - 1 - py
    own_y = (y, py, qy, ry)
    e = ((y + 1) // 2) % 2
    T, DX = hidden.shape
    WR, NALL = w_query.shape
    D = NX * DX
    CH = CORES * WR
    KY = NZ * CH
    KH = 2 * KY
    CT = CORES * T
    XM, ZM = NX // 2, NZ // 2
    BOTH = (1, -1)
    BLOCKS = (0, 1)

    def at(y_, z_, core):
        return (x, (y_ * NZ + z_) * CORES + core)

    def dev_x(step):
        return ((x + step + NX) % NX, ctx)

    def dev_z(step):
        return at(y, (z + step + NZ) % NZ, c)

    partner = at(y, z, p)
    pair_same = at(py, z, c)
    pair_other = at(py, z, p)
    across = at(qy, z, c)
    net = Net(wf, send_sems, recv_sems)

    def rows_of(start, size, unit=16):
        return pl.ds(pl.multiple_of(start, unit), size)

    def head_cols(core, parity, width):
        return pl.ds(pl.multiple_of((2 * core + parity) * width, width), width)

    def split(total, part, top=None):
        top = total // 2 if top is None else top
        return {"full": (0, total), "top": (0, top), "bot": (top, total - top)}[part]

    def part_of(direction, d, most):
        if d < most:
            return "full"
        return "top" if direction > 0 else "bot"

    def fresh(r, most):
        if r == 0:
            return [0]
        return [-r, r] if r < most else [most]

    w_mine = rows_of((y * NZ + z) * CH + c * WR, WR)
    t_mine = rows_of(c * T, T)
    x_mine = pl.ds(pl.multiple_of(x * DX, DX), DX)
    moves = [
        ("w", w_query.at[:, head_cols(c, e, FEAT)], wf.at[w_mine, :]),
        ("h", hidden, hf.at[t_mine, x_mine]),
        ("k0", key_input.at[:, head_cols(c, e, FEAT)], kb.at[0, t_mine, :]),
        ("k2", key_input.at[:, head_cols(c, 1 - e, FEAT)], kb.at[2, t_mine, :]),
        ("v0", values.at[:, head_cols(c, e, HEAD_DIM)], vb.at[0, t_mine, :]),
        ("v2", values.at[:, head_cols(c, 1 - e, HEAD_DIM)], vb.at[2, t_mine, :]),
        ("g", cotangent.at[:, head_cols(c, e, HEAD_DIM)], gb.at[0, t_mine, :]),
    ]
    local = {}
    for n, (name, src, dst) in enumerate(moves):
        local[name] = pltpu.make_async_copy(src, dst, local_sems.at[n])
        local[name].start()
    barrier = pltpu.get_barrier_semaphore()
    friends = [partner, pair_same, pair_other, across, at(ry, z, c)]
    friends += [dev_x(d) for d in sorted({1, NX - 1})]
    friends += [dev_z(d) for d in range(1, NZ)]
    for friend in friends:
        pl.semaphore_signal(barrier, inc=1, device_id=friend, device_id_type=MESH)
    pl.semaphore_wait(barrier, len(friends))
    pair_cores = ((c, pair_same), (p, pair_other))
    for core, to in pair_cores:
        net.send(("w", 1), w_query.at[:, head_cols(core, 1 - e, FEAT)], wf.at[w_mine, :], to, "in")
    net.send(("w", 0), w_query.at[:, head_cols(p, e, FEAT)], wf.at[w_mine, :], partner, "in")
    net.send("h1", hidden, hf.at[rows_of(CT + c * T, T), x_mine], pair_same, "in")
    for slot, parity in ((0, e), (2, 1 - e)):
        net.send(
            "kv0", key_input.at[:, head_cols(p, parity, FEAT)], kb.at[slot, t_mine, :], partner, "in"
        )
        net.send(
            "kv0", values.at[:, head_cols(p, parity, HEAD_DIM)], vb.at[slot, t_mine, :], partner, "in"
        )
    net.send("h0", hidden, hf.at[t_mine, x_mine], partner, "in")
    for core, to in pair_cores:
        cut, narrow = head_cols(core, 1 - e, FEAT), head_cols(core, 1 - e, HEAD_DIM)
        net.send("kv1", key_input.at[:, cut], kb.at[1, t_mine, :], to, "in")
        net.send("kv1", values.at[:, narrow], vb.at[1, t_mine, :], to, "in")
        net.send("kv1", cotangent.at[:, narrow], gb.at[1, t_mine, :], to, "in")
    net.send("g0", cotangent.at[:, head_cols(p, e, HEAD_DIM)], gb.at[0, t_mine, :], partner, "in")

    A_ROWS = CH * A_EIGHTHS // 8
    B_ROWS = CH - A_ROWS
    A_TOP, B_TOP = A_ROWS * A_FIFTHS // 5, B_ROWS // 3

    def w_piece(stream, which, rel_z, part):
        total, first = (A_ROWS, A_TOP) if stream == "A" else (B_ROWS, B_TOP)
        start, size = split(total, part, first)
        if stream == "B":
            start = start + A_ROWS
        return wf.at[rows_of((own_y[which] * NZ + (z + rel_z + NZ) % NZ) * CH + start, size), :]

    def w_ring(stream, which, d):
        for s in BOTH:
            piece = w_piece(stream, which, -s * (d - 1), part_of(s, d, ZM))
            net.send((stream, which, d), piece, piece, dev_z(s), ("w", which % 2))

    def w_across(stream, b, rel):
        piece = w_piece(stream, b, rel, "full")
        net.send((stream, "across", b), piece, piece, across, ("w", b))

    def w_next(stream, which, d):
        net.recv((stream, which, d))
        if d < ZM:
            w_ring(stream, which, d + 1)

    def w_begin(b):
        if b == 0:
            local["w"].wait()
        net.recv(("w", b))
        w_ring("A", b, 1)
        w_across("B", b, 0)
        w_across("A", b, 0)
        w_ring("B", b, 1)

    def w_a(b, r):
        w_next("A", b, r)
        for rel in fresh(r, ZM):
            w_across("A", b, rel)

    def w_turn(b):
        net.recv(("B", "across", b))
        w_ring("B", 2 + b, 1)

    def w_last(b):
        net.recv(("A", "across", b))

    def x_ring(name, piece, stage, lane):
        for s in BOTH:
            first, second = ("top", "bot") if s > 0 else ("bot", "top")
            back = 0 if stage < 3 else -s
            ref = piece(back, second if stage == 2 else first)
            net.send((*name, stage), ref, ref, dev_x(s), lane)

    def x_relay(name, piece, stage, lane):
        for s in BOTH:
            first, second = ("top", "bot") if s > 0 else ("bot", "top")
            ref = piece(-s if stage < 3 else -2 * s, second if stage == 2 else first)
            net.send(name, ref, ref, partner, lane)

    def x_begin(name, piece, lane):
        x_ring(name, piece, 1, lane)
        if XM > 1:
            x_ring(name, piece, 2, lane)

    def x_step(name, relay, piece, stage, lane):
        net.recv((*name, stage))
        if stage == 1 and XM > 1:
            x_ring(name, piece, 3, lane)
        x_relay(relay, piece, stage, lane)

    def h_piece(b):
        def piece(rel_x, part):
            start, size = split(T, part)
            xs = (x + rel_x + NX) % NX
            return hf.at[
                rows_of(b * CT + c * T + start, size), pl.ds(pl.multiple_of(xs * DX, DX), DX)
            ]

        return piece

    def h_begin(b):
        if b == 0:
            local["h"].wait()
        else:
            net.recv("h1")
        x_begin(("hx", b), h_piece(b), ("h", b))
        if b == 1:
            piece = h_piece(b)(0, "full")
            net.send(("hp", b), piece, piece, partner, ("h", b))

    def h_step(b, stage):
        x_step(("hx", b), ("hp", b), h_piece(b), stage, ("h", b))

    def h_all(b):
        if b == 0:
            net.recv("h0")
        net.recv(("hp", b))

    SR = FEAT // NZ

    def slice_at(k):
        return pl.ds(pl.multiple_of(k * SR, SR), SR)

    FAR_FIRST = sorted(range(1, NZ), key=lambda o: -min(o, NZ - o))

    def scan_start(kind):
        for o in FAR_FIRST:
            src = s_out.at[kind, :, slice_at((z + o) % NZ), :]
            net.send((kind, "s"), src, s_in.at[kind, o], dev_z(o), ("scan", kind))

    def scan_totals(kind):
        own = s_out[kind, :, slice_at(z), :].astype(F32)
        total = own
        net.recv((kind, "s"))
        pre[z] = own
        for o in range(1, NZ):
            came = s_in[kind, o].astype(F32)
            total = total + came
            pre[(z - o + NZ) % NZ] = came
        t_out[kind] = total.astype(BF16)
        if kind == 0:
            for n, to in ((1, pair_same), (2, across), (3, at(ry, z, c))):
                net.send((kind, "t"), t_out.at[kind], t_in.at[kind, n], to, ("scan", kind))
        else:
            net.send((kind, "t"), t_out.at[kind], t_in.at[kind, 2], across, ("scan", kind))

    def scan_back(kind, result):
        net.recv((kind, "t"))
        zero = jnp.zeros((SR, HEAD_DIM), F32)
        if kind == 0:
            offset = [zero, zero]
            for n in (1, 2, 3):
                for half in (0, 1):
                    term = t_in[0, n, half].astype(F32)
                    offset[half] = offset[half] + jnp.where(own_y[n] < y, term, 0.0)
        else:
            sums = (
                t_out[1, 0].astype(F32),
                t_out[1, 1].astype(F32),
                t_in[1, 2, 0].astype(F32),
                t_in[1, 2, 1].astype(F32),
            )
            offset = []
            for b in BLOCKS:
                total = zero
                for n in range(4):
                    if n != b:
                        total = total + jnp.where(own_y[n] > own_y[b], sums[n], 0.0)
                offset.append(total)
        for half in (0, 1):
            running = offset[half]
            for k in range(NZ) if kind == 0 else reversed(range(NZ)):
                b_out[kind, k, half] = running.astype(BF16)
                running = running + pre[k, half]
        for o in FAR_FIRST:
            src = b_out.at[kind, (z + o) % NZ]
            dst = result.at[pl.ds(0, 2), slice_at(z), :]
            net.send((kind, "b"), src, dst, dev_z(o), ("scan", kind))
        result[pl.ds(0, 2), slice_at(z), :] = b_out[kind, z]

    PT = T // NX

    def quarter(rel_x):
        xs = (x + rel_x + NX) % NX
        return pl.ds(pl.multiple_of(xs * PT, PT), PT)

    def h4_start():
        src = hf.at[
            rows_of(c * T + x * PT, PT), pl.ds(pl.multiple_of((1 - pair) * KH, KH), KH)
        ]
        net.send(("h4", 0), src, h4.at[0, c, quarter(0), :], across, "h4")

    def h4_piece(j):
        def piece(rel_x, part):
            start, size = {"full": (0, KH), "top": (0, KH // 2), "bot": (KH // 2, KH // 2)}[part]
            return h4.at[j, c, quarter(rel_x), pl.ds(start, size)]

        return piece

    def h4_begin(j):
        net.recv(("h4", j))
        x_begin(("h4x", j), h4_piece(j), "h4")
        mine = h4_piece(j)(0, "full")
        if j == 0:
            net.send(("h4", 1), mine, h4_piece(1)(0, "full"), pair_same, "h4")
        net.send(("h4p", j), mine, mine, partner, "h4")

    def h4_step(j, stage):
        x_step(("h4x", j), ("h4p", j), h4_piece(j), stage, "h4")

    WIDE = 256

    def h4_turn_own():
        for k in range(KH // WIDE):
            cols = pl.ds(pl.multiple_of(pair * KH + k * WIDE, WIDE), WIDE)
            h4t[k * WIDE : (k + 1) * WIDE, 0 : 2 * CT] = hf[:, cols].T

    def h4_turn(j):
        net.recv(("h4p", j))
        for k in range(KH // WIDE):
            cut = slice(k * WIDE, (k + 1) * WIDE)
            h4t[cut, (2 + j) * CT : (3 + j) * CT] = h4[j, :, :, cut].reshape(CT, WIDE).T

    def project(b, part):
        start, size = (pair * KH, KH) if part == 0 else (own_y[1 + part] * KY, KY)
        rows = pl.ds(pl.multiple_of(start, KY), size)
        block = slice(b * CT, (b + 1) * CT)
        product = dot_nn(hf[block, rows], wf[rows, :])
        q32[block, :] = product if part == 0 else q32[block, :] + product

    causal = lax.broadcasted_iota(jnp.int32, (CT, CT), 0) >= lax.broadcasted_iota(
        jnp.int32, (CT, CT), 1
    )

    def attend(b):
        if b == 1:
            net.recv("prior")
        proj = q32[b * CT : (b + 1) * CT, :]
        feats = jnp.maximum(proj, 0.0).astype(BF16)
        qf[b] = feats
        keys, vals = kf[b], vb[b]
        state = prior[e] if b == 0 else prior[2]
        scores = jnp.where(causal, dot_nt(feats, keys), 0.0).astype(BF16)
        sc[b] = scores
        numer = dot_nn(scores, vals) + dot_nn(feats, state)
        inv = lax.rsqrt(jnp.mean(numer * numer, axis=-1, keepdims=True) + EPSILON)
        normed = numer * inv
        att[b] = normed.astype(BF16)
        grad = gb[b].astype(F32)
        d_num = (inv * (grad - normed * jnp.mean(grad * normed, axis=-1, keepdims=True))).astype(BF16)
        dn[b] = d_num
        mixed = jnp.where(causal, dot_nt(d_num, vals), 0.0).astype(BF16)
        mx[b] = mixed
        d_feat = dot_nn(mixed, keys) + dot_nt(d_num, state)
        d_q = jnp.where(proj > 0, d_feat, 0.0).astype(BF16)
        mine = slice(b * CT, (b + 1) * CT)
        dq4[mine, :] = d_q
        theirs = slice((2 + b) * CT, (3 + b) * CT)
        if b == 0:
            net.send(("dq", 0), dq4.at[mine, :], dq4.at[theirs, :], across, "dq")
        else:
            for h in (0, 1):
                cols = half_cols(h)
                net.send(("dq", 1, h), dq4.at[mine, cols], dq4.at[theirs, cols], across, "dq")

    def state_send(b):
        s_out[1, b] = dot_tn(qf[b], dn[b]).astype(BF16)
        for o in FAR_FIRST:
            src = s_out.at[1, b, slice_at((z + o) % NZ), :]
            net.send((1, "s"), src, s_in.at[1, o, b], dev_z(o), ("scan", 1))

    def states():
        for name in ("k0", "k2", "v0", "v2"):
            local[name].wait()
        net.recv("kv0")
        kf[0] = jnp.maximum(kb[0], jnp.zeros_like(kb[0]))
        s_out[0, e] = dot_tn(kf[0], vb[0]).astype(BF16)
        s_out[0, 1 - e] = dot_tn(jnp.maximum(kb[2], jnp.zeros_like(kb[2])), vb[2]).astype(BF16)
        scan_start(0)

    def prior_send():
        net.recv((0, "b"))
        net.send("prior", prior.at[1 - e], prior.at[2], pair_same, "prior")

    def keys_in():
        net.recv("kv1")
        kf[1] = jnp.maximum(kb[1], jnp.zeros_like(kb[1]))

    def grads_in():
        local["g"].wait()
        net.recv("g0")

    def block_parts(b):
        vg32[b] = dot_tn(sc[b], dn[b])
        kg32[b] = dot_tn(mx[b], qf[b])

    def state_parts(b):
        state = later[b]
        vg[b] = (vg32[b] + dot_nn(kf[b], state)).astype(BF16)
        d_key = kg32[b] + dot_nt(vb[b], state)
        kg[b] = jnp.where(kb[b] > 0, d_key, 0.0).astype(BF16)

    def part_rows(k):
        return pl.ds(pl.multiple_of(((1 - u) if k == 0 else u) * KY, KY), KY)

    def contract_own(k):
        g32[k] = dot_nn(h4t[part_rows(k), 0 : 2 * CT], dq4[0 : 2 * CT, :])

    REST = slice(2 * CT, 4 * CT)

    def half_cols(h):
        return slice(h * FEAT // 2, (h + 1) * FEAT // 2)

    def contract_far(k, h):
        cols = half_cols(h)
        if k == 0:
            if h == 0:
                net.recv(("dq", 0))
            net.recv(("dq", 1, h))
        to = ((z + ZM) % NZ) * CH
        rows = rows_of(((1 - u) if k == 0 else u) * KY + to, CH)
        far = g32[k, rows_of(to, CH), cols] + dot_nn(h4t[rows, REST], dq4[REST, cols])
        for s in BOTH:
            rows = rs_rows(part_of(s, ZM, ZM))
            rs_out[k, 0 if s > 0 else 1, ZM - 1, rows, cols] = far[rows, :].astype(BF16)
            rs_put(k, h, s, ZM)

    def contract_rest(k, h):
        cols = half_cols(h)
        g32[k, :, cols] = g32[k, :, cols] + dot_nn(h4t[part_rows(k), REST], dq4[REST, cols])

    def rs_rows(part):
        start, size = split(CH, part, CH * RS_EIGHTHS // 8)
        return slice(start, start + size)

    def rs_put(k, h, s, d):
        way, rows, cols = 0 if s > 0 else 1, rs_rows(part_of(s, d, ZM)), half_cols(h)
        net.send(
            ("rs", k, h, s, d),
            rs_out.at[k, way, d - 1, rows, cols],
            rs_in.at[k, way, d - 1, rows, cols],
            dev_z(s),
            ("rs", k),
        )

    def rs_send(k, h, d):
        cols = half_cols(h)
        for s in BOTH:
            net.recv(("rs", k, h, s, d + 1))
            rows = rs_rows(part_of(s, d, ZM))
            size = rows.stop - rows.start
            to = (z + s * d + NZ) % NZ
            total = g32[k, rows_of(to * CH + rows.start, size), cols]
            way = 0 if s > 0 else 1
            rs_out[k, way, d - 1, rows, cols] = total.astype(BF16)
            came = rs_rows(part_of(s, d + 1, ZM))
            got = rs_in[k, way, d, came, cols].astype(F32)
            rs_out[k, way, d - 1, came, cols] = (total[came, :] + got).astype(BF16)
            rs_put(k, h, s, d)

    def rs_last(k, h):
        cols = half_cols(h)
        for s in BOTH:
            net.recv(("rs", k, h, s, 1))
        total = g32[k, rows_of(z * CH, CH), cols]
        if ZM > 1:
            total = total + rs_in[k, 0, 0, :, cols].astype(F32) + rs_in[k, 1, 0, :, cols].astype(F32)
        else:
            came = [
                rs_in[k, way, 0, rs_rows(part), cols].astype(F32)
                for way, part in enumerate(("top", "bot"))
            ]
            total = total + jnp.concatenate(came, axis=0)
        at_cols = (2 * c + e) * FEAT + h * (FEAT // 2)
        mine = out_qg.at[:, pl.ds(pl.multiple_of(at_cols, FEAT // 2), FEAT // 2)]

        if k == 0:
            qsend[:, cols] = total.astype(BF16)
            for core, to in pair_cores:
                piece = qsend.at[rows_of(core * WR, WR), cols]
                net.send("qin", piece, qin.at[c, :, cols], to, "out")
        else:
            qg[:, cols] = total
            net.send("qg", qg.at[rows_of(p * WR, WR), cols], mine, partner, "out")
            out_qg[:, pl.ds(pl.multiple_of(at_cols, FEAT // 2), FEAT // 2)] = qg[
                rows_of(c * WR, WR), cols
            ]

    def out_send(name, buf, out, rows, width):
        mine = out.at[:, head_cols(c, e, width)]

        def piece(block, core):
            return buf.at[block, rows_of(core * rows, rows), :]

        net.send(name, piece(1, c), mine, pair_same, "out")
        net.send(name, piece(1, p), mine, pair_other, "out")
        net.send(name, piece(0, p), mine, partner, "out")
        out[:, head_cols(c, e, width)] = buf[0, rows_of(c * rows, rows), :]

    def att_out():
        out_send("att", att, out_att, T, HEAD_DIM)

    def later_parts():
        net.recv((1, "b"))
        for b in BLOCKS:
            state_parts(b)
        out_send("kg", kg, out_kg, T, FEAT)
        out_send("vg", vg, out_vg, T, HEAD_DIM)

    tasks = {
        "w": w_begin,
        "A": w_a,
        "B": lambda which, d: w_next("B", which, d),
        "across": w_turn,
        "last": w_last,
        "h": h_begin,
        "hx": h_step,
        "hp": h_all,
        "state": states,
        "tot": scan_totals,
        "back": lambda kind: scan_back(kind, later if kind else prior),
        "prior": prior_send,
        "kv1": keys_in,
        "g0": grads_in,
        "h4s": h4_start,
        "h4": h4_begin,
        "h4x": h4_step,
        "turnown": h4_turn_own,
        "turn": h4_turn,
        "mm": project,
        "att": attend,
        "s1": state_send,
        "outatt": att_out,
        "blk": block_parts,
        "own": contract_own,
        "far": contract_far,
        "rest": contract_rest,
        "rs": rs_send,
        "rsl": rs_last,
        "later": later_parts,
    }
    for name, *where in ORDER:
        tasks[name](*where)
    for name in ("att", "kg", "vg"):
        net.recv(name)
    net.recv("qin")
    for core in (0, 1):
        out_qg[:, head_cols(core, 1 - e, FEAT)] = qin[core].astype(F32)
    net.recv("qg")
    net.finish()


def write_out(*refs):
    ins, outs, sems = refs[:4], refs[4:8], refs[8]
    copies = [
        pltpu.make_async_copy(src, dst, sems.at[n]) for n, (src, dst) in enumerate(zip(ins, outs))
    ]
    for copy in copies:
        copy.start()
    for copy in copies:
        copy.wait()


def solution(mesh):
    NX, ctx_size = mesh.shape["heads"], mesh.shape["ctx"]
    NY = 4
    NZ = ctx_size // (NY * CORES)
    sizes = (NX, NY, NZ)

    def body(hidden, w_query, key_input, values, cotangent):
        T, DX = hidden.shape
        WR, NALL = w_query.shape
        VALL = values.shape[1]
        D = NX * DX
        CH = CORES * WR
        KY = NZ * CH
        CT = CORES * T
        ZM = NZ // 2
        SR = FEAT // NZ
        any_space = pl.BlockSpec(memory_space=pl.ANY)
        vmem_space = pl.BlockSpec(memory_space=pltpu.VMEM)
        outs = (((T, VALL), BF16), ((WR, NALL), F32), ((T, NALL), BF16), ((T, VALL), BF16))

        def vmem(*shape, dtype=BF16):
            return pltpu.VMEM(shape, dtype)

        def run(*refs):
            kernel(sizes, *refs)

        parts = pl.pallas_call(
            run,
            out_shape=tuple(pltpu.VMEM(*of) for of in outs),
            in_specs=[any_space] * 5,
            out_specs=(vmem_space,) * 4,
            scratch_shapes=[
                vmem(2 * CT, D),
                vmem(D, FEAT),
                vmem(3, CT, FEAT),
                vmem(2, CT, FEAT),
                vmem(3, CT, HEAD_DIM),
                vmem(2, CT, HEAD_DIM),
                vmem(2 * CT, FEAT, dtype=F32),
                vmem(2, CT, FEAT),
                vmem(2, CT, HEAD_DIM),
                vmem(2, CT, HEAD_DIM),
                vmem(2, CT, CT),
                vmem(2, CT, CT),
                vmem(2, CT, HEAD_DIM, dtype=F32),
                vmem(2, CT, FEAT, dtype=F32),
                vmem(2, CT, FEAT),
                vmem(2, CT, HEAD_DIM),
                vmem(2, 2, FEAT, HEAD_DIM),
                vmem(2, NZ, 2, SR, HEAD_DIM),
                vmem(2, 2, SR, HEAD_DIM),
                vmem(2, NY, 2, SR, HEAD_DIM),
                vmem(2, NZ, 2, SR, HEAD_DIM),
                vmem(3, FEAT, HEAD_DIM),
                vmem(2, FEAT, HEAD_DIM),
                vmem(NZ, 2, SR, HEAD_DIM, dtype=F32),
                vmem(2, CORES, T, 2 * KY),
                vmem(2 * KY, 4 * CT),
                vmem(4 * CT, FEAT),
                vmem(2, KY, FEAT, dtype=F32),
                vmem(2, 2, ZM, CH, FEAT),
                vmem(2, 2, ZM, CH, FEAT),
                vmem(CH, FEAT, dtype=F32),
                vmem(CH, FEAT),
                vmem(CORES, WR, FEAT),
                pltpu.SemaphoreType.DMA((LANES,)),
                pltpu.SemaphoreType.DMA((GROUPS,)),
                pltpu.SemaphoreType.DMA((LOCALS,)),
            ],
            compiler_params=pltpu.CompilerParams(
                collective_id=0, has_side_effects=True, vmem_limit_bytes=60000 * 1024
            ),
        )(hidden, w_query, key_input, values, cotangent)
        return pl.pallas_call(
            write_out,
            out_shape=tuple(jax.ShapeDtypeStruct(*of) for of in outs),
            in_specs=[vmem_space] * 4,
            out_specs=(any_space,) * 4,
            scratch_shapes=[pltpu.SemaphoreType.DMA((4,))],
        )(*[pltpu.with_memory_space_constraint(part, pltpu.VMEM) for part in parts])

    spec = P("ctx", "heads")
    return jax.shard_map(
        body, mesh=mesh, in_specs=(spec,) * 5, out_specs=(spec,) * 4, check_vma=False
    )
```

```python
import jax
import jax.numpy as jnp
from jax import lax
from jax.experimental import pallas as pl
from jax.experimental.pallas import tpu as pltpu
from jax.sharding import PartitionSpec as P

HEAD_DIM = 128
FEAT = 256
CORES = 2
EPSILON = 1e-06
MESH = pl.DeviceIdType.MESH
F32 = jnp.float32
BF16 = jnp.bfloat16
GROUPS = 91
LANES = 7
LOCALS = 7
A_EIGHTHS = 5
A_FIFTHS = 1
RS_EIGHTHS = 2

ORDER = (
    ('h', 0),
    ('w', 0),
    ('state',),
    ('g0',),
    ('w', 1),
    ('across', 0),
    ('A', 0, 1),
    ('B', 0, 1),
    ('hx', 0, 1),
    ('across', 1),
    ('hx', 0, 2),
    ('A', 1, 1),
    ('h', 1),
    ('B', 1, 1),
    ('B', 2, 1),
    ('tot', 0),
    ('A', 0, 2),
    ('hx', 0, 3),
    ('B', 0, 2),
    ('h4s',),
    ('B', 3, 1),
    ('A', 1, 2),
    ('hp', 0),
    ('B', 1, 2),
    ('B', 2, 2),
    ('hx', 1, 1),
    ('kv1',),
    ('A', 0, 3),
    ('back', 0),
    ('B', 0, 3),
    ('B', 3, 2),
    ('A', 1, 3),
    ('hx', 1, 2),
    ('B', 1, 3),
    ('B', 2, 3),
    ('h4', 0),
    ('A', 0, 4),
    ('hx', 1, 3),
    ('h4x', 0, 1),
    ('B', 0, 4),
    ('hp', 1),
    ('turnown',),
    ('A', 1, 4),
    ('B', 3, 3),
    ('B', 1, 4),
    ('mm', 0, 0),
    ('B', 2, 4),
    ('h4', 1),
    ('h4x', 0, 2),
    ('prior',),
    ('mm', 1, 0),
    ('last', 0),
    ('mm', 0, 1),
    ('B', 3, 4),
    ('mm', 1, 1),
    ('last', 1),
    ('mm', 0, 2),
    ('att', 0),
    ('s1', 0),
    ('h4x', 1, 1),
    ('h4x', 0, 3),
    ('mm', 1, 2),
    ('att', 1),
    ('s1', 1),
    ('h4x', 1, 2),
    ('own', 0),
    ('own', 1),
    ('turn', 0),
    ('h4x', 1, 3),
    ('outatt',),
    ('blk', 0),
    ('blk', 1),
    ('turn', 1),
    ('far', 0, 0),
    ('far', 1, 0),
    ('tot', 1),
    ('far', 0, 1),
    ('far', 1, 1),
    ('rest', 0, 0),
    ('rest', 0, 1),
    ('rest', 1, 0),
    ('rest', 1, 1),
    ('rs', 0, 0, 3),
    ('rs', 0, 1, 3),
    ('back', 1),
    ('rs', 1, 0, 3),
    ('rs', 1, 1, 3),
    ('rs', 0, 0, 2),
    ('rs', 0, 1, 2),
    ('rs', 1, 0, 2),
    ('rs', 1, 1, 2),
    ('later',),
    ('rs', 0, 0, 1),
    ('rs', 0, 1, 1),
    ('rs', 1, 0, 1),
    ('rs', 1, 1, 1),
    ('rsl', 0, 0),
    ('rsl', 0, 1),
    ('rsl', 1, 0),
    ('rsl', 1, 1),
)


def dot_nn(a, b):
    return lax.dot_general(a, b, (((1,), (0,)), ((), ())), preferred_element_type=F32)


def dot_nt(a, b):
    return lax.dot_general(a, b, (((1,), (1,)), ((), ())), preferred_element_type=F32)


def dot_tn(a, b):
    return lax.dot_general(a, b, (((0,), (0,)), ((), ())), preferred_element_type=F32)


class Net:
    def __init__(self, ruler, send_sems, recv_sems):
        self.ruler, self.send_sems, self.recv_sems = ruler, send_sems, recv_sems
        self.groups = {}
        self.lanes = {}
        self.row_bytes = ruler.shape[1] * 2

    def send(self, group, src, dst, device, lane):
        size = 4 if src.dtype == F32 else 2
        for extent in src.shape:
            size *= extent
        group_at = self.groups.setdefault(group, [len(self.groups), 0, False])
        lane_at = self.lanes.setdefault(lane, [len(self.lanes), 0])
        group_at[1] += size
        lane_at[1] += size
        self.device = device
        pltpu.make_async_remote_copy(
            src_ref=src,
            dst_ref=dst,
            send_sem=self.send_sems.at[lane_at[0]],
            recv_sem=self.recv_sems.at[group_at[0]],
            device_id=device,
            device_id_type=MESH,
        ).start()

    def measure(self, size, send_at, recv_at):
        ref = self.ruler.at[pl.ds(0, size // self.row_bytes), :]
        return pltpu.make_async_remote_copy(
            src_ref=ref,
            dst_ref=ref,
            send_sem=self.send_sems.at[send_at],
            recv_sem=self.recv_sems.at[recv_at],
            device_id=self.device,
            device_id_type=MESH,
        )

    def recv(self, group):
        at = self.groups[group]
        assert not at[2]
        at[2] = True
        self.measure(at[1], 0, at[0]).wait_recv()

    def finish(self):
        assert len(self.groups) <= GROUPS and len(self.lanes) <= LANES
        assert all(at[2] for at in self.groups.values())
        for at, size in self.lanes.values():
            self.measure(size, at, 0).wait_send()


def kernel(
    sizes, hidden, w_query, key_input, values, cotangent,
    out_att, out_qg, out_kg, out_vg,
    hf, wf, kb, kf, vb, gb, q32, qf, att, dn, sc, mx, vg32, kg32, kg, vg,
    s_out, s_in, t_out, t_in, b_out, prior, later, pre,
    h4, h4t, dq4, g32, rs_out, rs_in, qg, qsend, qin,
    send_sems, recv_sems, local_sems,
):
    NX, NY, NZ = sizes
    x = lax.axis_index("heads")
    ctx = lax.axis_index("ctx")
    c = ctx % CORES
    z = (ctx // CORES) % NZ
    y = ctx // (CORES * NZ)
    p = 1 - c
    u = y % 2
    pair = y // 2
    py = y + 1 - 2 * u
    qy = NY - 1 - y
    ry = NY - 1 - py
    own_y = (y, py, qy, ry)
    e = ((y + 1) // 2) % 2
    T, DX = hidden.shape
    WR, NALL = w_query.shape
    D = NX * DX
    CH = CORES * WR
    KY = NZ * CH
    KH = 2 * KY
    CT = CORES * T
    XM, ZM = NX // 2, NZ // 2
    BOTH = (1, -1)
    BLOCKS = (0, 1)

    def at(y_, z_, core):
        return (x, (y_ * NZ + z_) * CORES + core)

    def dev_x(step):
        return ((x + step + NX) % NX, ctx)

    def dev_z(step):
        return at(y, (z + step + NZ) % NZ, c)

    partner = at(y, z, p)
    pair_same = at(py, z, c)
    pair_other = at(py, z, p)
    across = at(qy, z, c)
    net = Net(wf, send_sems, recv_sems)

    def rows_of(start, size, unit=16):
        return pl.ds(pl.multiple_of(start, unit), size)

    def head_cols(core, parity, width):
        return pl.ds(pl.multiple_of((2 * core + parity) * width, width), width)

    def split(total, part, top=None):
        top = total // 2 if top is None else top
        return {"full": (0, total), "top": (0, top), "bot": (top, total - top)}[part]

    def part_of(direction, d, most):
        if d < most:
            return "full"
        return "top" if direction > 0 else "bot"

    def fresh(r, most):
        if r == 0:
            return [0]
        return [-r, r] if r < most else [most]

    w_mine = rows_of((y * NZ + z) * CH + c * WR, WR)
    t_mine = rows_of(c * T, T)
    x_mine = pl.ds(pl.multiple_of(x * DX, DX), DX)
    moves = [
        ("w", w_query.at[:, head_cols(c, e, FEAT)], wf.at[w_mine, :]),
        ("h", hidden, hf.at[t_mine, x_mine]),
        ("k0", key_input.at[:, head_cols(c, e, FEAT)], kb.at[0, t_mine, :]),
        ("k2", key_input.at[:, head_cols(c, 1 - e, FEAT)], kb.at[2, t_mine, :]),
        ("v0", values.at[:, head_cols(c, e, HEAD_DIM)], vb.at[0, t_mine, :]),
        ("v2", values.at[:, head_cols(c, 1 - e, HEAD_DIM)], vb.at[2, t_mine, :]),
        ("g", cotangent.at[:, head_cols(c, e, HEAD_DIM)], gb.at[0, t_mine, :]),
    ]
    local = {}
    for n, (name, src, dst) in enumerate(moves):
        local[name] = pltpu.make_async_copy(src, dst, local_sems.at[n])
        local[name].start()
    barrier = pltpu.get_barrier_semaphore()
    friends = [partner, pair_same, pair_other, across, at(ry, z, c)]
    friends += [dev_x(d) for d in sorted({1, NX - 1})]
    friends += [dev_z(d) for d in range(1, NZ)]
    for friend in friends:
        pl.semaphore_signal(barrier, inc=1, device_id=friend, device_id_type=MESH)
    pl.semaphore_wait(barrier, len(friends))
    pair_cores = ((c, pair_same), (p, pair_other))
    for core, to in pair_cores:
        net.send(("w", 1), w_query.at[:, head_cols(core, 1 - e, FEAT)], wf.at[w_mine, :], to, "io")
    net.send(("w", 0), w_query.at[:, head_cols(p, e, FEAT)], wf.at[w_mine, :], partner, "io")
    net.send("h1", hidden, hf.at[rows_of(CT + c * T, T), x_mine], pair_same, "io")
    for slot, parity in ((0, e), (2, 1 - e)):
        net.send(
            "kv0", key_input.at[:, head_cols(p, parity, FEAT)], kb.at[slot, t_mine, :], partner, "in"
        )
        net.send(
            "kv0", values.at[:, head_cols(p, parity, HEAD_DIM)], vb.at[slot, t_mine, :], partner, "in"
        )
    net.send(("hp", 0), hidden, hf.at[t_mine, x_mine], partner, "io")
    for core, to in pair_cores:
        cut, narrow = head_cols(core, 1 - e, FEAT), head_cols(core, 1 - e, HEAD_DIM)
        net.send("kv1", key_input.at[:, cut], kb.at[1, t_mine, :], to, "io")
        net.send("kv1", values.at[:, narrow], vb.at[1, t_mine, :], to, "io")
        net.send("kv1", cotangent.at[:, narrow], gb.at[1, t_mine, :], to, "io")
    net.send("g0", cotangent.at[:, head_cols(p, e, HEAD_DIM)], gb.at[0, t_mine, :], partner, "io")

    A_ROWS = CH * A_EIGHTHS // 8
    B_ROWS = CH - A_ROWS
    A_TOP, B_TOP = A_ROWS * A_FIFTHS // 5, B_ROWS // 3

    def w_piece(stream, which, rel_z, part):
        total, first = (A_ROWS, A_TOP) if stream == "A" else (B_ROWS, B_TOP)
        start, size = split(total, part, first)
        if stream == "B":
            start = start + A_ROWS
        return wf.at[rows_of((own_y[which] * NZ + (z + rel_z + NZ) % NZ) * CH + start, size), :]

    def w_ring(stream, which, d):
        for s in BOTH:
            piece = w_piece(stream, which, -s * (d - 1), part_of(s, d, ZM))
            net.send((stream, which, d), piece, piece, dev_z(s), "w")

    def w_across(stream, b, rel):
        piece = w_piece(stream, b, rel, "full")
        net.send((stream, "across", b), piece, piece, across, "w")

    def w_next(stream, which, d):
        net.recv((stream, which, d))
        if d < ZM:
            w_ring(stream, which, d + 1)

    def w_begin(b):
        if b == 0:
            local["w"].wait()
        net.recv(("w", b))
        w_ring("A", b, 1)
        w_across("B", b, 0)
        w_across("A", b, 0)
        w_ring("B", b, 1)

    def w_a(b, r):
        w_next("A", b, r)
        for rel in fresh(r, ZM):
            w_across("A", b, rel)

    def w_turn(b):
        net.recv(("B", "across", b))
        w_ring("B", 2 + b, 1)

    def w_last(b):
        net.recv(("A", "across", b))

    def x_ring(name, piece, stage, lane):
        for s in BOTH:
            first, second = ("top", "bot") if s > 0 else ("bot", "top")
            back = 0 if stage < 3 else -s
            ref = piece(back, second if stage == 2 else first)
            net.send((*name, stage), ref, ref, dev_x(s), lane)

    def x_relay(name, piece, stage, lane):
        for s in BOTH:
            first, second = ("top", "bot") if s > 0 else ("bot", "top")
            ref = piece(-s if stage < 3 else -2 * s, second if stage == 2 else first)
            net.send(name, ref, ref, partner, lane)

    def x_begin(name, piece, lane):
        x_ring(name, piece, 1, lane)
        if XM > 1:
            x_ring(name, piece, 2, lane)

    def x_step(name, relay, piece, stage, lane):
        net.recv((*name, stage))
        if stage == 1 and XM > 1:
            x_ring(name, piece, 3, lane)
        x_relay(relay, piece, stage, lane)

    def h_piece(b):
        def piece(rel_x, part):
            start, size = split(T, part)
            xs = (x + rel_x + NX) % NX
            return hf.at[
                rows_of(b * CT + c * T + start, size), pl.ds(pl.multiple_of(xs * DX, DX), DX)
            ]

        return piece

    def h_begin(b):
        if b == 0:
            local["h"].wait()
        else:
            net.recv("h1")
        x_begin(("hx", b), h_piece(b), ("h", b))
        if b == 1:
            piece = h_piece(b)(0, "full")
            net.send(("hp", b), piece, piece, partner, ("h", b))

    def h_step(b, stage):
        x_step(("hx", b), ("hp", b), h_piece(b), stage, ("h", b))

    def h_all(b):
        net.recv(("hp", b))

    SR = FEAT // NZ

    def slice_at(k):
        return pl.ds(pl.multiple_of(k * SR, SR), SR)

    FAR_FIRST = sorted(range(1, NZ), key=lambda o: -min(o, NZ - o))

    def scan_start(kind):
        for o in FAR_FIRST:
            src = s_out.at[kind, :, slice_at((z + o) % NZ), :]
            net.send((kind, "s"), src, s_in.at[kind, o], dev_z(o), "sums")

    def scan_totals(kind):
        own = s_out[kind, :, slice_at(z), :].astype(F32)
        total = own
        net.recv((kind, "s"))
        pre[z] = own
        for o in range(1, NZ):
            came = s_in[kind, o].astype(F32)
            total = total + came
            pre[(z - o + NZ) % NZ] = came
        t_out[kind] = total.astype(BF16)
        if kind == 0:
            for n, to in ((1, pair_same), (2, across), (3, at(ry, z, c))):
                net.send((kind, "t"), t_out.at[kind], t_in.at[kind, n], to, "sums")
        else:
            net.send((kind, "t"), t_out.at[kind], t_in.at[kind, 2], across, "sums")

    def scan_back(kind, result):
        net.recv((kind, "t"))
        zero = jnp.zeros((SR, HEAD_DIM), F32)
        if kind == 0:
            offset = [zero, zero]
            for n in (1, 2, 3):
                for half in (0, 1):
                    term = t_in[0, n, half].astype(F32)
                    offset[half] = offset[half] + jnp.where(own_y[n] < y, term, 0.0)
        else:
            sums = (
                t_out[1, 0].astype(F32),
                t_out[1, 1].astype(F32),
                t_in[1, 2, 0].astype(F32),
                t_in[1, 2, 1].astype(F32),
            )
            offset = []
            for b in BLOCKS:
                total = zero
                for n in range(4):
                    if n != b:
                        total = total + jnp.where(own_y[n] > own_y[b], sums[n], 0.0)
                offset.append(total)
        for half in (0, 1):
            running = offset[half]
            for k in range(NZ) if kind == 0 else reversed(range(NZ)):
                b_out[kind, k, half] = running.astype(BF16)
                running = running + pre[k, half]
        for o in FAR_FIRST:
            src = b_out.at[kind, (z + o) % NZ]
            dst = result.at[pl.ds(0, 2), slice_at(z), :]
            net.send((kind, "b"), src, dst, dev_z(o), "sums")
        result[pl.ds(0, 2), slice_at(z), :] = b_out[kind, z]

    PT = T // NX

    def quarter(rel_x):
        xs = (x + rel_x + NX) % NX
        return pl.ds(pl.multiple_of(xs * PT, PT), PT)

    def h4_start():
        src = hf.at[
            rows_of(c * T + x * PT, PT), pl.ds(pl.multiple_of((1 - pair) * KH, KH), KH)
        ]
        net.send(("h4", 0), src, h4.at[0, c, quarter(0), :], across, "h4")

    def h4_piece(j):
        def piece(rel_x, part):
            start, size = {"full": (0, KH), "top": (0, KH // 2), "bot": (KH // 2, KH // 2)}[part]
            return h4.at[j, c, quarter(rel_x), pl.ds(start, size)]

        return piece

    def h4_begin(j):
        net.recv(("h4", j))
        x_begin(("h4x", j), h4_piece(j), "h4")
        mine = h4_piece(j)(0, "full")
        if j == 0:
            net.send(("h4", 1), mine, h4_piece(1)(0, "full"), pair_same, "h4")
        net.send(("h4p", j), mine, mine, partner, "h4")

    def h4_step(j, stage):
        x_step(("h4x", j), ("h4p", j), h4_piece(j), stage, "h4")

    WIDE = 256

    def h4_turn_own():
        for k in range(KH // WIDE):
            cols = pl.ds(pl.multiple_of(pair * KH + k * WIDE, WIDE), WIDE)
            h4t[k * WIDE : (k + 1) * WIDE, 0 : 2 * CT] = hf[:, cols].T

    def h4_turn(j):
        net.recv(("h4p", j))
        for k in range(KH // WIDE):
            cut = slice(k * WIDE, (k + 1) * WIDE)
            h4t[cut, (2 + j) * CT : (3 + j) * CT] = h4[j, :, :, cut].reshape(CT, WIDE).T

    def project(b, part):
        start, size = (pair * KH, KH) if part == 0 else (own_y[1 + part] * KY, KY)
        rows = pl.ds(pl.multiple_of(start, KY), size)
        block = slice(b * CT, (b + 1) * CT)
        product = dot_nn(hf[block, rows], wf[rows, :])
        q32[block, :] = product if part == 0 else q32[block, :] + product

    causal = lax.broadcasted_iota(jnp.int32, (CT, CT), 0) >= lax.broadcasted_iota(
        jnp.int32, (CT, CT), 1
    )

    def attend(b):
        if b == 1:
            net.recv("prior")
        proj = q32[b * CT : (b + 1) * CT, :]
        feats = jnp.maximum(proj, 0.0).astype(BF16)
        qf[b] = feats
        keys, vals = kf[b], vb[b]
        state = prior[e] if b == 0 else prior[2]
        scores = jnp.where(causal, dot_nt(feats, keys), 0.0).astype(BF16)
        sc[b] = scores
        numer = dot_nn(scores, vals) + dot_nn(feats, state)
        inv = lax.rsqrt(jnp.mean(numer * numer, axis=-1, keepdims=True) + EPSILON)
        normed = numer * inv
        att[b] = normed.astype(BF16)
        grad = gb[b].astype(F32)
        d_num = (inv * (grad - normed * jnp.mean(grad * normed, axis=-1, keepdims=True))).astype(BF16)
        dn[b] = d_num
        mixed = jnp.where(causal, dot_nt(d_num, vals), 0.0).astype(BF16)
        mx[b] = mixed
        d_feat = dot_nn(mixed, keys) + dot_nt(d_num, state)
        d_q = jnp.where(proj > 0, d_feat, 0.0).astype(BF16)
        mine = slice(b * CT, (b + 1) * CT)
        dq4[mine, :] = d_q
        theirs = slice((2 + b) * CT, (3 + b) * CT)
        if b == 0:
            net.send(("dq", 1, 0), dq4.at[mine, :], dq4.at[theirs, :], across, "sums")
        else:
            for h in (0, 1):
                cols = half_cols(h)
                net.send(("dq", 1, h), dq4.at[mine, cols], dq4.at[theirs, cols], across, "sums")

    def state_send(b):
        s_out[1, b] = dot_tn(qf[b], dn[b]).astype(BF16)
        for o in FAR_FIRST:
            src = s_out.at[1, b, slice_at((z + o) % NZ), :]
            net.send((1, "s"), src, s_in.at[1, o, b], dev_z(o), "sums")

    def states():
        for name in ("k0", "k2", "v0", "v2"):
            local[name].wait()
        net.recv("kv0")
        kf[0] = jnp.maximum(kb[0], jnp.zeros_like(kb[0]))
        s_out[0, e] = dot_tn(kf[0], vb[0]).astype(BF16)
        s_out[0, 1 - e] = dot_tn(jnp.maximum(kb[2], jnp.zeros_like(kb[2])), vb[2]).astype(BF16)
        scan_start(0)

    def prior_send():
        net.recv((0, "b"))
        net.send("prior", prior.at[1 - e], prior.at[2], pair_same, "sums")

    def keys_in():
        net.recv("kv1")
        kf[1] = jnp.maximum(kb[1], jnp.zeros_like(kb[1]))

    def grads_in():
        local["g"].wait()
        net.recv("g0")

    def block_parts(b):
        vg32[b] = dot_tn(sc[b], dn[b])
        kg32[b] = dot_tn(mx[b], qf[b])

    def state_parts(b):
        state = later[b]
        vg[b] = (vg32[b] + dot_nn(kf[b], state)).astype(BF16)
        d_key = kg32[b] + dot_nt(vb[b], state)
        kg[b] = jnp.where(kb[b] > 0, d_key, 0.0).astype(BF16)

    def part_rows(k):
        return pl.ds(pl.multiple_of(((1 - u) if k == 0 else u) * KY, KY), KY)

    def contract_own(k):
        g32[k] = dot_nn(h4t[part_rows(k), 0 : 2 * CT], dq4[0 : 2 * CT, :])

    REST = slice(2 * CT, 4 * CT)

    def half_cols(h):
        return slice(h * FEAT // 2, (h + 1) * FEAT // 2)

    def contract_far(k, h):
        cols = half_cols(h)
        if k == 0:
            net.recv(("dq", 1, h))
        to = ((z + ZM) % NZ) * CH
        rows = rows_of(((1 - u) if k == 0 else u) * KY + to, CH)
        far = g32[k, rows_of(to, CH), cols] + dot_nn(h4t[rows, REST], dq4[REST, cols])
        for s in BOTH:
            rows = rs_rows(part_of(s, ZM, ZM))
            rs_out[k, 0 if s > 0 else 1, ZM - 1, rows, cols] = far[rows, :].astype(BF16)
            rs_put(k, h, s, ZM)

    def contract_rest(k, h):
        cols = half_cols(h)
        g32[k, :, cols] = g32[k, :, cols] + dot_nn(h4t[part_rows(k), REST], dq4[REST, cols])

    def rs_rows(part):
        start, size = split(CH, part, CH * RS_EIGHTHS // 8)
        return slice(start, start + size)

    def rs_put(k, h, s, d):
        way, rows, cols = 0 if s > 0 else 1, rs_rows(part_of(s, d, ZM)), half_cols(h)
        net.send(
            ("rs", k, h, s, d) if d > 1 else ("rs", k, h),
            rs_out.at[k, way, d - 1, rows, cols],
            rs_in.at[k, way, d - 1, rows, cols],
            dev_z(s),
            "sums",
        )

    def rs_send(k, h, d):
        cols = half_cols(h)
        for s in BOTH:
            net.recv(("rs", k, h, s, d + 1))
            rows = rs_rows(part_of(s, d, ZM))
            size = rows.stop - rows.start
            to = (z + s * d + NZ) % NZ
            total = g32[k, rows_of(to * CH + rows.start, size), cols]
            way = 0 if s > 0 else 1
            rs_out[k, way, d - 1, rows, cols] = total.astype(BF16)
            came = rs_rows(part_of(s, d + 1, ZM))
            got = rs_in[k, way, d, came, cols].astype(F32)
            rs_out[k, way, d - 1, came, cols] = (total[came, :] + got).astype(BF16)
            rs_put(k, h, s, d)

    def rs_last(k, h):
        cols = half_cols(h)
        net.recv(("rs", k, h))
        total = g32[k, rows_of(z * CH, CH), cols]
        if ZM > 1:
            total = total + rs_in[k, 0, 0, :, cols].astype(F32) + rs_in[k, 1, 0, :, cols].astype(F32)
        else:
            came = [
                rs_in[k, way, 0, rs_rows(part), cols].astype(F32)
                for way, part in enumerate(("top", "bot"))
            ]
            total = total + jnp.concatenate(came, axis=0)
        at_cols = (2 * c + e) * FEAT + h * (FEAT // 2)
        mine = out_qg.at[:, pl.ds(pl.multiple_of(at_cols, FEAT // 2), FEAT // 2)]

        if k == 0:
            qsend[:, cols] = total.astype(BF16)
            for core, to in pair_cores:
                piece = qsend.at[rows_of(core * WR, WR), cols]
                net.send("qin", piece, qin.at[c, :, cols], to, "io")
        else:
            qg[:, cols] = total
            net.send("out", qg.at[rows_of(p * WR, WR), cols], mine, partner, "io")
            out_qg[:, pl.ds(pl.multiple_of(at_cols, FEAT // 2), FEAT // 2)] = qg[
                rows_of(c * WR, WR), cols
            ]

    def out_send(buf, out, rows, width):
        mine = out.at[:, head_cols(c, e, width)]

        def piece(block, core):
            return buf.at[block, rows_of(core * rows, rows), :]

        net.send("out", piece(1, c), mine, pair_same, "io")
        net.send("out", piece(1, p), mine, pair_other, "io")
        net.send("out", piece(0, p), mine, partner, "io")
        out[:, head_cols(c, e, width)] = buf[0, rows_of(c * rows, rows), :]

    def att_out():
        out_send(att, out_att, T, HEAD_DIM)

    def later_parts():
        net.recv((1, "b"))
        for b in BLOCKS:
            state_parts(b)
        out_send(kg, out_kg, T, FEAT)
        out_send(vg, out_vg, T, HEAD_DIM)

    tasks = {
        "w": w_begin,
        "A": w_a,
        "B": lambda which, d: w_next("B", which, d),
        "across": w_turn,
        "last": w_last,
        "h": h_begin,
        "hx": h_step,
        "hp": h_all,
        "state": states,
        "tot": scan_totals,
        "back": lambda kind: scan_back(kind, later if kind else prior),
        "prior": prior_send,
        "kv1": keys_in,
        "g0": grads_in,
        "h4s": h4_start,
        "h4": h4_begin,
        "h4x": h4_step,
        "turnown": h4_turn_own,
        "turn": h4_turn,
        "mm": project,
        "att": attend,
        "s1": state_send,
        "outatt": att_out,
        "blk": block_parts,
        "own": contract_own,
        "far": contract_far,
        "rest": contract_rest,
        "rs": rs_send,
        "rsl": rs_last,
        "later": later_parts,
    }
    for name, *where in ORDER:
        tasks[name](*where)
    net.recv("qin")
    for core in (0, 1):
        out_qg[:, head_cols(core, 1 - e, FEAT)] = qin[core].astype(F32)
    net.recv("out")
    net.finish()


def write_out(*refs):
    ins, outs, sems = refs[:4], refs[4:8], refs[8]
    copies = [
        pltpu.make_async_copy(src, dst, sems.at[n]) for n, (src, dst) in enumerate(zip(ins, outs))
    ]
    for copy in copies:
        copy.start()
    for copy in copies:
        copy.wait()


def solution(mesh):
    NX, ctx_size = mesh.shape["heads"], mesh.shape["ctx"]
    NY = 4
    NZ = ctx_size // (NY * CORES)
    sizes = (NX, NY, NZ)

    def body(hidden, w_query, key_input, values, cotangent):
        T, DX = hidden.shape
        WR, NALL = w_query.shape
        VALL = values.shape[1]
        D = NX * DX
        CH = CORES * WR
        KY = NZ * CH
        CT = CORES * T
        ZM = NZ // 2
        SR = FEAT // NZ
        any_space = pl.BlockSpec(memory_space=pl.ANY)
        vmem_space = pl.BlockSpec(memory_space=pltpu.VMEM)
        outs = (((T, VALL), BF16), ((WR, NALL), F32), ((T, NALL), BF16), ((T, VALL), BF16))

        def vmem(*shape, dtype=BF16):
            return pltpu.VMEM(shape, dtype)

        def run(*refs):
            kernel(sizes, *refs)

        parts = pl.pallas_call(
            run,
            out_shape=tuple(pltpu.VMEM(*of) for of in outs),
            in_specs=[any_space] * 5,
            out_specs=(vmem_space,) * 4,
            scratch_shapes=[
                vmem(2 * CT, D),
                vmem(D, FEAT),
                vmem(3, CT, FEAT),
                vmem(2, CT, FEAT),
                vmem(3, CT, HEAD_DIM),
                vmem(2, CT, HEAD_DIM),
                vmem(2 * CT, FEAT, dtype=F32),
                vmem(2, CT, FEAT),
                vmem(2, CT, HEAD_DIM),
                vmem(2, CT, HEAD_DIM),
                vmem(2, CT, CT),
                vmem(2, CT, CT),
                vmem(2, CT, HEAD_DIM, dtype=F32),
                vmem(2, CT, FEAT, dtype=F32),
                vmem(2, CT, FEAT),
                vmem(2, CT, HEAD_DIM),
                vmem(2, 2, FEAT, HEAD_DIM),
                vmem(2, NZ, 2, SR, HEAD_DIM),
                vmem(2, 2, SR, HEAD_DIM),
                vmem(2, NY, 2, SR, HEAD_DIM),
                vmem(2, NZ, 2, SR, HEAD_DIM),
                vmem(3, FEAT, HEAD_DIM),
                vmem(2, FEAT, HEAD_DIM),
                vmem(NZ, 2, SR, HEAD_DIM, dtype=F32),
                vmem(2, CORES, T, 2 * KY),
                vmem(2 * KY, 4 * CT),
                vmem(4 * CT, FEAT),
                vmem(2, KY, FEAT, dtype=F32),
                vmem(2, 2, ZM, CH, FEAT),
                vmem(2, 2, ZM, CH, FEAT),
                vmem(CH, FEAT, dtype=F32),
                vmem(CH, FEAT),
                vmem(CORES, WR, FEAT),
                pltpu.SemaphoreType.DMA((LANES,)),
                pltpu.SemaphoreType.DMA((GROUPS,)),
                pltpu.SemaphoreType.DMA((LOCALS,)),
            ],
            compiler_params=pltpu.CompilerParams(
                collective_id=0, has_side_effects=True, vmem_limit_bytes=60000 * 1024
            ),
        )(hidden, w_query, key_input, values, cotangent)
        return pl.pallas_call(
            write_out,
            out_shape=tuple(jax.ShapeDtypeStruct(*of) for of in outs),
            in_specs=[vmem_space] * 4,
            out_specs=(any_space,) * 4,
            scratch_shapes=[pltpu.SemaphoreType.DMA((4,))],
        )(*[pltpu.with_memory_space_constraint(part, pltpu.VMEM) for part in parts])

    spec = P("ctx", "heads")
    return jax.shard_map(
        body, mesh=mesh, in_specs=(spec,) * 5, out_specs=(spec,) * 4, check_vma=False
    )
```

```python
import jax
import jax.numpy as jnp
from jax import lax
from jax.experimental import pallas as pl
from jax.experimental.pallas import tpu as pltpu
from jax.sharding import PartitionSpec as P

HEAD_DIM = 128
FEAT = 256
CORES = 2
EPSILON = 1e-06
MESH = pl.DeviceIdType.MESH
F32 = jnp.float32
BF16 = jnp.bfloat16
GROUPS = 91
LANES = 7
LOCALS = 7
A_EIGHTHS = 5
A_FIFTHS = 1
RS_EIGHTHS = 2

ORDER = (
    ('h', 0),
    ('w', 0),
    ('state',),
    ('g0',),
    ('w', 1),
    ('across', 0),
    ('A', 0, 1),
    ('B', 0, 1),
    ('hx', 0, 1),
    ('across', 1),
    ('hx', 0, 2),
    ('A', 1, 1),
    ('h', 1),
    ('B', 1, 1),
    ('B', 2, 1),
    ('tot', 0),
    ('A', 0, 2),
    ('hx', 0, 3),
    ('B', 0, 2),
    ('h4s',),
    ('B', 3, 1),
    ('A', 1, 2),
    ('hp', 0),
    ('B', 1, 2),
    ('B', 2, 2),
    ('hx', 1, 1),
    ('kv1',),
    ('A', 0, 3),
    ('back', 0),
    ('B', 0, 3),
    ('B', 3, 2),
    ('A', 1, 3),
    ('hx', 1, 2),
    ('B', 1, 3),
    ('B', 2, 3),
    ('h4', 0),
    ('A', 0, 4),
    ('hx', 1, 3),
    ('h4x', 0, 1),
    ('h4', 1),
    ('B', 0, 4),
    ('hp', 1),
    ('turnown',),
    ('A', 1, 4),
    ('B', 3, 3),
    ('B', 1, 4),
    ('mm', 0, 0),
    ('B', 2, 4),
    ('h4x', 0, 2),
    ('prior',),
    ('mm', 1, 0),
    ('last', 0),
    ('mm', 0, 1),
    ('B', 3, 4),
    ('mm', 1, 1),
    ('last', 1),
    ('mm', 0, 2),
    ('att', 0),
    ('h4x', 1, 1),
    ('h4x', 0, 3),
    ('mm', 1, 2),
    ('att', 1),
    ('s1', 0),
    ('s1', 1),
    ('h4x', 1, 2),
    ('own', 0),
    ('own', 1),
    ('turn', 0),
    ('h4x', 1, 3),
    ('outatt',),
    ('blk', 0),
    ('blk', 1),
    ('turn', 1),
    ('far', 0, 0),
    ('far', 1, 0),
    ('tot', 1),
    ('far', 0, 1),
    ('far', 1, 1),
    ('rest', 0, 0),
    ('rest', 0, 1),
    ('rest', 1, 0),
    ('rest', 1, 1),
    ('rs', 0, 0, 3),
    ('rs', 0, 1, 3),
    ('back', 1),
    ('rs', 1, 0, 3),
    ('rs', 1, 1, 3),
    ('rs', 0, 0, 2),
    ('rs', 0, 1, 2),
    ('rs', 1, 0, 2),
    ('rs', 1, 1, 2),
    ('later',),
    ('rs', 0, 0, 1),
    ('rs', 0, 1, 1),
    ('rs', 1, 0, 1),
    ('rs', 1, 1, 1),
    ('rsl', 0, 0),
    ('rsl', 0, 1),
    ('rsl', 1, 0),
    ('rsl', 1, 1),
)


def dot_nn(a, b):
    return lax.dot_general(a, b, (((1,), (0,)), ((), ())), preferred_element_type=F32)


def dot_nt(a, b):
    return lax.dot_general(a, b, (((1,), (1,)), ((), ())), preferred_element_type=F32)


def dot_tn(a, b):
    return lax.dot_general(a, b, (((0,), (0,)), ((), ())), preferred_element_type=F32)


class Net:
    def __init__(self, ruler, send_sems, recv_sems):
        self.ruler, self.send_sems, self.recv_sems = ruler, send_sems, recv_sems
        self.groups = {}
        self.lanes = {}
        self.row_bytes = ruler.shape[1] * 2

    def send(self, group, src, dst, device, lane):
        size = 4 if src.dtype == F32 else 2
        for extent in src.shape:
            size *= extent
        group_at = self.groups.setdefault(group, [len(self.groups), 0, False])
        lane_at = self.lanes.setdefault(lane, [len(self.lanes), 0])
        group_at[1] += size
        lane_at[1] += size
        self.device = device
        pltpu.make_async_remote_copy(
            src_ref=src,
            dst_ref=dst,
            send_sem=self.send_sems.at[lane_at[0]],
            recv_sem=self.recv_sems.at[group_at[0]],
            device_id=device,
            device_id_type=MESH,
        ).start()

    def measure(self, size, send_at, recv_at):
        ref = self.ruler.at[pl.ds(0, size // self.row_bytes), :]
        return pltpu.make_async_remote_copy(
            src_ref=ref,
            dst_ref=ref,
            send_sem=self.send_sems.at[send_at],
            recv_sem=self.recv_sems.at[recv_at],
            device_id=self.device,
            device_id_type=MESH,
        )

    def recv(self, group):
        at = self.groups[group]
        assert not at[2]
        at[2] = True
        self.measure(at[1], 0, at[0]).wait_recv()

    def finish(self):
        assert len(self.groups) <= GROUPS and len(self.lanes) <= LANES
        assert all(at[2] for at in self.groups.values())
        for at, size in self.lanes.values():
            self.measure(size, at, 0).wait_send()


def kernel(
    sizes, hidden, w_query, key_input, values, cotangent,
    out_att, out_qg, out_kg, out_vg,
    hf, wf, kb, kf, vb, gb, q32, qf, att, dn, sc, mx, vg32, kg32, kg, vg,
    s_out, s_in, t_out, t_in, b_out, prior, later, pre,
    h4, h4t, dq4, g32, rs_out, rs_in, qg, qsend, qin,
    send_sems, recv_sems, local_sems,
):
    NX, NY, NZ = sizes
    x = lax.axis_index("heads")
    ctx = lax.axis_index("ctx")
    c = ctx % CORES
    z = (ctx // CORES) % NZ
    y = ctx // (CORES * NZ)
    p = 1 - c
    u = y % 2
    pair = y // 2
    py = y + 1 - 2 * u
    qy = NY - 1 - y
    ry = NY - 1 - py
    own_y = (y, py, qy, ry)
    e = ((y + 1) // 2) % 2
    T, DX = hidden.shape
    WR, NALL = w_query.shape
    D = NX * DX
    CH = CORES * WR
    KY = NZ * CH
    KH = 2 * KY
    CT = CORES * T
    XM, ZM = NX // 2, NZ // 2
    BOTH = (1, -1)
    BLOCKS = (0, 1)

    def at(y_, z_, core):
        return (x, (y_ * NZ + z_) * CORES + core)

    def dev_x(step):
        return ((x + step + NX) % NX, ctx)

    def dev_z(step):
        return at(y, (z + step + NZ) % NZ, c)

    partner = at(y, z, p)
    pair_same = at(py, z, c)
    pair_other = at(py, z, p)
    across = at(qy, z, c)
    net = Net(wf, send_sems, recv_sems)

    def rows_of(start, size, unit=16):
        return pl.ds(pl.multiple_of(start, unit), size)

    def head_cols(core, parity, width):
        return pl.ds(pl.multiple_of((2 * core + parity) * width, width), width)

    def split(total, part, top=None):
        top = total // 2 if top is None else top
        return {"full": (0, total), "top": (0, top), "bot": (top, total - top)}[part]

    def part_of(direction, d, most):
        if d < most:
            return "full"
        return "top" if direction > 0 else "bot"

    def fresh(r, most):
        if r == 0:
            return [0]
        return [-r, r] if r < most else [most]

    w_mine = rows_of((y * NZ + z) * CH + c * WR, WR)
    t_mine = rows_of(c * T, T)
    x_mine = pl.ds(pl.multiple_of(x * DX, DX), DX)
    moves = [
        ("w", w_query.at[:, head_cols(c, e, FEAT)], wf.at[w_mine, :]),
        ("h", hidden, hf.at[t_mine, x_mine]),
        ("k0", key_input.at[:, head_cols(c, e, FEAT)], kb.at[0, t_mine, :]),
        ("k2", key_input.at[:, head_cols(c, 1 - e, FEAT)], kb.at[2, t_mine, :]),
        ("v0", values.at[:, head_cols(c, e, HEAD_DIM)], vb.at[0, t_mine, :]),
        ("v2", values.at[:, head_cols(c, 1 - e, HEAD_DIM)], vb.at[2, t_mine, :]),
        ("g", cotangent.at[:, head_cols(c, e, HEAD_DIM)], gb.at[0, t_mine, :]),
    ]
    local = {}
    for n, (name, src, dst) in enumerate(moves):
        local[name] = pltpu.make_async_copy(src, dst, local_sems.at[n])
        local[name].start()
    barrier = pltpu.get_barrier_semaphore()
    friends = [partner, pair_same, pair_other, across, at(ry, z, c)]
    friends += [dev_x(d) for d in sorted({1, NX - 1})]
    friends += [dev_z(d) for d in range(1, NZ)]
    for friend in friends:
        pl.semaphore_signal(barrier, inc=1, device_id=friend, device_id_type=MESH)
    pl.semaphore_wait(barrier, len(friends))
    pair_cores = ((c, pair_same), (p, pair_other))
    for core, to in pair_cores:
        net.send(("w", 1), w_query.at[:, head_cols(core, 1 - e, FEAT)], wf.at[w_mine, :], to, "io")
    net.send(("w", 0), w_query.at[:, head_cols(p, e, FEAT)], wf.at[w_mine, :], partner, "io")
    net.send("h1", hidden, hf.at[rows_of(CT + c * T, T), x_mine], pair_same, "io")
    for slot, parity in ((0, e), (2, 1 - e)):
        net.send(
            "kv0", key_input.at[:, head_cols(p, parity, FEAT)], kb.at[slot, t_mine, :], partner, "in"
        )
        net.send(
            "kv0", values.at[:, head_cols(p, parity, HEAD_DIM)], vb.at[slot, t_mine, :], partner, "in"
        )
    net.send(("hp", 0), hidden, hf.at[t_mine, x_mine], partner, "io")
    for core, to in pair_cores:
        cut, narrow = head_cols(core, 1 - e, FEAT), head_cols(core, 1 - e, HEAD_DIM)
        net.send("kv1", key_input.at[:, cut], kb.at[1, t_mine, :], to, "io")
        net.send("kv1", values.at[:, narrow], vb.at[1, t_mine, :], to, "io")
        net.send("kv1", cotangent.at[:, narrow], gb.at[1, t_mine, :], to, "io")
    net.send("g0", cotangent.at[:, head_cols(p, e, HEAD_DIM)], gb.at[0, t_mine, :], partner, "io")

    A_ROWS = CH * A_EIGHTHS // 8
    B_ROWS = CH - A_ROWS
    A_TOP, B_TOP = A_ROWS * A_FIFTHS // 5, B_ROWS // 3

    def w_piece(stream, which, rel_z, part):
        total, first = (A_ROWS, A_TOP) if stream == "A" else (B_ROWS, B_TOP)
        start, size = split(total, part, first)
        if stream == "B":
            start = start + A_ROWS
        return wf.at[rows_of((own_y[which] * NZ + (z + rel_z + NZ) % NZ) * CH + start, size), :]

    def w_ring(stream, which, d):
        for s in BOTH:
            piece = w_piece(stream, which, -s * (d - 1), part_of(s, d, ZM))
            net.send((stream, which, d), piece, piece, dev_z(s), "w")

    def w_across(stream, b, rel):
        piece = w_piece(stream, b, rel, "full")
        net.send((stream, "across", b), piece, piece, across, "w")

    def w_next(stream, which, d):
        net.recv((stream, which, d))
        if d < ZM:
            w_ring(stream, which, d + 1)

    def w_begin(b):
        if b == 0:
            local["w"].wait()
        net.recv(("w", b))
        w_ring("A", b, 1)
        w_across("B", b, 0)
        w_across("A", b, 0)
        w_ring("B", b, 1)

    def w_a(b, r):
        w_next("A", b, r)
        for rel in fresh(r, ZM):
            w_across("A", b, rel)

    def w_turn(b):
        net.recv(("B", "across", b))
        w_ring("B", 2 + b, 1)

    def w_last(b):
        net.recv(("A", "across", b))

    def x_ring(name, piece, stage, lane):
        for s in BOTH:
            first, second = ("top", "bot") if s > 0 else ("bot", "top")
            back = 0 if stage < 3 else -s
            ref = piece(back, second if stage == 2 else first)
            net.send((*name, stage), ref, ref, dev_x(s), lane)

    def x_relay(name, piece, stage, lane):
        for s in BOTH:
            first, second = ("top", "bot") if s > 0 else ("bot", "top")
            ref = piece(-s if stage < 3 else -2 * s, second if stage == 2 else first)
            net.send(name, ref, ref, partner, lane)

    def x_begin(name, piece, lane):
        x_ring(name, piece, 1, lane)
        if XM > 1:
            x_ring(name, piece, 2, lane)

    def x_step(name, relay, piece, stage, lane):
        net.recv((*name, stage))
        if stage == 1 and XM > 1:
            x_ring(name, piece, 3, lane)
        x_relay(relay, piece, stage, lane)

    def h_piece(b):
        def piece(rel_x, part):
            start, size = split(T, part)
            xs = (x + rel_x + NX) % NX
            return hf.at[
                rows_of(b * CT + c * T + start, size), pl.ds(pl.multiple_of(xs * DX, DX), DX)
            ]

        return piece

    def h_begin(b):
        if b == 0:
            local["h"].wait()
        else:
            net.recv("h1")
        x_begin(("hx", b), h_piece(b), ("h", b))
        if b == 1:
            piece = h_piece(b)(0, "full")
            net.send(("hp", b), piece, piece, partner, ("h", b))

    def h_step(b, stage):
        x_step(("hx", b), ("hp", b), h_piece(b), stage, ("h", b))

    def h_all(b):
        net.recv(("hp", b))

    SR = FEAT // NZ

    def slice_at(k):
        return pl.ds(pl.multiple_of(k * SR, SR), SR)

    FAR_FIRST = sorted(range(1, NZ), key=lambda o: -min(o, NZ - o))

    def scan_start(kind):
        for o in FAR_FIRST:
            src = s_out.at[kind, :, slice_at((z + o) % NZ), :]
            net.send((kind, "s"), src, s_in.at[kind, o], dev_z(o), "sums")

    def scan_totals(kind):
        own = s_out[kind, :, slice_at(z), :].astype(F32)
        total = own
        net.recv((kind, "s"))
        pre[z] = own
        for o in range(1, NZ):
            came = s_in[kind, o].astype(F32)
            total = total + came
            pre[(z - o + NZ) % NZ] = came
        t_out[kind] = total.astype(BF16)
        if kind == 0:
            for n, to in ((1, pair_same), (2, across), (3, at(ry, z, c))):
                net.send((kind, "t"), t_out.at[kind], t_in.at[kind, n], to, "sums")
        else:
            net.send((kind, "t"), t_out.at[kind], t_in.at[kind, 2], across, "sums")

    def scan_back(kind, result):
        net.recv((kind, "t"))
        zero = jnp.zeros((SR, HEAD_DIM), F32)
        if kind == 0:
            offset = [zero, zero]
            for n in (1, 2, 3):
                for half in (0, 1):
                    term = t_in[0, n, half].astype(F32)
                    offset[half] = offset[half] + jnp.where(own_y[n] < y, term, 0.0)
        else:
            sums = (
                t_out[1, 0].astype(F32),
                t_out[1, 1].astype(F32),
                t_in[1, 2, 0].astype(F32),
                t_in[1, 2, 1].astype(F32),
            )
            offset = []
            for b in BLOCKS:
                total = zero
                for n in range(4):
                    if n != b:
                        total = total + jnp.where(own_y[n] > own_y[b], sums[n], 0.0)
                offset.append(total)
        for half in (0, 1):
            running = offset[half]
            for k in range(NZ) if kind == 0 else reversed(range(NZ)):
                b_out[kind, k, half] = running.astype(BF16)
                running = running + pre[k, half]
        for o in FAR_FIRST:
            src = b_out.at[kind, (z + o) % NZ]
            dst = result.at[pl.ds(0, 2), slice_at(z), :]
            net.send((kind, "b"), src, dst, dev_z(o), "sums")
        result[pl.ds(0, 2), slice_at(z), :] = b_out[kind, z]

    PT = T // NX

    def quarter(rel_x):
        xs = (x + rel_x + NX) % NX
        return pl.ds(pl.multiple_of(xs * PT, PT), PT)

    def h4_start():
        src = hf.at[
            rows_of(c * T + x * PT, PT), pl.ds(pl.multiple_of((1 - pair) * KH, KH), KH)
        ]
        net.send(("h4", 0), src, h4.at[0, c, quarter(0), :], across, "h4")

    def h4_piece(j):
        def piece(rel_x, part):
            start, size = {"full": (0, KH), "top": (0, KH // 2), "bot": (KH // 2, KH // 2)}[part]
            return h4.at[j, c, quarter(rel_x), pl.ds(start, size)]

        return piece

    def h4_begin(j):
        net.recv(("h4", j))
        x_begin(("h4x", j), h4_piece(j), "h4")
        mine = h4_piece(j)(0, "full")
        if j == 0:
            net.send(("h4", 1), mine, h4_piece(1)(0, "full"), pair_same, "h4")
        net.send(("h4p", j), mine, mine, partner, "h4")

    def h4_step(j, stage):
        x_step(("h4x", j), ("h4p", j), h4_piece(j), stage, "h4")

    WIDE = 256

    def h4_turn_own():
        for k in range(KH // WIDE):
            cols = pl.ds(pl.multiple_of(pair * KH + k * WIDE, WIDE), WIDE)
            h4t[k * WIDE : (k + 1) * WIDE, 0 : 2 * CT] = hf[:, cols].T

    def h4_turn(j):
        net.recv(("h4p", j))
        for k in range(KH // WIDE):
            cut = slice(k * WIDE, (k + 1) * WIDE)
            h4t[cut, (2 + j) * CT : (3 + j) * CT] = h4[j, :, :, cut].reshape(CT, WIDE).T

    def project(b, part):
        start, size = (pair * KH, KH) if part == 0 else (own_y[1 + part] * KY, KY)
        rows = pl.ds(pl.multiple_of(start, KY), size)
        block = slice(b * CT, (b + 1) * CT)
        product = dot_nn(hf[block, rows], wf[rows, :])
        q32[block, :] = product if part == 0 else q32[block, :] + product

    causal = lax.broadcasted_iota(jnp.int32, (CT, CT), 0) >= lax.broadcasted_iota(
        jnp.int32, (CT, CT), 1
    )

    def attend(b):
        if b == 1:
            net.recv("prior")
        proj = q32[b * CT : (b + 1) * CT, :]
        feats = jnp.maximum(proj, 0.0).astype(BF16)
        qf[b] = feats
        keys, vals = kf[b], vb[b]
        state = prior[e] if b == 0 else prior[2]
        scores = jnp.where(causal, dot_nt(feats, keys), 0.0).astype(BF16)
        sc[b] = scores
        numer = dot_nn(scores, vals) + dot_nn(feats, state)
        inv = lax.rsqrt(jnp.mean(numer * numer, axis=-1, keepdims=True) + EPSILON)
        normed = numer * inv
        att[b] = normed.astype(BF16)
        grad = gb[b].astype(F32)
        d_num = (inv * (grad - normed * jnp.mean(grad * normed, axis=-1, keepdims=True))).astype(BF16)
        dn[b] = d_num
        mixed = jnp.where(causal, dot_nt(d_num, vals), 0.0).astype(BF16)
        mx[b] = mixed
        d_feat = dot_nn(mixed, keys) + dot_nt(d_num, state)
        d_q = jnp.where(proj > 0, d_feat, 0.0).astype(BF16)
        mine = slice(b * CT, (b + 1) * CT)
        dq4[mine, :] = d_q
        theirs = slice((2 + b) * CT, (3 + b) * CT)
        if b == 0:
            net.send(("dq", 1, 0), dq4.at[mine, :], dq4.at[theirs, :], across, "sums")
        else:
            for h in (0, 1):
                cols = half_cols(h)
                net.send(("dq", 1, h), dq4.at[mine, cols], dq4.at[theirs, cols], across, "sums")

    def state_send(b):
        s_out[1, b] = dot_tn(qf[b], dn[b]).astype(BF16)
        for o in FAR_FIRST:
            src = s_out.at[1, b, slice_at((z + o) % NZ), :]
            net.send((1, "s"), src, s_in.at[1, o, b], dev_z(o), "sums")

    def states():
        for name in ("k0", "k2", "v0", "v2"):
            local[name].wait()
        net.recv("kv0")
        kf[0] = jnp.maximum(kb[0], jnp.zeros_like(kb[0]))
        s_out[0, e] = dot_tn(kf[0], vb[0]).astype(BF16)
        s_out[0, 1 - e] = dot_tn(jnp.maximum(kb[2], jnp.zeros_like(kb[2])), vb[2]).astype(BF16)
        scan_start(0)

    def prior_send():
        net.recv((0, "b"))
        net.send("prior", prior.at[1 - e], prior.at[2], pair_same, "sums")

    def keys_in():
        net.recv("kv1")
        kf[1] = jnp.maximum(kb[1], jnp.zeros_like(kb[1]))

    def grads_in():
        local["g"].wait()
        net.recv("g0")

    def block_parts(b):
        vg32[b] = dot_tn(sc[b], dn[b])
        kg32[b] = dot_tn(mx[b], qf[b])

    def state_parts(b):
        state = later[b]
        vg[b] = (vg32[b] + dot_nn(kf[b], state)).astype(BF16)
        d_key = kg32[b] + dot_nt(vb[b], state)
        kg[b] = jnp.where(kb[b] > 0, d_key, 0.0).astype(BF16)

    def part_rows(k):
        return pl.ds(pl.multiple_of(((1 - u) if k == 0 else u) * KY, KY), KY)

    def contract_own(k):
        g32[k] = dot_nn(h4t[part_rows(k), 0 : 2 * CT], dq4[0 : 2 * CT, :])

    REST = slice(2 * CT, 4 * CT)

    def half_cols(h):
        return slice(h * FEAT // 2, (h + 1) * FEAT // 2)

    def contract_far(k, h):
        cols = half_cols(h)
        if k == 0:
            net.recv(("dq", 1, h))
        to = ((z + ZM) % NZ) * CH
        rows = rows_of(((1 - u) if k == 0 else u) * KY + to, CH)
        far = g32[k, rows_of(to, CH), cols] + dot_nn(h4t[rows, REST], dq4[REST, cols])
        for s in BOTH:
            rows = rs_rows(part_of(s, ZM, ZM))
            rs_out[k, 0 if s > 0 else 1, ZM - 1, rows, cols] = far[rows, :].astype(BF16)
            rs_put(k, h, s, ZM)

    def contract_rest(k, h):
        cols = half_cols(h)
        g32[k, :, cols] = g32[k, :, cols] + dot_nn(h4t[part_rows(k), REST], dq4[REST, cols])

    def rs_rows(part):
        start, size = split(CH, part, CH * RS_EIGHTHS // 8)
        return slice(start, start + size)

    def rs_put(k, h, s, d):
        way, rows, cols = 0 if s > 0 else 1, rs_rows(part_of(s, d, ZM)), half_cols(h)
        net.send(
            ("rs", k, h, s, d) if d > 1 else ("rs", k, h),
            rs_out.at[k, way, d - 1, rows, cols],
            rs_in.at[k, way, d - 1, rows, cols],
            dev_z(s),
            "sums",
        )

    def rs_send(k, h, d):
        cols = half_cols(h)
        for s in BOTH:
            net.recv(("rs", k, h, s, d + 1))
            rows = rs_rows(part_of(s, d, ZM))
            size = rows.stop - rows.start
            to = (z + s * d + NZ) % NZ
            total = g32[k, rows_of(to * CH + rows.start, size), cols]
            way = 0 if s > 0 else 1
            rs_out[k, way, d - 1, rows, cols] = total.astype(BF16)
            came = rs_rows(part_of(s, d + 1, ZM))
            got = rs_in[k, way, d, came, cols].astype(F32)
            rs_out[k, way, d - 1, came, cols] = (total[came, :] + got).astype(BF16)
            rs_put(k, h, s, d)

    def rs_last(k, h):
        cols = half_cols(h)
        net.recv(("rs", k, h))
        total = g32[k, rows_of(z * CH, CH), cols]
        if ZM > 1:
            total = total + rs_in[k, 0, 0, :, cols].astype(F32) + rs_in[k, 1, 0, :, cols].astype(F32)
        else:
            came = [
                rs_in[k, way, 0, rs_rows(part), cols].astype(F32)
                for way, part in enumerate(("top", "bot"))
            ]
            total = total + jnp.concatenate(came, axis=0)
        at_cols = (2 * c + e) * FEAT + h * (FEAT // 2)
        mine = out_qg.at[:, pl.ds(pl.multiple_of(at_cols, FEAT // 2), FEAT // 2)]

        if k == 0:
            qsend[:, cols] = total.astype(BF16)
            for core, to in pair_cores:
                piece = qsend.at[rows_of(core * WR, WR), cols]
                net.send("qin", piece, qin.at[c, :, cols], to, "io")
        else:
            qg[:, cols] = total
            net.send("out", qg.at[rows_of(p * WR, WR), cols], mine, partner, "io")
            out_qg[:, pl.ds(pl.multiple_of(at_cols, FEAT // 2), FEAT // 2)] = qg[
                rows_of(c * WR, WR), cols
            ]

    def out_send(buf, out, rows, width):
        mine = out.at[:, head_cols(c, e, width)]

        def piece(block, core):
            return buf.at[block, rows_of(core * rows, rows), :]

        net.send("out", piece(1, c), mine, pair_same, "io")
        net.send("out", piece(1, p), mine, pair_other, "io")
        net.send("out", piece(0, p), mine, partner, "io")
        out[:, head_cols(c, e, width)] = buf[0, rows_of(c * rows, rows), :]

    def att_out():
        out_send(att, out_att, T, HEAD_DIM)

    def later_parts():
        net.recv((1, "b"))
        for b in BLOCKS:
            state_parts(b)
        out_send(kg, out_kg, T, FEAT)
        out_send(vg, out_vg, T, HEAD_DIM)

    tasks = {
        "w": w_begin,
        "A": w_a,
        "B": lambda which, d: w_next("B", which, d),
        "across": w_turn,
        "last": w_last,
        "h": h_begin,
        "hx": h_step,
        "hp": h_all,
        "state": states,
        "tot": scan_totals,
        "back": lambda kind: scan_back(kind, later if kind else prior),
        "prior": prior_send,
        "kv1": keys_in,
        "g0": grads_in,
        "h4s": h4_start,
        "h4": h4_begin,
        "h4x": h4_step,
        "turnown": h4_turn_own,
        "turn": h4_turn,
        "mm": project,
        "att": attend,
        "s1": state_send,
        "outatt": att_out,
        "blk": block_parts,
        "own": contract_own,
        "far": contract_far,
        "rest": contract_rest,
        "rs": rs_send,
        "rsl": rs_last,
        "later": later_parts,
    }
    for name, *where in ORDER:
        tasks[name](*where)
    net.recv("qin")
    for core in (0, 1):
        out_qg[:, head_cols(core, 1 - e, FEAT)] = qin[core].astype(F32)
    net.recv("out")
    net.finish()


def write_out(*refs):
    ins, outs, sems = refs[:4], refs[4:8], refs[8]
    copies = [
        pltpu.make_async_copy(src, dst, sems.at[n]) for n, (src, dst) in enumerate(zip(ins, outs))
    ]
    for copy in copies:
        copy.start()
    for copy in copies:
        copy.wait()


def solution(mesh):
    NX, ctx_size = mesh.shape["heads"], mesh.shape["ctx"]
    NY = 4
    NZ = ctx_size // (NY * CORES)
    sizes = (NX, NY, NZ)

    def body(hidden, w_query, key_input, values, cotangent):
        T, DX = hidden.shape
        WR, NALL = w_query.shape
        VALL = values.shape[1]
        D = NX * DX
        CH = CORES * WR
        KY = NZ * CH
        CT = CORES * T
        ZM = NZ // 2
        SR = FEAT // NZ
        any_space = pl.BlockSpec(memory_space=pl.ANY)
        vmem_space = pl.BlockSpec(memory_space=pltpu.VMEM)
        outs = (((T, VALL), BF16), ((WR, NALL), F32), ((T, NALL), BF16), ((T, VALL), BF16))

        def vmem(*shape, dtype=BF16):
            return pltpu.VMEM(shape, dtype)

        def run(*refs):
            kernel(sizes, *refs)

        parts = pl.pallas_call(
            run,
            out_shape=tuple(pltpu.VMEM(*of) for of in outs),
            in_specs=[any_space] * 5,
            out_specs=(vmem_space,) * 4,
            scratch_shapes=[
                vmem(2 * CT, D),
                vmem(D, FEAT),
                vmem(3, CT, FEAT),
                vmem(2, CT, FEAT),
                vmem(3, CT, HEAD_DIM),
                vmem(2, CT, HEAD_DIM),
                vmem(2 * CT, FEAT, dtype=F32),
                vmem(2, CT, FEAT),
                vmem(2, CT, HEAD_DIM),
                vmem(2, CT, HEAD_DIM),
                vmem(2, CT, CT),
                vmem(2, CT, CT),
                vmem(2, CT, HEAD_DIM, dtype=F32),
                vmem(2, CT, FEAT, dtype=F32),
                vmem(2, CT, FEAT),
                vmem(2, CT, HEAD_DIM),
                vmem(2, 2, FEAT, HEAD_DIM),
                vmem(2, NZ, 2, SR, HEAD_DIM),
                vmem(2, 2, SR, HEAD_DIM),
                vmem(2, NY, 2, SR, HEAD_DIM),
                vmem(2, NZ, 2, SR, HEAD_DIM),
                vmem(3, FEAT, HEAD_DIM),
                vmem(2, FEAT, HEAD_DIM),
                vmem(NZ, 2, SR, HEAD_DIM, dtype=F32),
                vmem(2, CORES, T, 2 * KY),
                vmem(2 * KY, 4 * CT),
                vmem(4 * CT, FEAT),
                vmem(2, KY, FEAT, dtype=F32),
                vmem(2, 2, ZM, CH, FEAT),
                vmem(2, 2, ZM, CH, FEAT),
                vmem(CH, FEAT, dtype=F32),
                vmem(CH, FEAT),
                vmem(CORES, WR, FEAT),
                pltpu.SemaphoreType.DMA((LANES,)),
                pltpu.SemaphoreType.DMA((GROUPS,)),
                pltpu.SemaphoreType.DMA((LOCALS,)),
            ],
            compiler_params=pltpu.CompilerParams(
                collective_id=0, has_side_effects=True, vmem_limit_bytes=60000 * 1024
            ),
        )(hidden, w_query, key_input, values, cotangent)
        return pl.pallas_call(
            write_out,
            out_shape=tuple(jax.ShapeDtypeStruct(*of) for of in outs),
            in_specs=[vmem_space] * 4,
            out_specs=(any_space,) * 4,
            scratch_shapes=[pltpu.SemaphoreType.DMA((4,))],
        )(*[pltpu.with_memory_space_constraint(part, pltpu.VMEM) for part in parts])

    spec = P("ctx", "heads")
    return jax.shard_map(
        body, mesh=mesh, in_specs=(spec,) * 5, out_specs=(spec,) * 4, check_vma=False
    )
```

```python
import jax
import jax.numpy as jnp
from jax import lax
from jax.experimental import pallas as pl
from jax.experimental.pallas import tpu as pltpu
from jax.sharding import PartitionSpec as P

HEAD_DIM = 128
FEAT = 256
CORES = 2
EPSILON = 1e-06
MESH = pl.DeviceIdType.MESH
F32 = jnp.float32
BF16 = jnp.bfloat16
GROUPS = 91
LANES = 7
LOCALS = 7
A_EIGHTHS = 5
A_FIFTHS = 1
RS_EIGHTHS = 2

ORDER = (
    ('h', 0),
    ('w', 0),
    ('state',),
    ('g0',),
    ('w', 1),
    ('across', 0),
    ('A', 0, 1),
    ('B', 0, 1),
    ('hx', 0, 1),
    ('across', 1),
    ('hx', 0, 2),
    ('A', 1, 1),
    ('h', 1),
    ('B', 1, 1),
    ('B', 2, 1),
    ('tot', 0),
    ('A', 0, 2),
    ('hx', 0, 3),
    ('B', 0, 2),
    ('h4s',),
    ('B', 3, 1),
    ('A', 1, 2),
    ('hp', 0),
    ('B', 1, 2),
    ('B', 2, 2),
    ('hx', 1, 1),
    ('kv1',),
    ('A', 0, 3),
    ('back', 0),
    ('B', 0, 3),
    ('B', 3, 2),
    ('A', 1, 3),
    ('hx', 1, 2),
    ('B', 1, 3),
    ('B', 2, 3),
    ('h4', 0),
    ('A', 0, 4),
    ('hx', 1, 3),
    ('h4x', 0, 1),
    ('h4', 1),
    ('B', 0, 4),
    ('hp', 1),
    ('turnown',),
    ('A', 1, 4),
    ('B', 3, 3),
    ('B', 1, 4),
    ('mm', 0, 0),
    ('B', 2, 4),
    ('h4x', 0, 2),
    ('prior',),
    ('mm', 1, 0),
    ('last', 0),
    ('mm', 0, 1),
    ('B', 3, 4),
    ('mm', 1, 1),
    ('last', 1),
    ('mm', 0, 2),
    ('att', 0),
    ('h4x', 1, 1),
    ('h4x', 0, 3),
    ('mm', 1, 2),
    ('att', 1),
    ('s1', 0),
    ('s1', 1),
    ('h4x', 1, 2),
    ('own', 0),
    ('own', 1),
    ('turn', 0),
    ('h4x', 1, 3),
    ('turn', 1),
    ('far', 0, 0),
    ('far', 1, 0),
    ('tot', 1),
    ('far', 0, 1),
    ('far', 1, 1),
    ('outatt',),
    ('rest', 0, 0),
    ('rest', 0, 1),
    ('rest', 1, 0),
    ('rest', 1, 1),
    ('blk', 0),
    ('blk', 1),
    ('rs', 0, 0, 3),
    ('rs', 0, 1, 3),
    ('back', 1),
    ('rs', 1, 0, 3),
    ('rs', 1, 1, 3),
    ('rs', 0, 0, 2),
    ('rs', 0, 1, 2),
    ('rs', 1, 0, 2),
    ('rs', 1, 1, 2),
    ('later',),
    ('rs', 0, 0, 1),
    ('rs', 0, 1, 1),
    ('rs', 1, 0, 1),
    ('rs', 1, 1, 1),
    ('rsl', 0, 0),
    ('rsl', 0, 1),
    ('rsl', 1, 0),
    ('rsl', 1, 1),
)


def dot_nn(a, b):
    return lax.dot_general(a, b, (((1,), (0,)), ((), ())), preferred_element_type=F32)


def dot_nt(a, b):
    return lax.dot_general(a, b, (((1,), (1,)), ((), ())), preferred_element_type=F32)


def dot_tn(a, b):
    return lax.dot_general(a, b, (((0,), (0,)), ((), ())), preferred_element_type=F32)


class Net:
    def __init__(self, ruler, send_sems, recv_sems):
        self.ruler, self.send_sems, self.recv_sems = ruler, send_sems, recv_sems
        self.groups = {}
        self.lanes = {}
        self.row_bytes = ruler.shape[1] * 2

    def send(self, group, src, dst, device, lane):
        size = 4 if src.dtype == F32 else 2
        for extent in src.shape:
            size *= extent
        group_at = self.groups.setdefault(group, [len(self.groups), 0, False])
        lane_at = self.lanes.setdefault(lane, [len(self.lanes), 0])
        group_at[1] += size
        lane_at[1] += size
        self.device = device
        pltpu.make_async_remote_copy(
            src_ref=src,
            dst_ref=dst,
            send_sem=self.send_sems.at[lane_at[0]],
            recv_sem=self.recv_sems.at[group_at[0]],
            device_id=device,
            device_id_type=MESH,
        ).start()

    def measure(self, size, send_at, recv_at):
        ref = self.ruler.at[pl.ds(0, size // self.row_bytes), :]
        return pltpu.make_async_remote_copy(
            src_ref=ref,
            dst_ref=ref,
            send_sem=self.send_sems.at[send_at],
            recv_sem=self.recv_sems.at[recv_at],
            device_id=self.device,
            device_id_type=MESH,
        )

    def recv(self, group):
        at = self.groups[group]
        assert not at[2]
        at[2] = True
        self.measure(at[1], 0, at[0]).wait_recv()

    def finish(self):
        assert len(self.groups) <= GROUPS and len(self.lanes) <= LANES
        assert all(at[2] for at in self.groups.values())
        for at, size in self.lanes.values():
            self.measure(size, at, 0).wait_send()


def kernel(
    sizes, hidden, w_query, key_input, values, cotangent,
    out_att, out_qg, out_kg, out_vg,
    hf, wf, kb, kf, vb, gb, q32, qf, att, dn, sc, mx, vg32, kg32, kg, vg,
    s_out, s_in, t_out, t_in, b_out, prior, later, pre,
    h4, h4t, dq4, g32, rs_out, rs_in, qg, qsend, qin,
    send_sems, recv_sems, local_sems,
):
    NX, NY, NZ = sizes
    x = lax.axis_index("heads")
    ctx = lax.axis_index("ctx")
    c = ctx % CORES
    z = (ctx // CORES) % NZ
    y = ctx // (CORES * NZ)
    p = 1 - c
    u = y % 2
    pair = y // 2
    py = y + 1 - 2 * u
    qy = NY - 1 - y
    ry = NY - 1 - py
    own_y = (y, py, qy, ry)
    e = ((y + 1) // 2) % 2
    T, DX = hidden.shape
    WR, NALL = w_query.shape
    D = NX * DX
    CH = CORES * WR
    KY = NZ * CH
    KH = 2 * KY
    CT = CORES * T
    XM, ZM = NX // 2, NZ // 2
    BOTH = (1, -1)
    BLOCKS = (0, 1)

    def at(y_, z_, core):
        return (x, (y_ * NZ + z_) * CORES + core)

    def dev_x(step):
        return ((x + step + NX) % NX, ctx)

    def dev_z(step):
        return at(y, (z + step + NZ) % NZ, c)

    partner = at(y, z, p)
    pair_same = at(py, z, c)
    pair_other = at(py, z, p)
    across = at(qy, z, c)
    net = Net(wf, send_sems, recv_sems)

    def rows_of(start, size, unit=16):
        return pl.ds(pl.multiple_of(start, unit), size)

    def head_cols(core, parity, width):
        return pl.ds(pl.multiple_of((2 * core + parity) * width, width), width)

    def split(total, part, top=None):
        top = total // 2 if top is None else top
        return {"full": (0, total), "top": (0, top), "bot": (top, total - top)}[part]

    def part_of(direction, d, most):
        if d < most:
            return "full"
        return "top" if direction > 0 else "bot"

    def fresh(r, most):
        if r == 0:
            return [0]
        return [-r, r] if r < most else [most]

    w_mine = rows_of((y * NZ + z) * CH + c * WR, WR)
    t_mine = rows_of(c * T, T)
    x_mine = pl.ds(pl.multiple_of(x * DX, DX), DX)
    moves = [
        ("w", w_query.at[:, head_cols(c, e, FEAT)], wf.at[w_mine, :]),
        ("h", hidden, hf.at[t_mine, x_mine]),
        ("k0", key_input.at[:, head_cols(c, e, FEAT)], kb.at[0, t_mine, :]),
        ("k2", key_input.at[:, head_cols(c, 1 - e, FEAT)], kb.at[2, t_mine, :]),
        ("v0", values.at[:, head_cols(c, e, HEAD_DIM)], vb.at[0, t_mine, :]),
        ("v2", values.at[:, head_cols(c, 1 - e, HEAD_DIM)], vb.at[2, t_mine, :]),
        ("g", cotangent.at[:, head_cols(c, e, HEAD_DIM)], gb.at[0, t_mine, :]),
    ]
    local = {}
    for n, (name, src, dst) in enumerate(moves):
        local[name] = pltpu.make_async_copy(src, dst, local_sems.at[n])
        local[name].start()
    barrier = pltpu.get_barrier_semaphore()
    friends = [partner, pair_same, pair_other, across, at(ry, z, c)]
    friends += [dev_x(d) for d in sorted({1, NX - 1})]
    friends += [dev_z(d) for d in range(1, NZ)]
    for friend in friends:
        pl.semaphore_signal(barrier, inc=1, device_id=friend, device_id_type=MESH)
    pl.semaphore_wait(barrier, len(friends))
    pair_cores = ((c, pair_same), (p, pair_other))
    for core, to in pair_cores:
        net.send(("w", 1), w_query.at[:, head_cols(core, 1 - e, FEAT)], wf.at[w_mine, :], to, "io")
    net.send(("w", 0), w_query.at[:, head_cols(p, e, FEAT)], wf.at[w_mine, :], partner, "io")
    net.send("h1", hidden, hf.at[rows_of(CT + c * T, T), x_mine], pair_same, "io")
    for slot, parity in ((0, e), (2, 1 - e)):
        net.send(
            "kv0", key_input.at[:, head_cols(p, parity, FEAT)], kb.at[slot, t_mine, :], partner, "in"
        )
        net.send(
            "kv0", values.at[:, head_cols(p, parity, HEAD_DIM)], vb.at[slot, t_mine, :], partner, "in"
        )
    net.send(("hp", 0), hidden, hf.at[t_mine, x_mine], partner, "io")
    for core, to in pair_cores:
        cut, narrow = head_cols(core, 1 - e, FEAT), head_cols(core, 1 - e, HEAD_DIM)
        net.send("kv1", key_input.at[:, cut], kb.at[1, t_mine, :], to, "io")
        net.send("kv1", values.at[:, narrow], vb.at[1, t_mine, :], to, "io")
        net.send("kv1", cotangent.at[:, narrow], gb.at[1, t_mine, :], to, "io")
    net.send("g0", cotangent.at[:, head_cols(p, e, HEAD_DIM)], gb.at[0, t_mine, :], partner, "io")

    A_ROWS = CH * A_EIGHTHS // 8
    B_ROWS = CH - A_ROWS
    A_TOP, B_TOP = A_ROWS * A_FIFTHS // 5, B_ROWS // 3

    def w_piece(stream, which, rel_z, part):
        total, first = (A_ROWS, A_TOP) if stream == "A" else (B_ROWS, B_TOP)
        start, size = split(total, part, first)
        if stream == "B":
            start = start + A_ROWS
        return wf.at[rows_of((own_y[which] * NZ + (z + rel_z + NZ) % NZ) * CH + start, size), :]

    def w_ring(stream, which, d):
        for s in BOTH:
            piece = w_piece(stream, which, -s * (d - 1), part_of(s, d, ZM))
            net.send((stream, which, d), piece, piece, dev_z(s), "w")

    def w_across(stream, b, rel):
        piece = w_piece(stream, b, rel, "full")
        net.send((stream, "across", b), piece, piece, across, "w")

    def w_next(stream, which, d):
        net.recv((stream, which, d))
        if d < ZM:
            w_ring(stream, which, d + 1)

    def w_begin(b):
        if b == 0:
            local["w"].wait()
        net.recv(("w", b))
        w_ring("A", b, 1)
        w_across("B", b, 0)
        w_across("A", b, 0)
        w_ring("B", b, 1)

    def w_a(b, r):
        w_next("A", b, r)
        for rel in fresh(r, ZM):
            w_across("A", b, rel)

    def w_turn(b):
        net.recv(("B", "across", b))
        w_ring("B", 2 + b, 1)

    def w_last(b):
        net.recv(("A", "across", b))

    def x_ring(name, piece, stage, lane):
        for s in BOTH:
            first, second = ("top", "bot") if s > 0 else ("bot", "top")
            back = 0 if stage < 3 else -s
            ref = piece(back, second if stage == 2 else first)
            net.send((*name, stage), ref, ref, dev_x(s), lane)

    def x_relay(name, piece, stage, lane):
        for s in BOTH:
            first, second = ("top", "bot") if s > 0 else ("bot", "top")
            ref = piece(-s if stage < 3 else -2 * s, second if stage == 2 else first)
            net.send(name, ref, ref, partner, lane)

    def x_begin(name, piece, lane):
        x_ring(name, piece, 1, lane)
        if XM > 1:
            x_ring(name, piece, 2, lane)

    def x_step(name, relay, piece, stage, lane):
        net.recv((*name, stage))
        if stage == 1 and XM > 1:
            x_ring(name, piece, 3, lane)
        x_relay(relay, piece, stage, lane)

    def h_piece(b):
        def piece(rel_x, part):
            start, size = split(T, part)
            xs = (x + rel_x + NX) % NX
            return hf.at[
                rows_of(b * CT + c * T + start, size), pl.ds(pl.multiple_of(xs * DX, DX), DX)
            ]

        return piece

    def h_begin(b):
        if b == 0:
            local["h"].wait()
        else:
            net.recv("h1")
        x_begin(("hx", b), h_piece(b), ("h", b))
        if b == 1:
            piece = h_piece(b)(0, "full")
            net.send(("hp", b), piece, piece, partner, ("h", b))

    def h_step(b, stage):
        x_step(("hx", b), ("hp", b), h_piece(b), stage, ("h", b))

    def h_all(b):
        net.recv(("hp", b))

    SR = FEAT // NZ

    def slice_at(k):
        return pl.ds(pl.multiple_of(k * SR, SR), SR)

    FAR_FIRST = sorted(range(1, NZ), key=lambda o: -min(o, NZ - o))

    def scan_start(kind):
        for o in FAR_FIRST:
            src = s_out.at[kind, :, slice_at((z + o) % NZ), :]
            net.send((kind, "s"), src, s_in.at[kind, o], dev_z(o), "sums")

    def scan_totals(kind):
        own = s_out[kind, :, slice_at(z), :].astype(F32)
        total = own
        net.recv((kind, "s"))
        pre[z] = own
        for o in range(1, NZ):
            came = s_in[kind, o].astype(F32)
            total = total + came
            pre[(z - o + NZ) % NZ] = came
        t_out[kind] = total.astype(BF16)
        if kind == 0:
            for n, to in ((1, pair_same), (2, across), (3, at(ry, z, c))):
                net.send((kind, "t"), t_out.at[kind], t_in.at[kind, n], to, "sums")
        else:
            net.send((kind, "t"), t_out.at[kind], t_in.at[kind, 2], across, "sums")

    def scan_back(kind, result):
        net.recv((kind, "t"))
        zero = jnp.zeros((SR, HEAD_DIM), F32)
        if kind == 0:
            offset = [zero, zero]
            for n in (1, 2, 3):
                for half in (0, 1):
                    term = t_in[0, n, half].astype(F32)
                    offset[half] = offset[half] + jnp.where(own_y[n] < y, term, 0.0)
        else:
            sums = (
                t_out[1, 0].astype(F32),
                t_out[1, 1].astype(F32),
                t_in[1, 2, 0].astype(F32),
                t_in[1, 2, 1].astype(F32),
            )
            offset = []
            for b in BLOCKS:
                total = zero
                for n in range(4):
                    if n != b:
                        total = total + jnp.where(own_y[n] > own_y[b], sums[n], 0.0)
                offset.append(total)
        for half in (0, 1):
            running = offset[half]
            for k in range(NZ) if kind == 0 else reversed(range(NZ)):
                b_out[kind, k, half] = running.astype(BF16)
                running = running + pre[k, half]
        for o in FAR_FIRST:
            src = b_out.at[kind, (z + o) % NZ]
            dst = result.at[pl.ds(0, 2), slice_at(z), :]
            net.send((kind, "b"), src, dst, dev_z(o), "sums")
        result[pl.ds(0, 2), slice_at(z), :] = b_out[kind, z]

    PT = T // NX

    def quarter(rel_x):
        xs = (x + rel_x + NX) % NX
        return pl.ds(pl.multiple_of(xs * PT, PT), PT)

    def h4_start():
        src = hf.at[
            rows_of(c * T + x * PT, PT), pl.ds(pl.multiple_of((1 - pair) * KH, KH), KH)
        ]
        net.send(("h4", 0), src, h4.at[0, c, quarter(0), :], across, "h4")

    def h4_piece(j):
        def piece(rel_x, part):
            start, size = {"full": (0, KH), "top": (0, KH // 2), "bot": (KH // 2, KH // 2)}[part]
            return h4.at[j, c, quarter(rel_x), pl.ds(start, size)]

        return piece

    def h4_begin(j):
        net.recv(("h4", j))
        x_begin(("h4x", j), h4_piece(j), "h4")
        mine = h4_piece(j)(0, "full")
        if j == 0:
            net.send(("h4", 1), mine, h4_piece(1)(0, "full"), pair_same, "h4")
        net.send(("h4p", j), mine, mine, partner, "h4")

    def h4_step(j, stage):
        x_step(("h4x", j), ("h4p", j), h4_piece(j), stage, "h4")

    WIDE = 256

    def h4_turn_own():
        for k in range(KH // WIDE):
            cols = pl.ds(pl.multiple_of(pair * KH + k * WIDE, WIDE), WIDE)
            h4t[k * WIDE : (k + 1) * WIDE, 0 : 2 * CT] = hf[:, cols].T

    def h4_turn(j):
        net.recv(("h4p", j))
        for k in range(KH // WIDE):
            cut = slice(k * WIDE, (k + 1) * WIDE)
            h4t[cut, (2 + j) * CT : (3 + j) * CT] = h4[j, :, :, cut].reshape(CT, WIDE).T

    def project(b, part):
        start, size = (pair * KH, KH) if part == 0 else (own_y[1 + part] * KY, KY)
        rows = pl.ds(pl.multiple_of(start, KY), size)
        block = slice(b * CT, (b + 1) * CT)
        product = dot_nn(hf[block, rows], wf[rows, :])
        q32[block, :] = product if part == 0 else q32[block, :] + product

    causal = lax.broadcasted_iota(jnp.int32, (CT, CT), 0) >= lax.broadcasted_iota(
        jnp.int32, (CT, CT), 1
    )

    def attend(b):
        if b == 1:
            net.recv("prior")
        proj = q32[b * CT : (b + 1) * CT, :]
        feats = jnp.maximum(proj, 0.0).astype(BF16)
        qf[b] = feats
        keys, vals = kf[b], vb[b]
        state = prior[e] if b == 0 else prior[2]
        scores = jnp.where(causal, dot_nt(feats, keys), 0.0).astype(BF16)
        sc[b] = scores
        numer = dot_nn(scores, vals) + dot_nn(feats, state)
        inv = lax.rsqrt(jnp.mean(numer * numer, axis=-1, keepdims=True) + EPSILON)
        normed = numer * inv
        att[b] = normed.astype(BF16)
        grad = gb[b].astype(F32)
        d_num = (inv * (grad - normed * jnp.mean(grad * normed, axis=-1, keepdims=True))).astype(BF16)
        dn[b] = d_num
        mixed = jnp.where(causal, dot_nt(d_num, vals), 0.0).astype(BF16)
        mx[b] = mixed
        d_feat = dot_nn(mixed, keys) + dot_nt(d_num, state)
        d_q = jnp.where(proj > 0, d_feat, 0.0).astype(BF16)
        mine = slice(b * CT, (b + 1) * CT)
        dq4[mine, :] = d_q
        theirs = slice((2 + b) * CT, (3 + b) * CT)
        if b == 0:
            net.send(("dq", 1, 0), dq4.at[mine, :], dq4.at[theirs, :], across, "sums")
        else:
            for h in (0, 1):
                cols = half_cols(h)
                net.send(("dq", 1, h), dq4.at[mine, cols], dq4.at[theirs, cols], across, "sums")

    def state_send(b):
        s_out[1, b] = dot_tn(qf[b], dn[b]).astype(BF16)
        for o in FAR_FIRST:
            src = s_out.at[1, b, slice_at((z + o) % NZ), :]
            net.send((1, "s"), src, s_in.at[1, o, b], dev_z(o), "sums")

    def states():
        for name in ("k0", "k2", "v0", "v2"):
            local[name].wait()
        net.recv("kv0")
        kf[0] = jnp.maximum(kb[0], jnp.zeros_like(kb[0]))
        s_out[0, e] = dot_tn(kf[0], vb[0]).astype(BF16)
        s_out[0, 1 - e] = dot_tn(jnp.maximum(kb[2], jnp.zeros_like(kb[2])), vb[2]).astype(BF16)
        scan_start(0)

    def prior_send():
        net.recv((0, "b"))
        net.send("prior", prior.at[1 - e], prior.at[2], pair_same, "sums")

    def keys_in():
        net.recv("kv1")
        kf[1] = jnp.maximum(kb[1], jnp.zeros_like(kb[1]))

    def grads_in():
        local["g"].wait()
        net.recv("g0")

    def block_parts(b):
        vg32[b] = dot_tn(sc[b], dn[b])
        kg32[b] = dot_tn(mx[b], qf[b])

    def state_parts(b):
        state = later[b]
        vg[b] = (vg32[b] + dot_nn(kf[b], state)).astype(BF16)
        d_key = kg32[b] + dot_nt(vb[b], state)
        kg[b] = jnp.where(kb[b] > 0, d_key, 0.0).astype(BF16)

    def part_rows(k):
        return pl.ds(pl.multiple_of(((1 - u) if k == 0 else u) * KY, KY), KY)

    def contract_own(k):
        g32[k] = dot_nn(h4t[part_rows(k), 0 : 2 * CT], dq4[0 : 2 * CT, :])

    REST = slice(2 * CT, 4 * CT)

    def half_cols(h):
        return slice(h * FEAT // 2, (h + 1) * FEAT // 2)

    def contract_far(k, h):
        cols = half_cols(h)
        if k == 0:
            net.recv(("dq", 1, h))
        to = ((z + ZM) % NZ) * CH
        rows = rows_of(((1 - u) if k == 0 else u) * KY + to, CH)
        far = g32[k, rows_of(to, CH), cols] + dot_nn(h4t[rows, REST], dq4[REST, cols])
        for s in BOTH:
            rows = rs_rows(part_of(s, ZM, ZM))
            rs_out[k, 0 if s > 0 else 1, ZM - 1, rows, cols] = far[rows, :].astype(BF16)
            rs_put(k, h, s, ZM)

    def contract_rest(k, h):
        cols = half_cols(h)
        g32[k, :, cols] = g32[k, :, cols] + dot_nn(h4t[part_rows(k), REST], dq4[REST, cols])

    def rs_rows(part):
        start, size = split(CH, part, CH * RS_EIGHTHS // 8)
        return slice(start, start + size)

    def rs_put(k, h, s, d):
        way, rows, cols = 0 if s > 0 else 1, rs_rows(part_of(s, d, ZM)), half_cols(h)
        net.send(
            ("rs", k, h, s, d) if d > 1 else ("rs", k, h),
            rs_out.at[k, way, d - 1, rows, cols],
            rs_in.at[k, way, d - 1, rows, cols],
            dev_z(s),
            "sums",
        )

    def rs_send(k, h, d):
        cols = half_cols(h)
        for s in BOTH:
            net.recv(("rs", k, h, s, d + 1))
            rows = rs_rows(part_of(s, d, ZM))
            size = rows.stop - rows.start
            to = (z + s * d + NZ) % NZ
            total = g32[k, rows_of(to * CH + rows.start, size), cols]
            way = 0 if s > 0 else 1
            rs_out[k, way, d - 1, rows, cols] = total.astype(BF16)
            came = rs_rows(part_of(s, d + 1, ZM))
            got = rs_in[k, way, d, came, cols].astype(F32)
            rs_out[k, way, d - 1, came, cols] = (total[came, :] + got).astype(BF16)
            rs_put(k, h, s, d)

    def rs_last(k, h):
        cols = half_cols(h)
        net.recv(("rs", k, h))
        total = g32[k, rows_of(z * CH, CH), cols]
        if ZM > 1:
            total = total + rs_in[k, 0, 0, :, cols].astype(F32) + rs_in[k, 1, 0, :, cols].astype(F32)
        else:
            came = [
                rs_in[k, way, 0, rs_rows(part), cols].astype(F32)
                for way, part in enumerate(("top", "bot"))
            ]
            total = total + jnp.concatenate(came, axis=0)
        at_cols = (2 * c + e) * FEAT + h * (FEAT // 2)
        mine = out_qg.at[:, pl.ds(pl.multiple_of(at_cols, FEAT // 2), FEAT // 2)]

        if k == 0:
            qsend[:, cols] = total.astype(BF16)
            for core, to in pair_cores:
                piece = qsend.at[rows_of(core * WR, WR), cols]
                net.send("qin", piece, qin.at[c, :, cols], to, "io")
        else:
            qg[:, cols] = total
            net.send("out", qg.at[rows_of(p * WR, WR), cols], mine, partner, "io")
            out_qg[:, pl.ds(pl.multiple_of(at_cols, FEAT // 2), FEAT // 2)] = qg[
                rows_of(c * WR, WR), cols
            ]

    def out_send(buf, out, rows, width):
        mine = out.at[:, head_cols(c, e, width)]

        def piece(block, core):
            return buf.at[block, rows_of(core * rows, rows), :]

        net.send("out", piece(1, c), mine, pair_same, "io")
        net.send("out", piece(1, p), mine, pair_other, "io")
        net.send("out", piece(0, p), mine, partner, "io")
        out[:, head_cols(c, e, width)] = buf[0, rows_of(c * rows, rows), :]

    def att_out():
        out_send(att, out_att, T, HEAD_DIM)

    def later_parts():
        net.recv((1, "b"))
        for b in BLOCKS:
            state_parts(b)
        out_send(kg, out_kg, T, FEAT)
        out_send(vg, out_vg, T, HEAD_DIM)

    tasks = {
        "w": w_begin,
        "A": w_a,
        "B": lambda which, d: w_next("B", which, d),
        "across": w_turn,
        "last": w_last,
        "h": h_begin,
        "hx": h_step,
        "hp": h_all,
        "state": states,
        "tot": scan_totals,
        "back": lambda kind: scan_back(kind, later if kind else prior),
        "prior": prior_send,
        "kv1": keys_in,
        "g0": grads_in,
        "h4s": h4_start,
        "h4": h4_begin,
        "h4x": h4_step,
        "turnown": h4_turn_own,
        "turn": h4_turn,
        "mm": project,
        "att": attend,
        "s1": state_send,
        "outatt": att_out,
        "blk": block_parts,
        "own": contract_own,
        "far": contract_far,
        "rest": contract_rest,
        "rs": rs_send,
        "rsl": rs_last,
        "later": later_parts,
    }
    for name, *where in ORDER:
        tasks[name](*where)
    net.recv("qin")
    for core in (0, 1):
        out_qg[:, head_cols(core, 1 - e, FEAT)] = qin[core].astype(F32)
    net.recv("out")
    net.finish()


def write_out(*refs):
    ins, outs, sems = refs[:4], refs[4:8], refs[8]
    copies = [
        pltpu.make_async_copy(src, dst, sems.at[n]) for n, (src, dst) in enumerate(zip(ins, outs))
    ]
    for copy in copies:
        copy.start()
    for copy in copies:
        copy.wait()


def solution(mesh):
    NX, ctx_size = mesh.shape["heads"], mesh.shape["ctx"]
    NY = 4
    NZ = ctx_size // (NY * CORES)
    sizes = (NX, NY, NZ)

    def body(hidden, w_query, key_input, values, cotangent):
        T, DX = hidden.shape
        WR, NALL = w_query.shape
        VALL = values.shape[1]
        D = NX * DX
        CH = CORES * WR
        KY = NZ * CH
        CT = CORES * T
        ZM = NZ // 2
        SR = FEAT // NZ
        any_space = pl.BlockSpec(memory_space=pl.ANY)
        vmem_space = pl.BlockSpec(memory_space=pltpu.VMEM)
        outs = (((T, VALL), BF16), ((WR, NALL), F32), ((T, NALL), BF16), ((T, VALL), BF16))

        def vmem(*shape, dtype=BF16):
            return pltpu.VMEM(shape, dtype)

        def run(*refs):
            kernel(sizes, *refs)

        parts = pl.pallas_call(
            run,
            out_shape=tuple(pltpu.VMEM(*of) for of in outs),
            in_specs=[any_space] * 5,
            out_specs=(vmem_space,) * 4,
            scratch_shapes=[
                vmem(2 * CT, D),
                vmem(D, FEAT),
                vmem(3, CT, FEAT),
                vmem(2, CT, FEAT),
                vmem(3, CT, HEAD_DIM),
                vmem(2, CT, HEAD_DIM),
                vmem(2 * CT, FEAT, dtype=F32),
                vmem(2, CT, FEAT),
                vmem(2, CT, HEAD_DIM),
                vmem(2, CT, HEAD_DIM),
                vmem(2, CT, CT),
                vmem(2, CT, CT),
                vmem(2, CT, HEAD_DIM, dtype=F32),
                vmem(2, CT, FEAT, dtype=F32),
                vmem(2, CT, FEAT),
                vmem(2, CT, HEAD_DIM),
                vmem(2, 2, FEAT, HEAD_DIM),
                vmem(2, NZ, 2, SR, HEAD_DIM),
                vmem(2, 2, SR, HEAD_DIM),
                vmem(2, NY, 2, SR, HEAD_DIM),
                vmem(2, NZ, 2, SR, HEAD_DIM),
                vmem(3, FEAT, HEAD_DIM),
                vmem(2, FEAT, HEAD_DIM),
                vmem(NZ, 2, SR, HEAD_DIM, dtype=F32),
                vmem(2, CORES, T, 2 * KY),
                vmem(2 * KY, 4 * CT),
                vmem(4 * CT, FEAT),
                vmem(2, KY, FEAT, dtype=F32),
                vmem(2, 2, ZM, CH, FEAT),
                vmem(2, 2, ZM, CH, FEAT),
                vmem(CH, FEAT, dtype=F32),
                vmem(CH, FEAT),
                vmem(CORES, WR, FEAT),
                pltpu.SemaphoreType.DMA((LANES,)),
                pltpu.SemaphoreType.DMA((GROUPS,)),
                pltpu.SemaphoreType.DMA((LOCALS,)),
            ],
            compiler_params=pltpu.CompilerParams(
                collective_id=0, has_side_effects=True, vmem_limit_bytes=60000 * 1024
            ),
        )(hidden, w_query, key_input, values, cotangent)
        return pl.pallas_call(
            write_out,
            out_shape=tuple(jax.ShapeDtypeStruct(*of) for of in outs),
            in_specs=[vmem_space] * 4,
            out_specs=(any_space,) * 4,
            scratch_shapes=[pltpu.SemaphoreType.DMA((4,))],
        )(*[pltpu.with_memory_space_constraint(part, pltpu.VMEM) for part in parts])

    spec = P("ctx", "heads")
    return jax.shard_map(
        body, mesh=mesh, in_specs=(spec,) * 5, out_specs=(spec,) * 4, check_vma=False
    )
```
